8 devices in a mesh: dp: 1 (over z), tp: 8 (over y, x, core).
Axes of the slice: x: 2, y: 2, z: 1, core: 2. Of those that a mesh axis runs over, the one named last changes fastest.
Arguments:
- x: bfloat16 [32, 1024], P('dp')
- k_cache: bfloat16 [32, 8192, 16, 64], P('dp', None, 'tp')
- v_cache: bfloat16 [32, 8192, 16, 64], P('dp', None, 'tp')
- seq_lens: int32 [32], P('dp')
- nbr_enc: bfloat16 [32, 256, 1024], P('dp', 'tp')
- ln1_gain: float32 [1024], replicated
- ln1_bias: float32 [1024], replicated
- w_q: bfloat16 [1024, 1024], P(None, 'tp')
- w_k: bfloat16 [1024, 1024], P(None, 'tp')
- w_v: bfloat16 [1024, 1024], P(None, 'tp')
- w_o: bfloat16 [1024, 1024], P('tp')
- ln2_gain: float32 [1024], replicated
- ln2_bias: float32 [1024], replicated
- wq_c: bfloat16 [1024, 1024], P(None, 'tp')
- wk_c: bfloat16 [1024, 1024], P(None, 'tp')
- wv_c: bfloat16 [1024, 1024], P(None, 'tp')
- wo_c: bfloat16 [1024, 1024], P('tp')
- ln3_gain: float32 [1024], replicated
- ln3_bias: float32 [1024], replicated
- w_up: bfloat16 [1024, 4096], P(None, 'tp')
- w_down: bfloat16 [4096, 1024], P('tp')
Outputs:
- output 1: bfloat16 [32, 1024], P('dp')
- output 2: bfloat16 [32, 16, 64], P('dp', 'tp')
- output 3: bfloat16 [32, 16, 64], P('dp', 'tp')
All inputs are finite; a program needn't handle non-finite values.
Results may differ from the reference program's by a relative error of at most 0.0159068.
Values are sent between devices in bfloat16 or wider.
A program may use at most 1 GiB of HBM per device.

```python
import jax
import jax.numpy as jnp
from jax import lax

D = 1024
HEADS = 16
HEAD = 64
ENC_DIM = 1024
NEIGHBOURS = 2
RET_LEN = 128
SEGMENT = 64
BATCH = 32
CTX_LEN = 8192

FF_DIM = 4 * D
WIDTH = HEADS * HEAD
NBR_TOKENS = NEIGHBOURS * RET_LEN
LN_EPS = 1e-5


def draw_lens(key):
    key_len, key_pick = jax.random.split(key)
    top_seg = CTX_LEN // SEGMENT - 1
    seg_count = jax.random.randint(key_len, (BATCH,), 1, top_seg + 1)
    pick_row = jax.random.randint(key_pick, (), 0, BATCH)
    seg_count = jnp.where(jnp.arange(BATCH) == pick_row, top_seg, seg_count)
    return (seg_count * SEGMENT).astype(jnp.int32)


def draw_weight(key, fan_in, fan_out, gain):
    return (jax.random.normal(key, (fan_in, fan_out), jnp.float32) * (gain * fan_in ** -0.5)).astype(jnp.bfloat16)


def setup_inputs(seed: int = 0, part: int = 0) -> dict:
    own_keys = jax.random.split(jax.random.fold_in(jax.random.key(seed), part), 8)
    shared_keys = jax.random.split(jax.random.key(seed + 1), 12)
    ramp = (2.0 * jnp.arange(CTX_LEN, dtype=jnp.float32) / CTX_LEN - 1.0)[None, :, None, None]
    cache_shape = (BATCH, CTX_LEN, HEADS, HEAD)
    head_shape = (BATCH, 1, HEADS, HEAD)
    k_dir = jax.random.normal(own_keys[1], head_shape, jnp.float32)
    k_cache = 3.0 * ramp * k_dir + jax.random.normal(own_keys[2], cache_shape, jnp.float32)
    v_base = jax.random.normal(own_keys[3], head_shape, jnp.float32)
    v_dir = jax.random.normal(own_keys[4], head_shape, jnp.float32)
    v_cache = v_base + ramp * v_dir + 0.5 * jax.random.normal(own_keys[5], cache_shape, jnp.float32)
    nbr_enc = jax.random.normal(own_keys[7], (BATCH, NBR_TOKENS, ENC_DIM), jnp.float32)
    ln_gains = 1.0 + 0.4 * jax.random.normal(shared_keys[0], (3, D), jnp.float32)
    ln_biases = 0.4 * jax.random.normal(shared_keys[1], (3, D), jnp.float32)
    return {
        'x': jax.random.normal(own_keys[0], (BATCH, D), jnp.float32).astype(jnp.bfloat16),
        'k_cache': k_cache.astype(jnp.bfloat16),
        'v_cache': v_cache.astype(jnp.bfloat16),
        'seq_lens': draw_lens(own_keys[6]),
        'nbr_enc': nbr_enc.astype(jnp.bfloat16),
        'ln1_gain': ln_gains[0],
        'ln1_bias': ln_biases[0],
        'w_q': draw_weight(shared_keys[2], D, WIDTH, 1.0),
        'w_k': draw_weight(shared_keys[3], D, WIDTH, 1.0),
        'w_v': draw_weight(shared_keys[4], D, WIDTH, 1.0),
        'w_o': draw_weight(shared_keys[5], WIDTH, D, 1.0),
        'ln2_gain': ln_gains[1],
        'ln2_bias': ln_biases[1],
        'wq_c': draw_weight(shared_keys[6], D, WIDTH, 1.0),
        'wk_c': draw_weight(shared_keys[7], ENC_DIM, WIDTH, 2.5),
        'wv_c': draw_weight(shared_keys[8], ENC_DIM, WIDTH, 1.0),
        'wo_c': draw_weight(shared_keys[9], WIDTH, D, 1.0),
        'ln3_gain': ln_gains[2],
        'ln3_bias': ln_biases[2],
        'w_up': draw_weight(shared_keys[10], D, FF_DIM, 1.0),
        'w_down': draw_weight(shared_keys[11], FF_DIM, D, 1.5),
    }


def layer_norm(values, ln_gain, ln_bias):
    row_mean = jnp.mean(values, axis=-1, keepdims=True)
    centred = values - row_mean
    row_var = jnp.mean(jnp.square(centred), axis=-1, keepdims=True)
    return (centred * lax.rsqrt(row_var + LN_EPS) * ln_gain + ln_bias).astype(jnp.bfloat16)


def project(operand, weight):
    return jnp.dot(operand, weight, preferred_element_type=jnp.float32).astype(jnp.bfloat16)


def reference(x, k_cache, v_cache, seq_lens, nbr_enc, ln1_gain, ln1_bias, w_q, w_k, w_v, w_o, ln2_gain, ln2_bias, wq_c, wk_c, wv_c, wo_c, ln3_gain, ln3_bias, w_up, w_down):
    q_scale = HEAD ** -0.5
    positions = jnp.arange(CTX_LEN)
    residual = x.astype(jnp.float32)
    a_norm = layer_norm(residual, ln1_gain, ln1_bias)
    q_new = project(a_norm, w_q).reshape(BATCH, HEADS, HEAD)
    k_new = project(a_norm, w_k).reshape(BATCH, HEADS, HEAD)
    v_new = project(a_norm, w_v).reshape(BATCH, HEADS, HEAD)

    def self_row(row_args):
        q_row, k_rows, v_rows, k_one, v_one, length = row_args
        q_f = q_row.astype(jnp.float32)
        s_old = jnp.einsum('hd,thd->ht', q_f, k_rows.astype(jnp.float32)) * q_scale
        s_old = jnp.where(positions[None, :] < length, s_old, -1e30)
        s_new = jnp.sum(q_f * k_one.astype(jnp.float32), axis=-1) * q_scale
        row_max = jnp.maximum(jnp.max(s_old, axis=-1), s_new)
        e_old = jnp.exp(s_old - row_max[:, None])
        e_new = jnp.exp(s_new - row_max)
        row_sum = jnp.sum(e_old, axis=-1) + e_new
        p_old = (e_old / row_sum[:, None]).astype(jnp.bfloat16).astype(jnp.float32)
        p_new = (e_new / row_sum).astype(jnp.bfloat16).astype(jnp.float32)
        head_out = jnp.einsum('ht,thd->hd', p_old, v_rows.astype(jnp.float32)) + p_new[:, None] * v_one.astype(jnp.float32)
        return head_out.astype(jnp.bfloat16)

    def cross_row(row_args):
        q_row, enc_row = row_args
        k_nbr = project(enc_row, wk_c).reshape(NBR_TOKENS, HEADS, HEAD).astype(jnp.float32)
        v_nbr = project(enc_row, wv_c).reshape(NBR_TOKENS, HEADS, HEAD).astype(jnp.float32)
        scores = jnp.einsum('hd,nhd->hn', q_row.astype(jnp.float32), k_nbr) * q_scale
        probs = jax.nn.softmax(scores, axis=-1).astype(jnp.bfloat16).astype(jnp.float32)
        return jnp.einsum('hn,nhd->hd', probs, v_nbr).astype(jnp.bfloat16)

    self_out = lax.map(self_row, (q_new, k_cache, v_cache, k_new, v_new, seq_lens))
    residual = residual + project(self_out.reshape(BATCH, WIDTH), w_o).astype(jnp.float32)
    c_norm = layer_norm(residual, ln2_gain, ln2_bias)
    q_cross = project(c_norm, wq_c).reshape(BATCH, HEADS, HEAD)
    cross_out = lax.map(cross_row, (q_cross, nbr_enc))
    residual = residual + project(cross_out.reshape(BATCH, WIDTH), wo_c).astype(jnp.float32)
    m_norm = layer_norm(residual, ln3_gain, ln3_bias)
    hidden = jax.nn.gelu(jnp.dot(m_norm, w_up, preferred_element_type=jnp.float32), approximate=False).astype(jnp.bfloat16)
    layer_out = (residual + project(hidden, w_down).astype(jnp.float32)).astype(jnp.bfloat16)
    return layer_out, k_new, v_new
```

```python
import functools

import jax
import jax.numpy as jnp
from jax import lax
from jax.experimental import pallas as pl
from jax.experimental.pallas import tpu as pltpu
from jax.sharding import PartitionSpec as P

LN_EPS = 1e-5
CHUNK = 1024
SLOTS = 8
UNROLL = 2
NEG = -1e30


def layer_norm(values, ln_gain, ln_bias):
    row_mean = jnp.mean(values, axis=-1, keepdims=True)
    centred = values - row_mean
    row_var = jnp.mean(jnp.square(centred), axis=-1, keepdims=True)
    return (centred * lax.rsqrt(row_var + LN_EPS) * ln_gain + ln_bias).astype(jnp.bfloat16)


def project(operand, weight):
    return jnp.dot(operand, weight, preferred_element_type=jnp.float32).astype(jnp.bfloat16)


def self_kernel(lens_ref, x_ref, gain_ref, bias_ref, wq_hbm, wk_hbm, wv_hbm, wo_hbm, k_hbm, v_hbm,
                part_ref, know_ref, vnow_ref,
                wq_buf, wk_buf, wv_buf, wo_buf, k_buf, v_buf, q_all, p_buf, acc, mx, sm, w_sem, k_sem, v_sem):
    batch = x_ref.shape[0]
    dim = k_buf.shape[1]
    weights = [pltpu.make_async_copy(src, dst, w_sem.at[i]) for i, (src, dst) in enumerate(
        ((wq_hbm, wq_buf), (wk_hbm, wk_buf), (wv_hbm, wv_buf), (wo_hbm, wo_buf)))]
    for w in weights:
        w.start()

    def length(b):
        return jnp.where(b < batch, lens_ref[jnp.minimum(b, batch - 1)], 64)

    def advance(item):
        b, j = item
        more = (j + 1) * CHUNK < length(b)
        return jnp.where(more, b, jnp.minimum(b + 1, batch)), jnp.where(more, j + 1, 0)

    def view(item):
        b, j = item
        rem = jnp.minimum(length(b) - j * CHUNK, CHUNK)
        size = pl.multiple_of((rem + 127) // 128 * 128, 128)
        return jnp.minimum(b, batch - 1), pl.multiple_of(j * CHUNK, CHUNK), size

    def fetch(hbm, buf, sem, item, slot):
        b, start, size = view(item)
        return pltpu.make_async_copy(hbm.at[b, :, pl.ds(start, size)], buf.at[slot, :, pl.ds(0, size)], sem.at[slot])

    items = []
    item = (jnp.int32(0), jnp.int32(0))
    for _ in range(SLOTS):
        items.append(item)
        item = advance(item)
    ahead = item
    for s in range(SLOTS):
        fetch(k_hbm, k_buf, k_sem, items[s], s).start()
    v_buf[...] = jnp.zeros_like(v_buf)
    for s in range(SLOTS):
        fetch(v_hbm, v_buf, v_sem, items[s], s).start()

    def count(b, total):
        return total + (lens_ref[b] + CHUNK - 1) // CHUNK

    groups = (lax.fori_loop(0, batch, count, jnp.int32(0)) + UNROLL - 1) // UNROLL

    normed = layer_norm(x_ref[...].astype(jnp.float32), gain_ref[...], bias_ref[...])
    for w in weights[:3]:
        w.wait()
    q_new = project(normed, wq_buf[...])
    k_new = project(normed, wk_buf[...])
    v_new = project(normed, wv_buf[...])
    half = dim // 2
    for h in range(2):
        know_ref[:, h, :] = k_new[:, h * half:(h + 1) * half]
        vnow_ref[:, h, :] = v_new[:, h * half:(h + 1) * half]
    lane = lax.broadcasted_iota(jnp.int32, (batch, 8, dim), 2)
    row = lax.broadcasted_iota(jnp.int32, (batch, 8, dim), 1)
    own = (lane // half) == row
    q_f = q_new.astype(jnp.float32)
    q_wide = jnp.where(own, q_f[:, None, :], 0.0)
    q_all[:batch] = q_wide.astype(jnp.bfloat16)
    q_all[batch] = jnp.zeros((8, dim), jnp.bfloat16)
    s_new = jnp.sum(q_wide * k_new.astype(jnp.float32)[:, None, :], axis=-1, keepdims=True) * (half ** -0.5)
    mx[:batch] = jnp.broadcast_to(s_new, (batch, 8, dim))
    sm[:batch] = jnp.ones((batch, 8, dim), jnp.float32)
    acc[:batch] = jnp.broadcast_to(v_new.astype(jnp.float32)[:, None, :], (batch, 8, dim))
    mx[batch] = jnp.zeros((8, dim), jnp.float32)
    sm[batch] = jnp.ones((8, dim), jnp.float32)
    acc[batch] = jnp.zeros((8, dim), jnp.float32)

    spot = lax.broadcasted_iota(jnp.int32, (8, CHUNK), 1)
    scale = half ** -0.5

    def scores(item, slot):
        b, j = item
        s = jnp.dot(q_all[b], k_buf[slot], preferred_element_type=jnp.float32) * scale
        s = jnp.where(spot < length(b) - j * CHUNK, s, NEG)
        top = jnp.max(s, axis=-1, keepdims=True)
        e = jnp.exp(s - top)
        return e.astype(jnp.bfloat16), top, jnp.sum(e, axis=-1, keepdims=True)

    def merge(item, p, top, total, slot):
        b, _ = item
        o = lax.dot_general(p, v_buf[slot], (((1,), (1,)), ((), ())), preferred_element_type=jnp.float32)
        old = mx[b]
        new = jnp.maximum(old, top)
        keep = jnp.exp(old - new)
        add = jnp.exp(top - new)
        mx[b] = new
        sm[b] = sm[b] * keep + total * add
        acc[b] = acc[b] * keep + o * add

    def stage_a(group_items, slot0):
        out = []
        for u in range(UNROLL):
            out.append(scores(group_items[u], slot0 + u))
        return out

    def slot_of(group):
        return lax.rem(group * UNROLL, SLOTS)

    def flat(seq):
        return tuple(x for pair in seq for x in pair)

    def pair(vals):
        return [(vals[2 * i], vals[2 * i + 1]) for i in range(UNROLL)]

    cur = [items[u] for u in range(UNROLL)]
    for u in range(UNROLL):
        fetch(k_hbm, k_buf, k_sem, cur[u], u).wait()
    first = stage_a(cur, 0)
    for u in range(UNROLL):
        p_buf[0, u] = first[u][0]
    k_next = []
    for u in range(UNROLL):
        k_next.append(ahead)
        ahead = advance(ahead)
    for u in range(UNROLL):
        fetch(k_hbm, k_buf, k_sem, k_next[u], u).start()
    depth = SLOTS // UNROLL

    def step(g, carry):
        prev = pair(carry[:2 * UNROLL])
        v_next = pair(carry[2 * UNROLL:4 * UNROLL])
        walk = (carry[4 * UNROLL], carry[4 * UNROLL + 1])
        stats = carry[4 * UNROLL + 2:]
        now = []
        it = advance(prev[-1])
        for _ in range(UNROLL):
            now.append(it)
            it = advance(it)
        slot_b = slot_of(g - 1)
        slot_a = slot_of(g)
        for u in range(UNROLL):
            fetch(v_hbm, v_buf, v_sem, prev[u], slot_b + u).wait()
            fetch(k_hbm, k_buf, k_sem, now[u], slot_a + u).wait()
        before = lax.rem(g - 1, 2)
        after = lax.rem(g, 2)
        for u in range(UNROLL):
            merge(prev[u], p_buf[before, u], stats[2 * u], stats[2 * u + 1], slot_b + u)
        out = stage_a(now, slot_a)
        for u in range(UNROLL):
            p_buf[after, u] = out[u][0]
        k_items = []
        for _ in range(UNROLL):
            k_items.append(walk)
            walk = advance(walk)

        @pl.when(g + depth <= groups)
        def _():
            for u in range(UNROLL):
                fetch(k_hbm, k_buf, k_sem, k_items[u], slot_a + u).start()

        @pl.when(g - 1 + depth < groups)
        def _():
            for u in range(UNROLL):
                fetch(v_hbm, v_buf, v_sem, v_next[u], slot_b + u).start()

        new_stats = tuple(x for u in range(UNROLL) for x in out[u][1:])
        return flat(now) + flat(k_items) + walk + new_stats

    init = flat(cur) + flat(k_next) + ahead + tuple(x for u in range(UNROLL) for x in first[u][1:])
    lax.fori_loop(1, groups + 1, step, init)

    lane2 = lax.broadcasted_iota(jnp.int32, (batch, dim), 1)
    o0 = acc[:batch, 0, :] / sm[:batch, 0, :]
    o1 = acc[:batch, 1, :] / sm[:batch, 1, :]
    out = jnp.where(lane2 < half, o0, o1).astype(jnp.bfloat16)
    weights[3].wait()
    part_ref[...] = project(out, wo_buf[...])


def self_attention(x, k_cache, v_cache, seq_lens, gain, bias, w_q, w_k, w_v, w_o):
    batch, ctx, heads, head_dim = k_cache.shape
    dim = heads * head_dim
    model = x.shape[1]
    k_t = k_cache.transpose(0, 2, 3, 1).reshape(batch, dim, ctx)
    v_t = v_cache.transpose(0, 2, 3, 1).reshape(batch, dim, ctx)
    vmem = pl.BlockSpec(memory_space=pltpu.VMEM)
    anywhere = pl.BlockSpec(memory_space=pl.ANY)
    f32, bf16 = jnp.float32, jnp.bfloat16
    return pl.pallas_call(
        self_kernel,
        out_shape=(jax.ShapeDtypeStruct((batch, model), bf16),
                   jax.ShapeDtypeStruct((batch, heads, head_dim), bf16),
                   jax.ShapeDtypeStruct((batch, heads, head_dim), bf16)),
        in_specs=[pl.BlockSpec(memory_space=pltpu.SMEM)] + [vmem] * 3 + [anywhere] * 6,
        out_specs=(vmem, vmem, vmem),
        scratch_shapes=[
            pltpu.VMEM((model, dim), bf16), pltpu.VMEM((model, dim), bf16), pltpu.VMEM((model, dim), bf16),
            pltpu.VMEM((dim, model), bf16),
            pltpu.VMEM((SLOTS, dim, CHUNK), bf16), pltpu.VMEM((SLOTS, dim, CHUNK), bf16),
            pltpu.VMEM((batch + 1, 8, dim), bf16),
            pltpu.VMEM((2, UNROLL, 8, CHUNK), bf16),
            pltpu.VMEM((batch + 1, 8, dim), f32), pltpu.VMEM((batch + 1, 8, dim), f32), pltpu.VMEM((batch + 1, 8, dim), f32),
            pltpu.SemaphoreType.DMA((4,)), pltpu.SemaphoreType.DMA((SLOTS,)), pltpu.SemaphoreType.DMA((SLOTS,)),
        ],
        cost_estimate=pl.CostEstimate(flops=2 * 2 * batch * ctx * dim * 8, bytes_accessed=batch * ctx * dim * 2, transcendentals=0),
        name="self_attention",
    )(seq_lens, x, gain.reshape(1, model), bias.reshape(1, model), w_q, w_k, w_v, w_o, k_t, v_t)


def cross_attention(q_cross, k_nbr, v_nbr, q_scale):
    scores = jnp.einsum('bhd,bnhd->bhn', q_cross, k_nbr, preferred_element_type=jnp.float32) * q_scale
    probs = jax.nn.softmax(scores, axis=-1).astype(jnp.bfloat16)
    return jnp.einsum('bhn,bnhd->bhd', probs, v_nbr, preferred_element_type=jnp.float32).astype(jnp.bfloat16)


def local_step(x, k_cache, v_cache, seq_lens, nbr_enc, ln1_gain, ln1_bias, w_q, w_k, w_v, w_o, ln2_gain, ln2_bias, wq_c, wk_c, wv_c, wo_c, ln3_gain, ln3_bias, w_up, w_down):
    batch = x.shape[0]
    heads = k_cache.shape[2]
    head_dim = k_cache.shape[3]
    q_scale = head_dim ** -0.5
    residual = x.astype(jnp.float32)
    self_part, k_new, v_new = self_attention(x, k_cache, v_cache, seq_lens, ln1_gain, ln1_bias, w_q, w_k, w_v, w_o)
    residual = residual + lax.psum(self_part, 'tp').astype(jnp.float32)
    c_norm = layer_norm(residual, ln2_gain, ln2_bias)
    q_cross = project(c_norm, wq_c).reshape(batch, heads, head_dim)
    enc_all = lax.all_gather(nbr_enc, 'tp', axis=1, tiled=True)
    nbr_tokens = enc_all.shape[1]
    k_nbr = jnp.einsum('bne,ef->bnf', enc_all, wk_c, preferred_element_type=jnp.float32).astype(jnp.bfloat16).reshape(batch, nbr_tokens, heads, head_dim)
    v_nbr = jnp.einsum('bne,ef->bnf', enc_all, wv_c, preferred_element_type=jnp.float32).astype(jnp.bfloat16).reshape(batch, nbr_tokens, heads, head_dim)
    cross_out = cross_attention(q_cross, k_nbr, v_nbr, q_scale)
    cross_part = project(cross_out.reshape(batch, heads * head_dim), wo_c)
    residual = residual + lax.psum(cross_part, 'tp').astype(jnp.float32)
    m_norm = layer_norm(residual, ln3_gain, ln3_bias)
    hidden = jax.nn.gelu(jnp.dot(m_norm, w_up, preferred_element_type=jnp.float32), approximate=False).astype(jnp.bfloat16)
    mlp_part = project(hidden, w_down)
    layer_out = (residual + lax.psum(mlp_part, 'tp').astype(jnp.float32)).astype(jnp.bfloat16)
    return layer_out, k_new, v_new


def solution(mesh):
    row_spec = P('dp', None)
    cache_spec = P('dp', None, 'tp', None)
    head_spec = P('dp', 'tp', None)
    vec_spec = P(None)
    col_split = P(None, 'tp')
    row_split = P('tp', None)
    in_specs = (row_spec, cache_spec, cache_spec, P('dp'), P('dp', 'tp', None), vec_spec, vec_spec, col_split, col_split, col_split, row_split, vec_spec, vec_spec, col_split, col_split, col_split, row_split, vec_spec, vec_spec, col_split, row_split)
    out_specs = (row_spec, head_spec, head_spec)
    return jax.shard_map(local_step, mesh=mesh, in_specs=in_specs, out_specs=out_specs, check_vma=False)
```

```python
import functools

import jax
import jax.numpy as jnp
from jax import lax
from jax.experimental import pallas as pl
from jax.experimental.pallas import tpu as pltpu
from jax.sharding import PartitionSpec as P

LN_EPS = 1e-5
CHUNK = 1024
SLOTS = 24
UNROLL = 2
NEG = -1e30


def layer_norm(values, ln_gain, ln_bias):
    row_mean = jnp.mean(values, axis=-1, keepdims=True)
    centred = values - row_mean
    row_var = jnp.mean(jnp.square(centred), axis=-1, keepdims=True)
    return (centred * lax.rsqrt(row_var + LN_EPS) * ln_gain + ln_bias).astype(jnp.bfloat16)


def project(operand, weight):
    return jnp.dot(operand, weight, preferred_element_type=jnp.float32).astype(jnp.bfloat16)


def self_kernel(lens_ref, x_ref, gain_ref, bias_ref, wq_hbm, wk_hbm, wv_hbm, wo_hbm, k_hbm, v_hbm,
                part_ref, know_ref, vnow_ref,
                wq_buf, wk_buf, wv_buf, wo_buf, k_buf, v_buf, q_all, p_buf, acc, mx, sm, row_tab, start_tab, rem_tab,
                w_sem, k_sem, v_sem):
    batch = x_ref.shape[0]
    dim = k_buf.shape[1]
    weights = [pltpu.make_async_copy(src, dst, w_sem.at[i]) for i, (src, dst) in enumerate(
        ((wq_hbm, wq_buf), (wk_hbm, wk_buf), (wv_hbm, wv_buf), (wo_hbm, wo_buf)))]
    for w in weights:
        w.start()

    def build(i, carry):
        b, start, left = carry
        row_tab[i] = b
        start_tab[i] = start
        rem_tab[i] = jnp.minimum(left, CHUNK)
        more = left > CHUNK
        nb = jnp.minimum(b + 1, batch)
        fresh = jnp.where(nb < batch, lens_ref[jnp.minimum(nb, batch - 1)], 64)
        return jnp.where(more, b, nb), jnp.where(more, start + CHUNK, 0), jnp.where(more, left - CHUNK, fresh)

    def size_of(i):
        return pl.multiple_of((rem_tab[i] + 127) // 128 * 128, 128)

    def fetch(hbm, buf, sem, i, slot):
        size = size_of(i)
        b = jnp.minimum(row_tab[i], batch - 1)
        return pltpu.make_async_copy(
            hbm.at[b, :, pl.ds(pl.multiple_of(start_tab[i], CHUNK), size)], buf.at[slot, :, pl.ds(0, size)], sem.at[slot])

    def fetch_k(i, slot):
        return fetch(k_hbm, k_buf, k_sem, i, slot)

    def fetch_v(i, slot):
        return fetch(v_hbm, v_buf, v_sem, i, slot)

    def open_k(i, carry):
        carry = build(i, carry)
        fetch_k(i, i).start(priority=0)
        return carry

    carry = lax.fori_loop(0, SLOTS, open_k, (jnp.int32(0), jnp.int32(0), lens_ref[0]))
    v_buf[...] = jnp.zeros_like(v_buf)

    def open_v(i, _):
        fetch_v(i, i).start(priority=1)
        return 0

    lax.fori_loop(0, SLOTS, open_v, 0)

    def count(b, total):
        return total + (lens_ref[b] + CHUNK - 1) // CHUNK

    groups = (lax.fori_loop(0, batch, count, jnp.int32(0)) + UNROLL - 1) // UNROLL
    lax.fori_loop(SLOTS, (groups + 1) * UNROLL, build, carry)

    normed = layer_norm(x_ref[...].astype(jnp.float32), gain_ref[...], bias_ref[...])
    for w in weights[:3]:
        w.wait()
    q_new = project(normed, wq_buf[...])
    k_new = project(normed, wk_buf[...])
    v_new = project(normed, wv_buf[...])
    half = dim // 2
    for h in range(2):
        know_ref[:, h, :] = k_new[:, h * half:(h + 1) * half]
        vnow_ref[:, h, :] = v_new[:, h * half:(h + 1) * half]
    lane = lax.broadcasted_iota(jnp.int32, (batch, 8, dim), 2)
    row = lax.broadcasted_iota(jnp.int32, (batch, 8, dim), 1)
    own = (lane // half) == row
    q_f = q_new.astype(jnp.float32)
    q_wide = jnp.where(own, q_f[:, None, :], 0.0)
    q_all[:batch] = q_wide.astype(jnp.bfloat16)
    q_all[batch] = jnp.zeros((8, dim), jnp.bfloat16)
    s_new = jnp.sum(q_wide * k_new.astype(jnp.float32)[:, None, :], axis=-1, keepdims=True) * (half ** -0.5)
    mx[:batch] = jnp.broadcast_to(s_new, (batch, 8, dim))
    sm[:batch] = jnp.ones((batch, 8, dim), jnp.float32)
    acc[:batch] = jnp.broadcast_to(v_new.astype(jnp.float32)[:, None, :], (batch, 8, dim))
    mx[batch] = jnp.zeros((8, dim), jnp.float32)
    sm[batch] = jnp.ones((8, dim), jnp.float32)
    acc[batch] = jnp.zeros((8, dim), jnp.float32)

    spot = lax.broadcasted_iota(jnp.int32, (8, CHUNK), 1)
    scale = half ** -0.5

    def scores(i, slot):
        s = jnp.dot(q_all[row_tab[i]], k_buf[slot], preferred_element_type=jnp.float32) * scale
        s = jnp.where(spot < rem_tab[i], s, NEG)
        top = jnp.max(s, axis=-1, keepdims=True)
        e = jnp.exp(s - top)
        return e.astype(jnp.bfloat16), top, jnp.sum(e, axis=-1, keepdims=True)

    def weigh(p, slot):
        return lax.dot_general(p, v_buf[slot], (((1,), (1,)), ((), ())), preferred_element_type=jnp.float32)

    def merge(i, o, top, total):
        b = row_tab[i]
        old = mx[b]
        new = jnp.maximum(old, top)
        keep = jnp.exp(old - new)
        add = jnp.exp(top - new)
        mx[b] = new
        sm[b] = sm[b] * keep + total * add
        acc[b] = acc[b] * keep + o * add

    for u in range(UNROLL):
        fetch_k(u, u).wait()
    first = [scores(u, u) for u in range(UNROLL)]
    for u in range(UNROLL):
        p_buf[0, u] = first[u][0]
    for u in range(UNROLL):
        fetch_k(SLOTS + u, u).start(priority=0)
    depth = SLOTS // UNROLL

    def step(g, stats):
        prev = (g - 1) * UNROLL
        now = g * UNROLL
        slot_b = lax.rem(prev, SLOTS)
        slot_a = lax.rem(now, SLOTS)
        for u in range(UNROLL):
            fetch_k(now + u, slot_a + u).wait()
        for u in range(UNROLL):
            fetch_v(prev + u, slot_b + u).wait()
        before = lax.rem(g - 1, 2)
        after = lax.rem(g, 2)
        p_prev = [p_buf[before, u] for u in range(UNROLL)]
        out = [scores(now + u, slot_a + u) for u in range(UNROLL)]
        o_prev = [weigh(p_prev[u], slot_b + u) for u in range(UNROLL)]
        for u in range(UNROLL):
            merge(prev + u, o_prev[u], stats[2 * u], stats[2 * u + 1])
        for u in range(UNROLL):
            p_buf[after, u] = out[u][0]

        @pl.when(g + depth <= groups)
        def _():
            for u in range(UNROLL):
                fetch_k(now + SLOTS + u, slot_a + u).start(priority=0)

        @pl.when(g - 1 + depth < groups)
        def _():
            for u in range(UNROLL):
                fetch_v(prev + SLOTS + u, slot_b + u).start(priority=1)

        return tuple(x for u in range(UNROLL) for x in out[u][1:])

    lax.fori_loop(1, groups + 1, step, tuple(x for u in range(UNROLL) for x in first[u][1:]))

    lane2 = lax.broadcasted_iota(jnp.int32, (batch, dim), 1)
    o0 = acc[:batch, 0, :] / sm[:batch, 0, :]
    o1 = acc[:batch, 1, :] / sm[:batch, 1, :]
    out = jnp.where(lane2 < half, o0, o1).astype(jnp.bfloat16)
    weights[3].wait()
    part_ref[...] = project(out, wo_buf[...])


def self_attention(x, k_cache, v_cache, seq_lens, gain, bias, w_q, w_k, w_v, w_o):
    batch, ctx, heads, head_dim = k_cache.shape
    dim = heads * head_dim
    model = x.shape[1]
    most = batch * (ctx // CHUNK) + 2 * UNROLL + SLOTS
    k_t = k_cache.transpose(0, 2, 3, 1).reshape(batch, dim, ctx)
    v_t = v_cache.transpose(0, 2, 3, 1).reshape(batch, dim, ctx)
    vmem = pl.BlockSpec(memory_space=pltpu.VMEM)
    anywhere = pl.BlockSpec(memory_space=pl.ANY)
    f32, bf16 = jnp.float32, jnp.bfloat16
    return pl.pallas_call(
        self_kernel,
        out_shape=(jax.ShapeDtypeStruct((batch, model), bf16),
                   jax.ShapeDtypeStruct((batch, heads, head_dim), bf16),
                   jax.ShapeDtypeStruct((batch, heads, head_dim), bf16)),
        in_specs=[pl.BlockSpec(memory_space=pltpu.SMEM)] + [vmem] * 3 + [anywhere] * 6,
        out_specs=(vmem, vmem, vmem),
        scratch_shapes=[
            pltpu.VMEM((model, dim), bf16), pltpu.VMEM((model, dim), bf16), pltpu.VMEM((model, dim), bf16),
            pltpu.VMEM((dim, model), bf16),
            pltpu.VMEM((SLOTS, dim, CHUNK), bf16), pltpu.VMEM((SLOTS, dim, CHUNK), bf16),
            pltpu.VMEM((batch + 1, 8, dim), bf16),
            pltpu.VMEM((2, UNROLL, 8, CHUNK), bf16),
            pltpu.VMEM((batch + 1, 8, dim), f32), pltpu.VMEM((batch + 1, 8, dim), f32), pltpu.VMEM((batch + 1, 8, dim), f32),
            pltpu.SMEM((most,), jnp.int32), pltpu.SMEM((most,), jnp.int32), pltpu.SMEM((most,), jnp.int32),
            pltpu.SemaphoreType.DMA((4,)), pltpu.SemaphoreType.DMA((SLOTS,)), pltpu.SemaphoreType.DMA((SLOTS,)),
        ],
        cost_estimate=pl.CostEstimate(flops=2 * 2 * batch * ctx * dim * 8, bytes_accessed=batch * ctx * dim * 2, transcendentals=0),
        name="self_attention",
    )(seq_lens, x, gain.reshape(1, model), bias.reshape(1, model), w_q, w_k, w_v, w_o, k_t, v_t)


def cross_attention(q_cross, k_nbr, v_nbr, q_scale):
    scores = jnp.einsum('bhd,bnhd->bhn', q_cross, k_nbr, preferred_element_type=jnp.float32) * q_scale
    probs = jax.nn.softmax(scores, axis=-1).astype(jnp.bfloat16)
    return jnp.einsum('bhn,bnhd->bhd', probs, v_nbr, preferred_element_type=jnp.float32).astype(jnp.bfloat16)


def local_step(x, k_cache, v_cache, seq_lens, nbr_enc, ln1_gain, ln1_bias, w_q, w_k, w_v, w_o, ln2_gain, ln2_bias, wq_c, wk_c, wv_c, wo_c, ln3_gain, ln3_bias, w_up, w_down):
    batch = x.shape[0]
    heads = k_cache.shape[2]
    head_dim = k_cache.shape[3]
    q_scale = head_dim ** -0.5
    residual = x.astype(jnp.float32)
    self_part, k_new, v_new = self_attention(x, k_cache, v_cache, seq_lens, ln1_gain, ln1_bias, w_q, w_k, w_v, w_o)
    residual = residual + lax.psum(self_part, 'tp').astype(jnp.float32)
    c_norm = layer_norm(residual, ln2_gain, ln2_bias)
    q_cross = project(c_norm, wq_c).reshape(batch, heads, head_dim)
    enc_all = lax.all_gather(nbr_enc, 'tp', axis=1, tiled=True)
    nbr_tokens = enc_all.shape[1]
    k_nbr = jnp.einsum('bne,ef->bnf', enc_all, wk_c, preferred_element_type=jnp.float32).astype(jnp.bfloat16).reshape(batch, nbr_tokens, heads, head_dim)
    v_nbr = jnp.einsum('bne,ef->bnf', enc_all, wv_c, preferred_element_type=jnp.float32).astype(jnp.bfloat16).reshape(batch, nbr_tokens, heads, head_dim)
    cross_out = cross_attention(q_cross, k_nbr, v_nbr, q_scale)
    cross_part = project(cross_out.reshape(batch, heads * head_dim), wo_c)
    residual = residual + lax.psum(cross_part, 'tp').astype(jnp.float32)
    m_norm = layer_norm(residual, ln3_gain, ln3_bias)
    hidden = jax.nn.gelu(jnp.dot(m_norm, w_up, preferred_element_type=jnp.float32), approximate=False).astype(jnp.bfloat16)
    mlp_part = project(hidden, w_down)
    layer_out = (residual + lax.psum(mlp_part, 'tp').astype(jnp.float32)).astype(jnp.bfloat16)
    return layer_out, k_new, v_new


def solution(mesh):
    row_spec = P('dp', None)
    cache_spec = P('dp', None, 'tp', None)
    head_spec = P('dp', 'tp', None)
    vec_spec = P(None)
    col_split = P(None, 'tp')
    row_split = P('tp', None)
    in_specs = (row_spec, cache_spec, cache_spec, P('dp'), P('dp', 'tp', None), vec_spec, vec_spec, col_split, col_split, col_split, row_split, vec_spec, vec_spec, col_split, col_split, col_split, row_split, vec_spec, vec_spec, col_split, row_split)
    out_specs = (row_spec, head_spec, head_spec)
    return jax.shard_map(local_step, mesh=mesh, in_specs=in_specs, out_specs=out_specs, check_vma=False)
```

```python
import functools

import jax
import jax.numpy as jnp
from jax import lax
from jax.experimental import pallas as pl
from jax.experimental.pallas import tpu as pltpu
from jax.sharding import PartitionSpec as P

LN_EPS = 1e-5
CHUNK = 1024
SLOTS = 24
UNROLL = 2
NEG = -1e30
HEADS_DIM = 64
PROJ_ROWS = 256
FAR_FIRST = (7, 6, 5, 4, 3, 2, 1)
MESH = pl.DeviceIdType.MESH


def layer_norm(values, ln_gain, ln_bias):
    row_mean = jnp.mean(values, axis=-1, keepdims=True)
    centred = values - row_mean
    row_var = jnp.mean(jnp.square(centred), axis=-1, keepdims=True)
    return (centred * lax.rsqrt(row_var + LN_EPS) * ln_gain + ln_bias).astype(jnp.bfloat16)


def project(operand, weight):
    return jnp.dot(operand, weight, preferred_element_type=jnp.float32).astype(jnp.bfloat16)


def self_kernel(lens_ref, x_hbm, gain_hbm, bias_hbm, wq_hbm, wk_hbm, wv_hbm, wo_hbm, k_hbm, v_hbm,
                part_ref, know_ref, vnow_ref,
                x_ref, gain_ref, bias_ref, wq_buf, wk_buf, wv_buf, wo_buf, k_buf, v_buf, q_all, p_buf, acc, mx, sm, row_tab, start_tab, rem_tab,
                w_sem, k_sem, v_sem):
    batch = x_ref.shape[0]
    dim = k_buf.shape[1]
    weights = [pltpu.make_async_copy(src, dst, w_sem.at[i]) for i, (src, dst) in enumerate(
        ((x_hbm, x_ref), (gain_hbm, gain_ref), (bias_hbm, bias_ref), (wq_hbm, wq_buf), (wk_hbm, wk_buf), (wv_hbm, wv_buf),
         (wo_hbm, wo_buf)))]
    for w in weights:
        w.start()

    def build(i, carry):
        b, start, left = carry
        row_tab[i] = b
        start_tab[i] = start
        rem_tab[i] = jnp.minimum(left, CHUNK)
        more = left > CHUNK
        nb = jnp.minimum(b + 1, batch)
        fresh = jnp.where(nb < batch, lens_ref[jnp.minimum(nb, batch - 1)], 64)
        return jnp.where(more, b, nb), jnp.where(more, start + CHUNK, 0), jnp.where(more, left - CHUNK, fresh)

    def size_of(i):
        return pl.multiple_of((rem_tab[i] + 127) // 128 * 128, 128)

    def fetch(hbm, buf, sem, i, slot):
        size = size_of(i)
        b = jnp.minimum(row_tab[i], batch - 1)
        return pltpu.make_async_copy(
            hbm.at[b, :, pl.ds(pl.multiple_of(start_tab[i], CHUNK), size)], buf.at[slot, :, pl.ds(0, size)], sem.at[slot])

    def fetch_k(i, slot):
        return fetch(k_hbm, k_buf, k_sem, i, slot)

    def fetch_v(i, slot):
        return fetch(v_hbm, v_buf, v_sem, i, slot)

    def open_k(i, carry):
        carry = build(i, carry)
        fetch_k(i, i).start(priority=0)
        return carry

    carry = lax.fori_loop(0, SLOTS, open_k, (jnp.int32(0), jnp.int32(0), lens_ref[0]))
    v_buf[...] = jnp.zeros_like(v_buf)

    def open_v(i, _):
        fetch_v(i, i).start(priority=1)
        return 0

    lax.fori_loop(0, SLOTS, open_v, 0)

    def count(b, total):
        return total + (lens_ref[b] + CHUNK - 1) // CHUNK

    groups = (lax.fori_loop(0, batch, count, jnp.int32(0)) + UNROLL - 1) // UNROLL
    lax.fori_loop(SLOTS, (groups + 1) * UNROLL, build, carry)

    for w in weights[:3]:
        w.wait()
    normed = layer_norm(x_ref[...].astype(jnp.float32), gain_ref[...], bias_ref[...])
    for w in weights[3:6]:
        w.wait()
    q_new = project(normed, wq_buf[...])
    k_new = project(normed, wk_buf[...])
    v_new = project(normed, wv_buf[...])
    half = dim // 2
    for h in range(2):
        know_ref[:, h, :] = k_new[:, h * half:(h + 1) * half]
        vnow_ref[:, h, :] = v_new[:, h * half:(h + 1) * half]
    lane = lax.broadcasted_iota(jnp.int32, (batch, 8, dim), 2)
    row = lax.broadcasted_iota(jnp.int32, (batch, 8, dim), 1)
    own = (lane // half) == row
    q_f = q_new.astype(jnp.float32)
    q_wide = jnp.where(own, q_f[:, None, :], 0.0)
    q_all[:batch] = q_wide.astype(jnp.bfloat16)
    q_all[batch] = jnp.zeros((8, dim), jnp.bfloat16)
    s_new = jnp.sum(q_wide * k_new.astype(jnp.float32)[:, None, :], axis=-1, keepdims=True) * (half ** -0.5)
    mx[:batch] = jnp.broadcast_to(s_new, (batch, 8, dim))
    sm[:batch] = jnp.ones((batch, 8, dim), jnp.float32)
    acc[:batch] = jnp.broadcast_to(v_new.astype(jnp.float32)[:, None, :], (batch, 8, dim))
    mx[batch] = jnp.zeros((8, dim), jnp.float32)
    sm[batch] = jnp.ones((8, dim), jnp.float32)
    acc[batch] = jnp.zeros((8, dim), jnp.float32)

    spot = lax.broadcasted_iota(jnp.int32, (8, CHUNK), 1)
    scale = half ** -0.5

    def scores(i, slot):
        s = jnp.dot(q_all[row_tab[i]], k_buf[slot], preferred_element_type=jnp.float32) * scale
        s = jnp.where(spot < rem_tab[i], s, NEG)
        top = jnp.max(s, axis=-1, keepdims=True)
        e = jnp.exp(s - top)
        return e.astype(jnp.bfloat16), top, jnp.sum(e, axis=-1, keepdims=True)

    def weigh(p, slot):
        return lax.dot_general(p, v_buf[slot], (((1,), (1,)), ((), ())), preferred_element_type=jnp.float32)

    def merge(i, o, top, total):
        b = row_tab[i]
        old = mx[b]
        new = jnp.maximum(old, top)
        keep = jnp.exp(old - new)
        add = jnp.exp(top - new)
        mx[b] = new
        sm[b] = sm[b] * keep + total * add
        acc[b] = acc[b] * keep + o * add

    for u in range(UNROLL):
        fetch_k(u, u).wait()
    first = [scores(u, u) for u in range(UNROLL)]
    for u in range(UNROLL):
        p_buf[0, u] = first[u][0]
    for u in range(UNROLL):
        fetch_k(SLOTS + u, u).start(priority=0)
    depth = SLOTS // UNROLL

    def step(g, stats):
        prev = (g - 1) * UNROLL
        now = g * UNROLL
        slot_b = lax.rem(prev, SLOTS)
        slot_a = lax.rem(now, SLOTS)
        for u in range(UNROLL):
            fetch_k(now + u, slot_a + u).wait()
        for u in range(UNROLL):
            fetch_v(prev + u, slot_b + u).wait()
        before = lax.rem(g - 1, 2)
        after = lax.rem(g, 2)
        p_prev = [p_buf[before, u] for u in range(UNROLL)]
        out = [scores(now + u, slot_a + u) for u in range(UNROLL)]
        o_prev = [weigh(p_prev[u], slot_b + u) for u in range(UNROLL)]
        for u in range(UNROLL):
            merge(prev + u, o_prev[u], stats[2 * u], stats[2 * u + 1])
        for u in range(UNROLL):
            p_buf[after, u] = out[u][0]

        @pl.when(g + depth <= groups)
        def _():
            for u in range(UNROLL):
                fetch_k(now + SLOTS + u, slot_a + u).start(priority=0)

        @pl.when(g - 1 + depth < groups)
        def _():
            for u in range(UNROLL):
                fetch_v(prev + SLOTS + u, slot_b + u).start(priority=1)

        return tuple(x for u in range(UNROLL) for x in out[u][1:])

    lax.fori_loop(1, groups + 1, step, tuple(x for u in range(UNROLL) for x in first[u][1:]))

    lane2 = lax.broadcasted_iota(jnp.int32, (batch, dim), 1)
    o0 = acc[:batch, 0, :] / sm[:batch, 0, :]
    o1 = acc[:batch, 1, :] / sm[:batch, 1, :]
    out = jnp.where(lane2 < half, o0, o1).astype(jnp.bfloat16)
    weights[6].wait()
    part = project(out, wo_buf[...])
    for i in range(8):
        part_ref[i] = part[:, i * 128:(i + 1) * 128]


def self_attention(x, k_cache, v_cache, seq_lens, gain, bias, w_q, w_k, w_v, w_o):
    batch, ctx, heads, head_dim = k_cache.shape
    dim = heads * head_dim
    model = x.shape[1]
    most = batch * (ctx // CHUNK) + 2 * UNROLL + SLOTS
    k_t = k_cache.transpose(0, 2, 3, 1).reshape(batch, dim, ctx)
    v_t = v_cache.transpose(0, 2, 3, 1).reshape(batch, dim, ctx)
    vmem = pl.BlockSpec(memory_space=pltpu.VMEM)
    f32, bf16 = jnp.float32, jnp.bfloat16
    return pl.pallas_call(
        self_kernel,
        out_shape=(jax.ShapeDtypeStruct((8, batch, model // 8), bf16),
                   jax.ShapeDtypeStruct((batch, heads, head_dim), bf16),
                   jax.ShapeDtypeStruct((batch, heads, head_dim), bf16)),
        in_specs=[pl.BlockSpec(memory_space=pltpu.SMEM)] + [pl.BlockSpec(memory_space=pltpu.HBM)] * 9,
        out_specs=(vmem, vmem, vmem),
        scratch_shapes=[
            pltpu.VMEM((batch, model), bf16), pltpu.VMEM((1, model), f32), pltpu.VMEM((1, model), f32),
            pltpu.VMEM((model, dim), bf16), pltpu.VMEM((model, dim), bf16), pltpu.VMEM((model, dim), bf16),
            pltpu.VMEM((dim, model), bf16),
            pltpu.VMEM((SLOTS, dim, CHUNK), bf16), pltpu.VMEM((SLOTS, dim, CHUNK), bf16),
            pltpu.VMEM((batch + 1, 8, dim), bf16),
            pltpu.VMEM((2, UNROLL, 8, CHUNK), bf16),
            pltpu.VMEM((batch + 1, 8, dim), f32), pltpu.VMEM((batch + 1, 8, dim), f32), pltpu.VMEM((batch + 1, 8, dim), f32),
            pltpu.SMEM((most,), jnp.int32), pltpu.SMEM((most,), jnp.int32), pltpu.SMEM((most,), jnp.int32),
            pltpu.SemaphoreType.DMA((7,)), pltpu.SemaphoreType.DMA((SLOTS,)), pltpu.SemaphoreType.DMA((SLOTS,)),
        ],
        cost_estimate=pl.CostEstimate(flops=2 * 2 * batch * ctx * dim * 8, bytes_accessed=batch * ctx * dim * 2, transcendentals=0),
        compiler_params=pltpu.CompilerParams(vmem_limit_bytes=32 << 20),
        name="self_attention",
    )(seq_lens, x, gain.reshape(1, model), bias.reshape(1, model), w_q, w_k, w_v, w_o, k_t, v_t)


def post_kernel(part_ref, x_ref, gain2_ref, bias2_ref, gain3_ref, bias3_ref, *refs):
    (mate_ref, wk1, wk2, wk3, wv1, wv2, wv3, wqc, enc, wk0, wv0, woc, wup, wdn, out_ref,
     k_all, v_all, q_buf, o_out, o_in, p_buf, rs_buf, ag_buf, h_buf,
     q_send, q_recv, o_send, o_recv, rs_send, rs_recv, ag_send, ag_recv) = refs
    f32, bf16 = jnp.float32, jnp.bfloat16
    batch, model = x_ref.shape
    me = lax.axis_index('tp')
    my, mx, mc = me // 4, (me // 2) % 2, me % 2

    def peer(r):
        py = 1 - my if r // 4 else my
        px = 1 - mx if (r // 2) % 2 else mx
        pc = 1 - mc if r % 2 else mc
        return 4 * py + 2 * px + pc

    barrier = pltpu.get_barrier_semaphore()
    for r in FAR_FIRST:
        pl.semaphore_signal(barrier, inc=1, device_id={'tp': peer(r)}, device_id_type=MESH)

    side = 2 * HEADS_DIM
    pl.semaphore_wait(barrier, 7)

    sends = []

    def send(src, dst, send_sem, recv_sem, r):
        copy = pltpu.make_async_remote_copy(src_ref=src, dst_ref=dst, send_sem=send_sem, recv_sem=recv_sem,
                                            device_id={'tp': peer(r)}, device_id_type=MESH)
        copy.start()
        sends.append(copy)
        return copy

    def scatter(n, parts):
        return [send(parts.at[peer(r)], rs_buf.at[n, r], rs_send.at[n, r], rs_recv.at[n, r], r) for r in FAR_FIRST]

    def collect(n, mine, copies):
        for copy in copies:
            copy.wait_recv()
        total = mine.astype(f32)
        for r in range(1, 8):
            total = total + rs_buf[n, r].astype(f32)
        return total.astype(bf16)

    def gather(n, mine):
        ag_buf[n, me] = mine
        return [send(ag_buf.at[n, me], ag_buf.at[n, me], ag_send.at[n, r], ag_recv.at[n, r], r) for r in FAR_FIRST]

    def whole(n, copies):
        for copy in copies:
            copy.wait_recv()
        return jnp.concatenate([ag_buf[n, i] for i in range(8)], axis=1)

    rows = PROJ_ROWS
    per = rows // enc.shape[1]

    tokens = enc.shape[1]

    def project_tokens(source, half, weights, dest):
        def body(i, _):
            lines = source[pl.ds(i * per, per)].reshape(rows, model)
            weight = jnp.concatenate([w[...] for w in weights], axis=1)
            got = project(lines, weight).reshape(per, tokens, 4 * side)
            dest[pl.ds(i * per, per), half * tokens:(half + 1) * tokens, :] = got
            return 0
        lax.fori_loop(0, batch // per, body, 0)

    rs = scatter(0, part_ref)
    wks, wvs = (wk0, wk1, wk2, wk3), (wv0, wv1, wv2, wv3)
    project_tokens(enc, 0, wks, k_all)
    summed = collect(0, part_ref[me], rs)
    ag = gather(0, summed)
    project_tokens(mate_ref, 1, wks, k_all)
    hidden = x_ref[...].astype(f32) + whole(0, ag).astype(f32)
    normed = layer_norm(hidden, gain2_ref[...], bias2_ref[...])
    q_buf[0] = project(normed, wqc[...])
    qs = [send(q_buf.at[0], q_buf.at[k], q_send.at[k], q_recv.at[k], 2 * k) for k in (3, 2, 1)]
    project_tokens(enc, 0, wvs, v_all)
    project_tokens(mate_ref, 1, wvs, v_all)
    for copy in qs:
        copy.wait_recv()
    q_eight = jnp.concatenate([q_buf[k] for k in range(4)], axis=1).astype(f32)
    wide = q_eight.shape[1]
    own = (lax.broadcasted_iota(jnp.int32, (8, wide), 1) // HEADS_DIM) == lax.broadcasted_iota(jnp.int32, (8, wide), 0)
    nt = (((1,), (1,)), ((), ()))
    scale = HEADS_DIM ** -0.5
    outs, tops, sums = [], [], []
    for b in range(batch):
        q_b = jnp.where(own, q_eight[b:b + 1, :], 0.0).astype(bf16)
        s = lax.dot_general(q_b, k_all[b], nt, preferred_element_type=f32) * scale
        top = jnp.max(s, axis=-1, keepdims=True)
        e = jnp.exp(s - top)
        o = jnp.dot(e.astype(bf16), v_all[b], preferred_element_type=f32)
        outs.append(jnp.sum(jnp.where(own, o, 0.0), axis=0, keepdims=True))
        tops.append(top)
        sums.append(jnp.sum(e, axis=-1, keepdims=True))
    lane = lax.broadcasted_iota(jnp.int32, (8, side), 1)
    line = lax.broadcasted_iota(jnp.int32, (8, side), 0)
    for b in range(batch):
        stat = jnp.where(lane % HEADS_DIM < HEADS_DIM // 2, tops[b], sums[b])
        for k in range(4):
            o_out[k, b:b + 1, :] = outs[b][:, k * side:(k + 1) * side]
            o_out[k, batch + b:batch + b + 1, :] = jnp.sum(jnp.where(line == 2 * k + lane // HEADS_DIM, stat, 0.0), axis=0, keepdims=True)
    os = [send(o_out.at[k], o_in.at[k], o_send.at[k], o_recv.at[k], 2 * k) for k in (3, 2, 1)]
    for copy in os:
        copy.wait_recv()
    low = lax.broadcasted_iota(jnp.int32, (batch, side), 1) < HEADS_DIM
    third = HEADS_DIM // 2

    def spread(stat, at):
        return jnp.where(low, stat[:, at:at + 1], stat[:, HEADS_DIM + at:HEADS_DIM + at + 1])

    pieces = [o_out[0]] + [o_in[k] for k in range(1, 4)]
    top_of = [spread(p[batch:], 0) for p in pieces]
    sum_of = [spread(p[batch:], third) for p in pieces]
    top = functools.reduce(jnp.maximum, top_of)
    shares = [jnp.exp(t - top) for t in top_of]
    denom = sum(s * w for s, w in zip(sum_of, shares))
    numer = sum(p[:batch] * w for p, w in zip(pieces, shares))
    cross = (numer / denom).astype(bf16)
    part2 = project(cross, woc[...])
    for i in range(8):
        p_buf[0, i] = part2[:, i * 128:(i + 1) * 128]
    rs = scatter(1, p_buf.at[0])
    summed = collect(1, p_buf[0, me], rs)
    ag = gather(1, summed)
    hidden = hidden + whole(1, ag).astype(f32)
    normed = layer_norm(hidden, gain3_ref[...], bias3_ref[...])
    for i in range(8):
        h_buf[i] = hidden[:, i * 128:(i + 1) * 128]
    up = jnp.dot(normed, wup[...], preferred_element_type=f32)
    up = (0.5 * up * (1.0 + lax.erf(up * (2.0 ** -0.5)))).astype(bf16)
    part3 = project(up, wdn[...])
    for i in range(8):
        p_buf[1, i] = part3[:, i * 128:(i + 1) * 128]
    rs = scatter(2, p_buf.at[1])
    summed = collect(2, p_buf[1, me], rs)
    ag = gather(2, (h_buf[me] + summed.astype(f32)).astype(bf16))
    out_ref[...] = whole(2, ag)
    for copy in sends:
        copy.wait_send()


def post_attention(part, x, gain2, bias2, gain3, bias3, own, mate, wks, wvs, wq_c, wo_c, w_up, w_down):
    batch, model = x.shape
    f32, bf16 = jnp.float32, jnp.bfloat16
    vmem = pl.BlockSpec(memory_space=pltpu.VMEM)
    tokens = own.shape[1]
    side = wq_c.shape[1]
    dma = pltpu.SemaphoreType.DMA
    return pl.pallas_call(
        post_kernel,
        out_shape=jax.ShapeDtypeStruct((batch, model), bf16),
        in_specs=[vmem] * 20,
        out_specs=vmem,
        scratch_shapes=[
            pltpu.VMEM((batch, 2 * tokens, 4 * side), bf16), pltpu.VMEM((batch, 2 * tokens, 4 * side), bf16),
            pltpu.VMEM((4, batch, side), bf16), pltpu.VMEM((4, 2 * batch, side), f32), pltpu.VMEM((4, 2 * batch, side), f32),
            pltpu.VMEM((2, 8, batch, 128), bf16), pltpu.VMEM((3, 8, batch, 128), bf16), pltpu.VMEM((3, 8, batch, 128), bf16),
            pltpu.VMEM((8, batch, 128), f32),
            dma((4,)), dma((4,)), dma((4,)), dma((4,)), dma((3, 8)), dma((3, 8)), dma((3, 8)), dma((3, 8)),
        ],
        compiler_params=pltpu.CompilerParams(collective_id=0, has_side_effects=True, vmem_limit_bytes=24 << 20),
        cost_estimate=pl.CostEstimate(flops=2 * batch * 2 * tokens * model * 8 * side, bytes_accessed=9 << 20, transcendentals=0),
        name="post_attention",
    )(part, x, gain2.reshape(1, model), bias2.reshape(1, model), gain3.reshape(1, model), bias3.reshape(1, model),
      mate, *wks[1:], *wvs[1:], wq_c, own, wks[0], wvs[0], wo_c, w_up, w_down)


def local_step(x, k_cache, v_cache, seq_lens, nbr_enc, ln1_gain, ln1_bias, w_q, w_k, w_v, w_o, ln2_gain, ln2_bias, wq_c, wk_c, wv_c, wo_c, ln3_gain, ln3_bias, w_up, w_down):
    def swap(value, r):
        return lax.ppermute(value, 'tp', [(t, t ^ r) for t in range(8)])

    mate = swap(nbr_enc, 1)
    wks = [wk_c] + [swap(wk_c, 2 * k) for k in (1, 2, 3)]
    wvs = [wv_c] + [swap(wv_c, 2 * k) for k in (1, 2, 3)]
    part, k_new, v_new = self_attention(x, k_cache, v_cache, seq_lens, ln1_gain, ln1_bias, w_q, w_k, w_v, w_o)
    out = post_attention(part, x, ln2_gain, ln2_bias, ln3_gain, ln3_bias, nbr_enc, mate, wks, wvs, wq_c, wo_c, w_up, w_down)
    return out, k_new, v_new


def solution(mesh):
    row_spec = P('dp', None)
    cache_spec = P('dp', None, 'tp', None)
    head_spec = P('dp', 'tp', None)
    vec_spec = P(None)
    col_split = P(None, 'tp')
    row_split = P('tp', None)
    in_specs = (row_spec, cache_spec, cache_spec, P('dp'), P('dp', 'tp', None), vec_spec, vec_spec, col_split, col_split, col_split, row_split, vec_spec, vec_spec, col_split, col_split, col_split, row_split, vec_spec, vec_spec, col_split, row_split)
    out_specs = (row_spec, head_spec, head_spec)
    return jax.shard_map(local_step, mesh=mesh, in_specs=in_specs, out_specs=out_specs, check_vma=False)
```

```python
import functools

import jax
import jax.numpy as jnp
from jax import lax
from jax.experimental import pallas as pl
from jax.experimental.pallas import tpu as pltpu
from jax.sharding import PartitionSpec as P

LN_EPS = 1e-5
CHUNK = 2048
SLOTS = 12
UNROLL = 1
NEG = -1e30
HEADS_DIM = 64
PROJ_ROWS = 256
MESH = pl.DeviceIdType.MESH


def layer_norm(values, ln_gain, ln_bias):
    row_mean = jnp.mean(values, axis=-1, keepdims=True)
    centred = values - row_mean
    row_var = jnp.mean(jnp.square(centred), axis=-1, keepdims=True)
    return (centred * lax.rsqrt(row_var + LN_EPS) * ln_gain + ln_bias).astype(jnp.bfloat16)


def project(operand, weight):
    return jnp.dot(operand, weight, preferred_element_type=jnp.float32).astype(jnp.bfloat16)


def self_kernel(lens_ref, x_hbm, gain_hbm, bias_hbm, wq_hbm, wk_hbm, wv_hbm, wo_hbm, k_hbm, v_hbm,
                part_ref, know_ref, vnow_ref,
                x_ref, gain_ref, bias_ref, wq_buf, wk_buf, wv_buf, wo_buf, k_buf, v_buf, q_all, p_buf, acc, mx, sm, row_tab, start_tab, rem_tab,
                w_sem, k_sem, v_sem):
    batch = x_ref.shape[0]
    dim = k_buf.shape[1]
    weights = [pltpu.make_async_copy(src, dst, w_sem.at[i]) for i, (src, dst) in enumerate(
        ((x_hbm, x_ref), (gain_hbm, gain_ref), (bias_hbm, bias_ref), (wq_hbm, wq_buf), (wk_hbm, wk_buf), (wv_hbm, wv_buf),
         (wo_hbm, wo_buf)))]
    for w in weights:
        w.start()

    def build(i, carry):
        b, start, left = carry
        row_tab[i] = b
        start_tab[i] = start
        rem_tab[i] = jnp.minimum(left, CHUNK)
        more = left > CHUNK
        nb = jnp.minimum(b + 1, batch)
        fresh = jnp.where(nb < batch, lens_ref[jnp.minimum(nb, batch - 1)], 64)
        return jnp.where(more, b, nb), jnp.where(more, start + CHUNK, 0), jnp.where(more, left - CHUNK, fresh)

    def size_of(i):
        return pl.multiple_of((rem_tab[i] + 127) // 128 * 128, 128)

    def fetch(hbm, buf, sem, i, slot):
        size = size_of(i)
        b = jnp.minimum(row_tab[i], batch - 1)
        return pltpu.make_async_copy(
            hbm.at[b, :, pl.ds(pl.multiple_of(start_tab[i], CHUNK), size)], buf.at[slot, :, pl.ds(0, size)], sem.at[slot])

    def fetch_k(i, slot):
        return fetch(k_hbm, k_buf, k_sem, i, slot)

    def fetch_v(i, slot):
        return fetch(v_hbm, v_buf, v_sem, i, slot)

    def open_k(i, carry):
        carry = build(i, carry)
        fetch_k(i, i).start(priority=0)
        return carry

    carry = lax.fori_loop(0, SLOTS, open_k, (jnp.int32(0), jnp.int32(0), lens_ref[0]))
    v_buf[...] = jnp.zeros_like(v_buf)

    def open_v(i, _):
        fetch_v(i, i).start(priority=1)
        return 0

    lax.fori_loop(0, SLOTS, open_v, 0)

    def count(b, total):
        return total + (lens_ref[b] + CHUNK - 1) // CHUNK

    groups = (lax.fori_loop(0, batch, count, jnp.int32(0)) + UNROLL - 1) // UNROLL
    lax.fori_loop(SLOTS, (groups + 1) * UNROLL, build, carry)

    for w in weights[:3]:
        w.wait()
    normed = layer_norm(x_ref[...].astype(jnp.float32), gain_ref[...], bias_ref[...])
    for w in weights[3:6]:
        w.wait()
    q_new = project(normed, wq_buf[...])
    k_new = project(normed, wk_buf[...])
    v_new = project(normed, wv_buf[...])
    half = dim // 2
    for h in range(2):
        know_ref[:, h, :] = k_new[:, h * half:(h + 1) * half]
        vnow_ref[:, h, :] = v_new[:, h * half:(h + 1) * half]
    lane = lax.broadcasted_iota(jnp.int32, (batch, 8, dim), 2)
    row = lax.broadcasted_iota(jnp.int32, (batch, 8, dim), 1)
    own = (lane // half) == row
    q_f = q_new.astype(jnp.float32)
    q_wide = jnp.where(own, q_f[:, None, :], 0.0)
    q_all[:batch] = q_wide.astype(jnp.bfloat16)
    q_all[batch] = jnp.zeros((8, dim), jnp.bfloat16)
    s_new = jnp.sum(q_wide * k_new.astype(jnp.float32)[:, None, :], axis=-1, keepdims=True) * (half ** -0.5)
    mx[:batch] = jnp.broadcast_to(s_new, (batch, 8, dim))
    sm[:batch] = jnp.ones((batch, 8, dim), jnp.float32)
    acc[:batch] = jnp.broadcast_to(v_new.astype(jnp.float32)[:, None, :], (batch, 8, dim))
    mx[batch] = jnp.zeros((8, dim), jnp.float32)
    sm[batch] = jnp.ones((8, dim), jnp.float32)
    acc[batch] = jnp.zeros((8, dim), jnp.float32)

    spot = lax.broadcasted_iota(jnp.int32, (8, CHUNK), 1)
    scale = half ** -0.5

    def scores(i, slot):
        s = jnp.dot(q_all[row_tab[i]], k_buf[slot], preferred_element_type=jnp.float32) * scale
        s = jnp.where(spot < rem_tab[i], s, NEG)
        top = jnp.max(s, axis=-1, keepdims=True)
        e = jnp.exp(s - top)
        return e.astype(jnp.bfloat16), top, jnp.sum(e, axis=-1, keepdims=True)

    def weigh(p, slot):
        return lax.dot_general(p, v_buf[slot], (((1,), (1,)), ((), ())), preferred_element_type=jnp.float32)

    def merge(i, o, top, total):
        b = row_tab[i]
        old = mx[b]
        new = jnp.maximum(old, top)
        keep = jnp.exp(old - new)
        add = jnp.exp(top - new)
        mx[b] = new
        sm[b] = sm[b] * keep + total * add
        acc[b] = acc[b] * keep + o * add

    for u in range(UNROLL):
        fetch_k(u, u).wait()
    first = [scores(u, u) for u in range(UNROLL)]
    for u in range(UNROLL):
        p_buf[0, u] = first[u][0]
    for u in range(UNROLL):
        fetch_k(SLOTS + u, u).start(priority=0)
    depth = SLOTS // UNROLL

    def step(g, stats):
        prev = (g - 1) * UNROLL
        now = g * UNROLL
        slot_b = lax.rem(prev, SLOTS)
        slot_a = lax.rem(now, SLOTS)
        for u in range(UNROLL):
            fetch_k(now + u, slot_a + u).wait()
        for u in range(UNROLL):
            fetch_v(prev + u, slot_b + u).wait()
        before = lax.rem(g - 1, 2)
        after = lax.rem(g, 2)
        p_prev = [p_buf[before, u] for u in range(UNROLL)]
        out = [scores(now + u, slot_a + u) for u in range(UNROLL)]
        o_prev = [weigh(p_prev[u], slot_b + u) for u in range(UNROLL)]
        for u in range(UNROLL):
            merge(prev + u, o_prev[u], stats[2 * u], stats[2 * u + 1])
        for u in range(UNROLL):
            p_buf[after, u] = out[u][0]

        @pl.when(g + depth <= groups)
        def _():
            for u in range(UNROLL):
                fetch_k(now + SLOTS + u, slot_a + u).start(priority=0)

        @pl.when(g - 1 + depth < groups)
        def _():
            for u in range(UNROLL):
                fetch_v(prev + SLOTS + u, slot_b + u).start(priority=1)

        return tuple(x for u in range(UNROLL) for x in out[u][1:])

    lax.fori_loop(1, groups + 1, step, tuple(x for u in range(UNROLL) for x in first[u][1:]))

    lane2 = lax.broadcasted_iota(jnp.int32, (batch, dim), 1)
    o0 = acc[:batch, 0, :] / sm[:batch, 0, :]
    o1 = acc[:batch, 1, :] / sm[:batch, 1, :]
    out = jnp.where(lane2 < half, o0, o1).astype(jnp.bfloat16)
    weights[6].wait()
    part = project(out, wo_buf[...])
    cut = part_ref.shape[2]
    for i in range(2):
        part_ref[i] = part[:, i * cut:(i + 1) * cut]


def self_attention(x, k_cache, v_cache, seq_lens, gain, bias, w_q, w_k, w_v, w_o):
    batch, ctx, heads, head_dim = k_cache.shape
    dim = heads * head_dim
    model = x.shape[1]
    most = batch * (ctx // CHUNK) + 2 * UNROLL + SLOTS
    k_t = k_cache.transpose(0, 2, 3, 1).reshape(batch, dim, ctx)
    v_t = v_cache.transpose(0, 2, 3, 1).reshape(batch, dim, ctx)
    vmem = pl.BlockSpec(memory_space=pltpu.VMEM)
    f32, bf16 = jnp.float32, jnp.bfloat16
    return pl.pallas_call(
        self_kernel,
        out_shape=(jax.ShapeDtypeStruct((2, batch, model // 2), bf16),
                   jax.ShapeDtypeStruct((batch, heads, head_dim), bf16),
                   jax.ShapeDtypeStruct((batch, heads, head_dim), bf16)),
        in_specs=[pl.BlockSpec(memory_space=pltpu.SMEM)] + [pl.BlockSpec(memory_space=pltpu.HBM)] * 9,
        out_specs=(vmem, vmem, vmem),
        scratch_shapes=[
            pltpu.VMEM((batch, model), bf16), pltpu.VMEM((1, model), f32), pltpu.VMEM((1, model), f32),
            pltpu.VMEM((model, dim), bf16), pltpu.VMEM((model, dim), bf16), pltpu.VMEM((model, dim), bf16),
            pltpu.VMEM((dim, model), bf16),
            pltpu.VMEM((SLOTS, dim, CHUNK), bf16), pltpu.VMEM((SLOTS, dim, CHUNK), bf16),
            pltpu.VMEM((batch + 1, 8, dim), bf16),
            pltpu.VMEM((2, UNROLL, 8, CHUNK), bf16),
            pltpu.VMEM((batch + 1, 8, dim), f32), pltpu.VMEM((batch + 1, 8, dim), f32), pltpu.VMEM((batch + 1, 8, dim), f32),
            pltpu.SMEM((most,), jnp.int32), pltpu.SMEM((most,), jnp.int32), pltpu.SMEM((most,), jnp.int32),
            pltpu.SemaphoreType.DMA((7,)), pltpu.SemaphoreType.DMA((SLOTS,)), pltpu.SemaphoreType.DMA((SLOTS,)),
        ],
        cost_estimate=pl.CostEstimate(flops=2 * 2 * batch * ctx * dim * 8, bytes_accessed=batch * ctx * dim * 2, transcendentals=0),
        compiler_params=pltpu.CompilerParams(vmem_limit_bytes=32 << 20),
        name="self_attention",
    )(seq_lens, *[pltpu.with_memory_space_constraint(v, pltpu.HBM)
                  for v in (x, gain.reshape(1, model), bias.reshape(1, model), w_q, w_k, w_v, w_o, k_t, v_t)])


def post_kernel(part_ref, x_ref, gain2_ref, bias2_ref, gain3_ref, bias3_ref, enc, w0, w1, w2, w3, woc, wup, wdn, out_ref,
                mate_ref, k_all, v_all, o_out, o_in, p_buf, a_buf, b_buf, c_buf,
                e_sem, a_send, a_recv, b_send, b_recv, c_send, c_recv, o_send, o_recv):
    f32, bf16 = jnp.float32, jnp.bfloat16
    batch, model = x_ref.shape
    half = model // 2
    me = lax.axis_index('tp')
    chip, core = me // 2, me % 2
    chip_y, chip_x = chip // 2, chip % 2
    mate = 2 * chip + 1 - core

    def other(k):
        return 2 * (2 * (1 - chip_y if k // 2 else chip_y) + (1 - chip_x if k % 2 else chip_x)) + core

    barrier = pltpu.get_barrier_semaphore()
    for device in (other(3), other(2), other(1), mate):
        pl.semaphore_signal(barrier, inc=1, device_id={'tp': device}, device_id_type=MESH)
    pl.semaphore_wait(barrier, 4)

    sends = []

    def send(src, dst, send_sem, recv_sem, device):
        copy = pltpu.make_async_remote_copy(src_ref=src, dst_ref=dst, send_sem=send_sem, recv_sem=recv_sem,
                                            device_id={'tp': device}, device_id_type=MESH)
        copy.start()
        sends.append(copy)
        return copy

    def swap_halves(n, parts):
        return send(parts.at[1 - core], a_buf.at[n], a_send.at[n], a_recv.at[n], mate)

    def share(n, mine, copy):
        copy.wait_recv()
        b_buf[n, chip] = (mine.astype(f32) + a_buf[n].astype(f32)).astype(bf16)
        return [send(b_buf.at[n, chip], b_buf.at[n, chip], b_send.at[n, k], b_recv.at[n, k], other(k)) for k in (3, 2, 1)]

    def finish(n, copies):
        for copy in copies:
            copy.wait_recv()
        total = b_buf[n, 0].astype(f32)
        for i in range(1, 4):
            total = total + b_buf[n, i].astype(f32)
        c_buf[n, core] = total.astype(bf16)
        return send(c_buf.at[n, core], c_buf.at[n, core], c_send.at[n], c_recv.at[n], mate)

    def whole(n, copy):
        copy.wait_recv()
        return jnp.concatenate([c_buf[n, 0], c_buf[n, 1]], axis=1).astype(f32)

    tokens = enc.shape[1]
    rows = PROJ_ROWS
    per = rows // tokens
    side = 2 * HEADS_DIM
    wide = 4 * side

    def weight(i):
        return jnp.concatenate([w[:, i * side:(i + 1) * side] for w in (w0, w1, w2, w3)], axis=1)

    def project_tokens(source, place, i, dest):
        def body(j, _):
            lines = source[pl.ds(j * per, per)].reshape(rows, model)
            got = project(lines, weight(i)).reshape(per, tokens, wide)
            dest[pl.ds(j * per, per), place * tokens:(place + 1) * tokens, :] = got
            return 0
        lax.fori_loop(0, batch // per, body, 0)

    a = swap_halves(0, part_ref)
    e = send(enc, mate_ref, e_sem.at[0], e_sem.at[1], mate)
    b = share(0, part_ref[core], a)
    project_tokens(enc, 0, 0, k_all)
    project_tokens(enc, 0, 1, v_all)
    e.wait_recv()
    project_tokens(mate_ref, 1, 0, k_all)
    c = finish(0, b)
    project_tokens(mate_ref, 1, 1, v_all)
    hidden = x_ref[...].astype(f32) + whole(0, c)
    normed = layer_norm(hidden, gain2_ref[...], bias2_ref[...])
    q_eight = project(normed, weight(2)).astype(f32)
    own = (lax.broadcasted_iota(jnp.int32, (8, wide), 1) // HEADS_DIM) == lax.broadcasted_iota(jnp.int32, (8, wide), 0)
    nt = (((1,), (1,)), ((), ()))
    scale = HEADS_DIM ** -0.5
    outs, tops, sums = [], [], []
    for b in range(batch):
        q_b = jnp.where(own, q_eight[b:b + 1, :], 0.0).astype(bf16)
        s = lax.dot_general(q_b, k_all[b], nt, preferred_element_type=f32) * scale
        top = jnp.max(s, axis=-1, keepdims=True)
        e = jnp.exp(s - top)
        o = jnp.dot(e.astype(bf16), v_all[b], preferred_element_type=f32)
        outs.append(jnp.sum(jnp.where(own, o, 0.0), axis=0, keepdims=True))
        tops.append(top)
        sums.append(jnp.sum(e, axis=-1, keepdims=True))
    lane = lax.broadcasted_iota(jnp.int32, (8, side), 1)
    line = lax.broadcasted_iota(jnp.int32, (8, side), 0)
    for b in range(batch):
        stat = jnp.where(lane % HEADS_DIM < HEADS_DIM // 2, tops[b], sums[b])
        for k in range(4):
            o_out[k, b:b + 1, :] = outs[b][:, k * side:(k + 1) * side]
            o_out[k, batch + b:batch + b + 1, :] = jnp.sum(jnp.where(line == 2 * k + lane // HEADS_DIM, stat, 0.0), axis=0, keepdims=True)
    os = [send(o_out.at[k], o_in.at[k], o_send.at[k], o_recv.at[k], other(k)) for k in (3, 2, 1)]
    for copy in os:
        copy.wait_recv()
    low = lax.broadcasted_iota(jnp.int32, (batch, side), 1) < HEADS_DIM
    middle = HEADS_DIM // 2

    def spread(stat, at):
        return jnp.where(low, stat[:, at:at + 1], stat[:, HEADS_DIM + at:HEADS_DIM + at + 1])

    pieces = [o_out[0]] + [o_in[k] for k in range(1, 4)]
    top_of = [spread(p[batch:], 0) for p in pieces]
    sum_of = [spread(p[batch:], middle) for p in pieces]
    top = functools.reduce(jnp.maximum, top_of)
    shares = [jnp.exp(t - top) for t in top_of]
    denom = sum(s * w for s, w in zip(sum_of, shares))
    numer = sum(p[:batch] * w for p, w in zip(pieces, shares))
    cross = (numer / denom).astype(bf16)
    part2 = project(cross, woc[...])
    for i in range(2):
        p_buf[0, i] = part2[:, i * half:(i + 1) * half]
    a = swap_halves(1, p_buf.at[0])
    c = finish(1, share(1, p_buf[0, core], a))
    hidden = hidden + whole(1, c)
    normed = layer_norm(hidden, gain3_ref[...], bias3_ref[...])
    up = jnp.dot(normed, wup[...], preferred_element_type=f32)
    up = (0.5 * up * (1.0 + lax.erf(up * (2.0 ** -0.5)))).astype(bf16)
    part3 = project(up, wdn[...])
    for i in range(2):
        p_buf[1, i] = part3[:, i * half:(i + 1) * half]
    a = swap_halves(2, p_buf.at[1])
    c = finish(2, share(2, p_buf[1, core], a))
    out_ref[...] = (hidden + whole(2, c)).astype(bf16)
    for copy in sends:
        copy.wait_send()


def post_attention(part, x, gain2, bias2, gain3, bias3, enc, weights, wo_c, w_up, w_down):
    batch, model = x.shape
    f32, bf16 = jnp.float32, jnp.bfloat16
    vmem = pl.BlockSpec(memory_space=pltpu.VMEM)
    tokens = enc.shape[1]
    side = 2 * HEADS_DIM
    dma = pltpu.SemaphoreType.DMA
    return pl.pallas_call(
        post_kernel,
        out_shape=jax.ShapeDtypeStruct((batch, model), bf16),
        in_specs=[vmem] * 14,
        out_specs=vmem,
        scratch_shapes=[
            pltpu.VMEM((batch, tokens, model), bf16),
            pltpu.VMEM((batch, 2 * tokens, 4 * side), bf16), pltpu.VMEM((batch, 2 * tokens, 4 * side), bf16),
            pltpu.VMEM((4, 2 * batch, side), f32), pltpu.VMEM((4, 2 * batch, side), f32),
            pltpu.VMEM((2, 2, batch, model // 2), bf16), pltpu.VMEM((3, batch, model // 2), bf16),
            pltpu.VMEM((3, 4, batch, model // 2), bf16), pltpu.VMEM((3, 2, batch, model // 2), bf16),
            dma((2,)), dma((3,)), dma((3,)), dma((3, 4)), dma((3, 4)), dma((3,)), dma((3,)), dma((4,)), dma((4,)),
        ],
        compiler_params=pltpu.CompilerParams(collective_id=0, has_side_effects=True, vmem_limit_bytes=24 << 20),
        cost_estimate=pl.CostEstimate(flops=2 * batch * 2 * tokens * model * 8 * side, bytes_accessed=9 << 20, transcendentals=0),
        name="post_attention",
    )(part, x, gain2.reshape(1, model), bias2.reshape(1, model), gain3.reshape(1, model), bias3.reshape(1, model),
      enc, *weights, wo_c, w_up, w_down)


def local_step(x, k_cache, v_cache, seq_lens, nbr_enc, ln1_gain, ln1_bias, w_q, w_k, w_v, w_o, ln2_gain, ln2_bias, wq_c, wk_c, wv_c, wo_c, ln3_gain, ln3_bias, w_up, w_down):
    mine = jnp.concatenate([wk_c, wv_c, wq_c], axis=1)
    weights = [mine] + [lax.ppermute(mine, 'tp', [(t, t ^ (2 * k)) for t in range(8)]) for k in (1, 2, 3)]
    part, k_new, v_new = self_attention(x, k_cache, v_cache, seq_lens, ln1_gain, ln1_bias, w_q, w_k, w_v, w_o)
    out = post_attention(part, x, ln2_gain, ln2_bias, ln3_gain, ln3_bias, nbr_enc, weights, wo_c, w_up, w_down)
    return out, k_new, v_new


def solution(mesh):
    row_spec = P('dp', None)
    cache_spec = P('dp', None, 'tp', None)
    head_spec = P('dp', 'tp', None)
    vec_spec = P(None)
    col_split = P(None, 'tp')
    row_split = P('tp', None)
    in_specs = (row_spec, cache_spec, cache_spec, P('dp'), P('dp', 'tp', None), vec_spec, vec_spec, col_split, col_split, col_split, row_split, vec_spec, vec_spec, col_split, col_split, col_split, row_split, vec_spec, vec_spec, col_split, row_split)
    out_specs = (row_spec, head_spec, head_spec)
    return jax.shard_map(local_step, mesh=mesh, in_specs=in_specs, out_specs=out_specs, check_vma=False)
```

```python
import functools

import jax
import jax.numpy as jnp
from jax import lax
from jax.experimental import pallas as pl
from jax.experimental.pallas import tpu as pltpu
from jax.sharding import PartitionSpec as P

LN_EPS = 1e-5
CHUNK = 2048
SLOTS = 5
NEG = -1e30
HEADS_DIM = 64
PROJ_ROWS = 256
MESH = pl.DeviceIdType.MESH


def layer_norm(values, ln_gain, ln_bias):
    row_mean = jnp.mean(values, axis=-1, keepdims=True)
    centred = values - row_mean
    row_var = jnp.mean(jnp.square(centred), axis=-1, keepdims=True)
    return (centred * lax.rsqrt(row_var + LN_EPS) * ln_gain + ln_bias).astype(jnp.bfloat16)


def project(operand, weight):
    return jnp.dot(operand, weight, preferred_element_type=jnp.float32).astype(jnp.bfloat16)


def self_kernel(lens_ref, x_hbm, gain_hbm, bias_hbm, wq_hbm, wk_hbm, wv_hbm, wo_hbm, k_hbm, v_hbm,
                part_ref, know_ref, vnow_ref,
                x_ref, gain_ref, bias_ref, wq_buf, wk_buf, wv_buf, wo_buf, k_buf, v_buf, q_all, p_buf, acc, mx, sm, row_tab, off_tab,
                w_sem, k_sem, v_sem):
    batch = x_ref.shape[0]
    dim = k_buf.shape[1]
    weights = [pltpu.make_async_copy(src, dst, w_sem.at[i]) for i, (src, dst) in enumerate(
        ((x_hbm, x_ref), (gain_hbm, gain_ref), (bias_hbm, bias_ref), (wq_hbm, wq_buf), (wk_hbm, wk_buf), (wv_hbm, wv_buf),
         (wo_hbm, wo_buf)))]
    for w in weights:
        w.start()

    def fetch(hbm, buf, sem, b):
        size = pl.multiple_of((lens_ref[b] + 127) // 128 * 128, 128)
        slot = lax.rem(b, SLOTS)
        return pltpu.make_async_copy(hbm.at[b, :, pl.ds(0, size)], buf.at[slot, :, pl.ds(0, size)], sem.at[slot])

    def fetch_k(b):
        return fetch(k_hbm, k_buf, k_sem, b)

    def fetch_v(b):
        return fetch(v_hbm, v_buf, v_sem, b)

    for b in range(SLOTS):
        fetch_k(b).start(priority=0)
    v_buf[...] = jnp.zeros_like(v_buf)
    for b in range(SLOTS):
        fetch_v(b).start(priority=1)

    def build_row(b, at):
        def build(j, at):
            row_tab[at] = b
            off_tab[at] = j * CHUNK
            return at + 1
        return lax.fori_loop(0, (lens_ref[b] + CHUNK - 1) // CHUNK, build, at)

    items = lax.fori_loop(0, batch, build_row, jnp.int32(0))
    row_tab[items] = batch
    off_tab[items] = 0

    for w in weights[:3]:
        w.wait()
    normed = layer_norm(x_ref[...].astype(jnp.float32), gain_ref[...], bias_ref[...])
    for w in weights[3:6]:
        w.wait()
    q_new = project(normed, wq_buf[...])
    k_new = project(normed, wk_buf[...])
    v_new = project(normed, wv_buf[...])
    half = dim // 2
    for h in range(2):
        know_ref[:, h, :] = k_new[:, h * half:(h + 1) * half]
        vnow_ref[:, h, :] = v_new[:, h * half:(h + 1) * half]
    lane = lax.broadcasted_iota(jnp.int32, (batch, 8, dim), 2)
    row = lax.broadcasted_iota(jnp.int32, (batch, 8, dim), 1)
    own = (lane // half) == row
    q_f = q_new.astype(jnp.float32)
    q_wide = jnp.where(own, q_f[:, None, :], 0.0)
    q_all[:batch] = q_wide.astype(jnp.bfloat16)
    q_all[batch] = jnp.zeros((8, dim), jnp.bfloat16)
    s_new = jnp.sum(q_wide * k_new.astype(jnp.float32)[:, None, :], axis=-1, keepdims=True) * (half ** -0.5)
    mx[:batch] = jnp.broadcast_to(s_new, (batch, 8, dim))
    sm[:batch] = jnp.ones((batch, 8, dim), jnp.float32)
    acc[:batch] = jnp.broadcast_to(v_new.astype(jnp.float32)[:, None, :], (batch, 8, dim))
    mx[batch] = jnp.zeros((8, dim), jnp.float32)
    sm[batch] = jnp.ones((8, dim), jnp.float32)
    acc[batch] = jnp.zeros((8, dim), jnp.float32)

    spot = lax.broadcasted_iota(jnp.int32, (8, CHUNK), 1)
    scale = half ** -0.5

    def chunk(buf, i):
        return buf.at[lax.rem(row_tab[i], SLOTS), :, pl.ds(pl.multiple_of(off_tab[i], CHUNK), CHUNK)]

    def scores(i):
        b = row_tab[i]
        s = jnp.dot(q_all[b], chunk(k_buf, i)[...], preferred_element_type=jnp.float32) * scale
        s = jnp.where(spot < lens_ref[jnp.minimum(b, batch - 1)] - off_tab[i], s, NEG)
        top = jnp.max(s, axis=-1, keepdims=True)
        e = jnp.exp(s - top)
        return e.astype(jnp.bfloat16), top, jnp.sum(e, axis=-1, keepdims=True)

    def merge(i, o, top, total):
        b = row_tab[i]
        old = mx[b]
        new = jnp.maximum(old, top)
        keep = jnp.exp(old - new)
        add = jnp.exp(top - new)
        mx[b] = new
        sm[b] = sm[b] * keep + total * add
        acc[b] = acc[b] * keep + o * add

    def await_first(copy, i):
        @pl.when((off_tab[i] == 0) & (row_tab[i] < batch))
        def _():
            copy(row_tab[i]).wait()

    def refill_after(copy, i):
        @pl.when((off_tab[i + 1] == 0) & (row_tab[i] + SLOTS < batch))
        def _():
            copy(row_tab[i] + SLOTS).start(priority=0 if copy is fetch_k else 1)

    await_first(fetch_k, 0)
    p, top, total = scores(0)
    p_buf[0] = p
    refill_after(fetch_k, 0)

    def step(g, stats):
        await_first(fetch_k, g)
        await_first(fetch_v, g - 1)
        p_prev = p_buf[lax.rem(g - 1, 2)]
        p, top, total = scores(g)
        o = lax.dot_general(p_prev, chunk(v_buf, g - 1)[...], (((1,), (1,)), ((), ())), preferred_element_type=jnp.float32)
        merge(g - 1, o, *stats)
        p_buf[lax.rem(g, 2)] = p
        refill_after(fetch_k, g)
        refill_after(fetch_v, g - 1)
        return top, total

    lax.fori_loop(1, items + 1, step, (top, total))

    lane2 = lax.broadcasted_iota(jnp.int32, (batch, dim), 1)
    o0 = acc[:batch, 0, :] / sm[:batch, 0, :]
    o1 = acc[:batch, 1, :] / sm[:batch, 1, :]
    out = jnp.where(lane2 < half, o0, o1).astype(jnp.bfloat16)
    weights[6].wait()
    part = project(out, wo_buf[...])
    cut = part_ref.shape[2]
    for i in range(2):
        part_ref[i] = part[:, i * cut:(i + 1) * cut]


def self_attention(x, k_cache, v_cache, seq_lens, gain, bias, w_q, w_k, w_v, w_o):
    batch, ctx, heads, head_dim = k_cache.shape
    dim = heads * head_dim
    model = x.shape[1]
    most = batch * (ctx // CHUNK) + 2
    k_t = k_cache.transpose(0, 2, 3, 1).reshape(batch, dim, ctx)
    v_t = v_cache.transpose(0, 2, 3, 1).reshape(batch, dim, ctx)
    vmem = pl.BlockSpec(memory_space=pltpu.VMEM)
    f32, bf16 = jnp.float32, jnp.bfloat16
    return pl.pallas_call(
        self_kernel,
        out_shape=(jax.ShapeDtypeStruct((2, batch, model // 2), bf16),
                   jax.ShapeDtypeStruct((batch, heads, head_dim), bf16),
                   jax.ShapeDtypeStruct((batch, heads, head_dim), bf16)),
        in_specs=[pl.BlockSpec(memory_space=pltpu.SMEM)] + [pl.BlockSpec(memory_space=pltpu.HBM)] * 9,
        out_specs=(vmem, vmem, vmem),
        scratch_shapes=[
            pltpu.VMEM((batch, model), bf16), pltpu.VMEM((1, model), f32), pltpu.VMEM((1, model), f32),
            pltpu.VMEM((model, dim), bf16), pltpu.VMEM((model, dim), bf16), pltpu.VMEM((model, dim), bf16),
            pltpu.VMEM((dim, model), bf16),
            pltpu.VMEM((SLOTS, dim, ctx), bf16), pltpu.VMEM((SLOTS, dim, ctx), bf16),
            pltpu.VMEM((batch + 1, 8, dim), bf16),
            pltpu.VMEM((2, 8, CHUNK), bf16),
            pltpu.VMEM((batch + 1, 8, dim), f32), pltpu.VMEM((batch + 1, 8, dim), f32), pltpu.VMEM((batch + 1, 8, dim), f32),
            pltpu.SMEM((most,), jnp.int32), pltpu.SMEM((most,), jnp.int32),
            pltpu.SemaphoreType.DMA((7,)), pltpu.SemaphoreType.DMA((SLOTS,)), pltpu.SemaphoreType.DMA((SLOTS,)),
        ],
        cost_estimate=pl.CostEstimate(flops=2 * 2 * batch * ctx * dim * 8, bytes_accessed=batch * ctx * dim * 2, transcendentals=0),
        compiler_params=pltpu.CompilerParams(vmem_limit_bytes=32 << 20),
        name="self_attention",
    )(*[pltpu.with_memory_space_constraint(v, pltpu.HBM)
        for v in (seq_lens, x, gain.reshape(1, model), bias.reshape(1, model), w_q, w_k, w_v, w_o, k_t, v_t)])


def pack_kernel(a_hbm, b_hbm, c_hbm, out_ref, sem):
    width = a_hbm.shape[1]
    copies = [pltpu.make_async_copy(src, out_ref.at[:, pl.ds(i * width, width)], sem.at[i]) for i, src in enumerate((a_hbm, b_hbm, c_hbm))]
    for copy in copies:
        copy.start()
    for copy in copies:
        copy.wait()


def pack(*parts):
    model, width = parts[0].shape
    return pl.pallas_call(
        pack_kernel,
        out_shape=jax.ShapeDtypeStruct((model, 3 * width), parts[0].dtype),
        in_specs=[pl.BlockSpec(memory_space=pltpu.HBM)] * 3,
        out_specs=pl.BlockSpec(memory_space=pltpu.VMEM),
        scratch_shapes=[pltpu.SemaphoreType.DMA((3,))],
        compiler_params=pltpu.CompilerParams(vmem_limit_bytes=8 << 20),
        name="pack_weights",
    )(*[pltpu.with_memory_space_constraint(v, pltpu.HBM) for v in parts])


def post_kernel(part_ref, x_ref, gain2_ref, bias2_ref, gain3_ref, bias3_ref, enc, w0, w1, w2, w3, woc, wup, wdn, out_ref,
                mate_ref, k_all, v_all, o_out, o_in, p_buf, a_buf, b_buf, c_buf,
                e_sem, a_send, a_recv, b_send, b_recv, c_send, c_recv, o_send, o_recv):
    f32, bf16 = jnp.float32, jnp.bfloat16
    batch, model = x_ref.shape
    half = model // 2
    me = lax.axis_index('tp')
    chip, core = me // 2, me % 2
    chip_y, chip_x = chip // 2, chip % 2
    mate = 2 * chip + 1 - core

    def other(k):
        return 2 * (2 * (1 - chip_y if k // 2 else chip_y) + (1 - chip_x if k % 2 else chip_x)) + core

    barrier = pltpu.get_barrier_semaphore()
    for device in (other(3), other(2), other(1), mate):
        pl.semaphore_signal(barrier, inc=1, device_id={'tp': device}, device_id_type=MESH)
    with jax.named_scope('barrier'):
        pl.semaphore_wait(barrier, 4)

    sends = []

    def send(src, dst, send_sem, recv_sem, device):
        copy = pltpu.make_async_remote_copy(src_ref=src, dst_ref=dst, send_sem=send_sem, recv_sem=recv_sem,
                                            device_id={'tp': device}, device_id_type=MESH)
        copy.start()
        sends.append(copy)
        return copy

    def swap_halves(n, parts):
        return send(parts.at[1 - core], a_buf.at[n], a_send.at[n], a_recv.at[n], mate)

    def share(n, mine, copy):
        with jax.named_scope('mate_half'):
            copy.wait_recv()
        b_buf[n, chip] = (mine.astype(f32) + a_buf[n].astype(f32)).astype(bf16)
        return [send(b_buf.at[n, chip], b_buf.at[n, chip], b_send.at[n, k], b_recv.at[n, k], other(k)) for k in (3, 2, 1)]

    def finish(n, copies):
        with jax.named_scope('chip_sums'):
            for copy in copies:
                copy.wait_recv()
        total = b_buf[n, 0].astype(f32)
        for i in range(1, 4):
            total = total + b_buf[n, i].astype(f32)
        c_buf[n, core] = total.astype(bf16)
        return send(c_buf.at[n, core], c_buf.at[n, core], c_send.at[n], c_recv.at[n], mate)

    def whole(n, copy):
        with jax.named_scope('mate_sum'):
            copy.wait_recv()
        return jnp.concatenate([c_buf[n, 0], c_buf[n, 1]], axis=1).astype(f32)

    tokens = enc.shape[1]
    rows = PROJ_ROWS
    per = rows // tokens
    side = 2 * HEADS_DIM
    wide = 4 * side

    def weight(i):
        return jnp.concatenate([w[:, i * side:(i + 1) * side] for w in (w0, w1, w2, w3)], axis=1)

    def project_tokens(source, place, i, dest):
        def body(j, _):
            lines = source[pl.ds(j * per, per)].reshape(rows, model)
            got = project(lines, weight(i)).reshape(per, tokens, wide)
            dest[pl.ds(j * per, per), place * tokens:(place + 1) * tokens, :] = got
            return 0
        lax.fori_loop(0, batch // per, body, 0)

    a = swap_halves(0, part_ref)
    e = send(enc, mate_ref, e_sem.at[0], e_sem.at[1], mate)
    b = share(0, part_ref[core], a)
    project_tokens(enc, 0, 0, k_all)
    project_tokens(enc, 0, 1, v_all)
    with jax.named_scope('mate_tokens'):
        e.wait_recv()
    project_tokens(mate_ref, 1, 0, k_all)
    c = finish(0, b)
    project_tokens(mate_ref, 1, 1, v_all)
    hidden = x_ref[...].astype(f32) + whole(0, c)
    normed = layer_norm(hidden, gain2_ref[...], bias2_ref[...])
    q_eight = project(normed, weight(2)).astype(f32)
    own = (lax.broadcasted_iota(jnp.int32, (8, wide), 1) // HEADS_DIM) == lax.broadcasted_iota(jnp.int32, (8, wide), 0)
    nt = (((1,), (1,)), ((), ()))
    scale = HEADS_DIM ** -0.5
    outs, tops, sums = [], [], []
    for b in range(batch):
        q_b = jnp.where(own, q_eight[b:b + 1, :], 0.0).astype(bf16)
        s = lax.dot_general(q_b, k_all[b], nt, preferred_element_type=f32) * scale
        top = jnp.max(s, axis=-1, keepdims=True)
        e = jnp.exp(s - top)
        o = jnp.dot(e.astype(bf16), v_all[b], preferred_element_type=f32)
        outs.append(jnp.sum(jnp.where(own, o, 0.0), axis=0, keepdims=True))
        tops.append(top)
        sums.append(jnp.sum(e, axis=-1, keepdims=True))
    lane = lax.broadcasted_iota(jnp.int32, (8, side), 1)
    line = lax.broadcasted_iota(jnp.int32, (8, side), 0)
    for b in range(batch):
        stat = jnp.where(lane % HEADS_DIM < HEADS_DIM // 2, tops[b], sums[b])
        for k in range(4):
            o_out[k, b:b + 1, :] = outs[b][:, k * side:(k + 1) * side]
            o_out[k, batch + b:batch + b + 1, :] = jnp.sum(jnp.where(line == 2 * k + lane // HEADS_DIM, stat, 0.0), axis=0, keepdims=True)
    os = [send(o_out.at[k], o_in.at[k], o_send.at[k], o_recv.at[k], other(k)) for k in (3, 2, 1)]
    with jax.named_scope('partial_heads'):
        for copy in os:
            copy.wait_recv()
    low = lax.broadcasted_iota(jnp.int32, (batch, side), 1) < HEADS_DIM
    middle = HEADS_DIM // 2

    def spread(stat, at):
        return jnp.where(low, stat[:, at:at + 1], stat[:, HEADS_DIM + at:HEADS_DIM + at + 1])

    pieces = [o_out[0]] + [o_in[k] for k in range(1, 4)]
    top_of = [spread(p[batch:], 0) for p in pieces]
    sum_of = [spread(p[batch:], middle) for p in pieces]
    top = functools.reduce(jnp.maximum, top_of)
    shares = [jnp.exp(t - top) for t in top_of]
    denom = sum(s * w for s, w in zip(sum_of, shares))
    numer = sum(p[:batch] * w for p, w in zip(pieces, shares))
    cross = (numer / denom).astype(bf16)
    part2 = project(cross, woc[...])
    for i in range(2):
        p_buf[0, i] = part2[:, i * half:(i + 1) * half]
    a = swap_halves(1, p_buf.at[0])
    c = finish(1, share(1, p_buf[0, core], a))
    hidden = hidden + whole(1, c)
    normed = layer_norm(hidden, gain3_ref[...], bias3_ref[...])
    up = jnp.dot(normed, wup[...], preferred_element_type=f32)
    up = (0.5 * up * (1.0 + lax.erf(up * (2.0 ** -0.5)))).astype(bf16)
    part3 = project(up, wdn[...])
    for i in range(2):
        p_buf[1, i] = part3[:, i * half:(i + 1) * half]
    a = swap_halves(2, p_buf.at[1])
    c = finish(2, share(2, p_buf[1, core], a))
    out_ref[...] = (hidden + whole(2, c)).astype(bf16)
    with jax.named_scope('drain'):
        for copy in sends:
            copy.wait_send()


def post_attention(part, x, gain2, bias2, gain3, bias3, enc, weights, wo_c, w_up, w_down):
    batch, model = x.shape
    f32, bf16 = jnp.float32, jnp.bfloat16
    vmem = pl.BlockSpec(memory_space=pltpu.VMEM)
    tokens = enc.shape[1]
    side = 2 * HEADS_DIM
    dma = pltpu.SemaphoreType.DMA
    return pl.pallas_call(
        post_kernel,
        out_shape=jax.ShapeDtypeStruct((batch, model), bf16),
        in_specs=[vmem] * 14,
        out_specs=vmem,
        scratch_shapes=[
            pltpu.VMEM((batch, tokens, model), bf16),
            pltpu.VMEM((batch, 2 * tokens, 4 * side), bf16), pltpu.VMEM((batch, 2 * tokens, 4 * side), bf16),
            pltpu.VMEM((4, 2 * batch, side), f32), pltpu.VMEM((4, 2 * batch, side), f32),
            pltpu.VMEM((2, 2, batch, model // 2), bf16), pltpu.VMEM((3, batch, model // 2), bf16),
            pltpu.VMEM((3, 4, batch, model // 2), bf16), pltpu.VMEM((3, 2, batch, model // 2), bf16),
            dma((2,)), dma((3,)), dma((3,)), dma((3, 4)), dma((3, 4)), dma((3,)), dma((3,)), dma((4,)), dma((4,)),
        ],
        compiler_params=pltpu.CompilerParams(collective_id=0, has_side_effects=True, vmem_limit_bytes=24 << 20),
        cost_estimate=pl.CostEstimate(flops=2 * batch * 2 * tokens * model * 8 * side, bytes_accessed=9 << 20, transcendentals=0),
        name="post_attention",
    )(part, x, gain2.reshape(1, model), bias2.reshape(1, model), gain3.reshape(1, model), bias3.reshape(1, model),
      enc, *weights, wo_c, w_up, w_down)


def local_step(x, k_cache, v_cache, seq_lens, nbr_enc, ln1_gain, ln1_bias, w_q, w_k, w_v, w_o, ln2_gain, ln2_bias, wq_c, wk_c, wv_c, wo_c, ln3_gain, ln3_bias, w_up, w_down):
    mine = pack(wk_c, wv_c, wq_c)
    weights = [mine] + [lax.ppermute(mine, 'tp', [(t, t ^ (2 * k)) for t in range(8)]) for k in (1, 2, 3)]
    part, k_new, v_new = self_attention(x, k_cache, v_cache, seq_lens, ln1_gain, ln1_bias, w_q, w_k, w_v, w_o)
    out = post_attention(part, x, ln2_gain, ln2_bias, ln3_gain, ln3_bias, nbr_enc, weights, wo_c, w_up, w_down)
    return out, k_new, v_new


def solution(mesh):
    row_spec = P('dp', None)
    cache_spec = P('dp', None, 'tp', None)
    head_spec = P('dp', 'tp', None)
    vec_spec = P(None)
    col_split = P(None, 'tp')
    row_split = P('tp', None)
    in_specs = (row_spec, cache_spec, cache_spec, P('dp'), P('dp', 'tp', None), vec_spec, vec_spec, col_split, col_split, col_split, row_split, vec_spec, vec_spec, col_split, col_split, col_split, row_split, vec_spec, vec_spec, col_split, row_split)
    out_specs = (row_spec, head_spec, head_spec)
    return jax.shard_map(local_step, mesh=mesh, in_specs=in_specs, out_specs=out_specs, check_vma=False)
```

```python
import functools

import jax
import jax.numpy as jnp
from jax import lax
from jax.experimental import pallas as pl
from jax.experimental.pallas import tpu as pltpu
from jax.sharding import PartitionSpec as P

LN_EPS = 1e-5
CHUNK = 2048
SLOTS = 5
NEG = -1e30
HEADS_DIM = 64
PROJ_ROWS = 512
GROUP = 4
MESH = pl.DeviceIdType.MESH


def layer_norm(values, ln_gain, ln_bias):
    row_mean = jnp.mean(values, axis=-1, keepdims=True)
    centred = values - row_mean
    row_var = jnp.mean(jnp.square(centred), axis=-1, keepdims=True)
    return (centred * lax.rsqrt(row_var + LN_EPS) * ln_gain + ln_bias).astype(jnp.bfloat16)


def project(operand, weight):
    return jnp.dot(operand, weight, preferred_element_type=jnp.float32).astype(jnp.bfloat16)


def self_kernel(lens_ref, x_hbm, gain_hbm, bias_hbm, wq_hbm, wk_hbm, wv_hbm, wo_hbm, k_hbm, v_hbm,
                part_ref, know_ref, vnow_ref,
                x_ref, gain_ref, bias_ref, wq_buf, wk_buf, wv_buf, wo_buf, k_buf, v_buf, q_all, p_buf, acc, mx, sm, row_tab, off_tab,
                w_sem, k_sem, v_sem):
    batch = x_ref.shape[0]
    dim = k_buf.shape[1]
    weights = [pltpu.make_async_copy(src, dst, w_sem.at[i]) for i, (src, dst) in enumerate(
        ((x_hbm, x_ref), (gain_hbm, gain_ref), (bias_hbm, bias_ref), (wq_hbm, wq_buf), (wk_hbm, wk_buf), (wv_hbm, wv_buf),
         (wo_hbm, wo_buf)))]
    for w in weights:
        w.start()

    def fetch(hbm, buf, sem, b):
        size = pl.multiple_of((lens_ref[b] + 127) // 128 * 128, 128)
        slot = lax.rem(b, SLOTS)
        return pltpu.make_async_copy(hbm.at[b, :, pl.ds(0, size)], buf.at[slot, :, pl.ds(0, size)], sem.at[slot])

    def fetch_k(b):
        return fetch(k_hbm, k_buf, k_sem, b)

    def fetch_v(b):
        return fetch(v_hbm, v_buf, v_sem, b)

    for b in range(SLOTS):
        k_buf[b] = jnp.zeros(k_buf.shape[1:], k_buf.dtype)
        fetch_k(b).start(priority=0)
        v_buf[b] = jnp.zeros(v_buf.shape[1:], v_buf.dtype)
        fetch_v(b).start(priority=1)

    def build_row(b, at):
        def build(j, at):
            row_tab[at] = b
            off_tab[at] = j * CHUNK
            return at + 1
        return lax.fori_loop(0, (lens_ref[b] + CHUNK - 1) // CHUNK, build, at)

    items = lax.fori_loop(0, batch, build_row, jnp.int32(0))
    row_tab[items] = batch
    off_tab[items] = 0

    for w in weights[:3]:
        w.wait()
    normed = layer_norm(x_ref[...].astype(jnp.float32), gain_ref[...], bias_ref[...])
    for w in weights[3:6]:
        w.wait()
    q_new = project(normed, wq_buf[...])
    k_new = project(normed, wk_buf[...])
    v_new = project(normed, wv_buf[...])
    half = dim // 2
    for h in range(2):
        know_ref[:, h, :] = k_new[:, h * half:(h + 1) * half]
        vnow_ref[:, h, :] = v_new[:, h * half:(h + 1) * half]
    lane = lax.broadcasted_iota(jnp.int32, (batch, 8, 2 * dim), 2)
    row = lax.broadcasted_iota(jnp.int32, (batch, 8, 2 * dim), 1)
    q_f = q_new.astype(jnp.float32)
    q_wide = jnp.where(lane // half == row, jnp.concatenate([q_f, q_f], axis=1)[:, None, :], 0.0)
    q_all[:batch] = jnp.where(lane // half == row, jnp.concatenate([q_f, q_f], axis=1)[:, None, :], 0.0).astype(jnp.bfloat16)
    q_all[batch] = jnp.zeros((8, 2 * dim), jnp.bfloat16)
    s_new = jnp.sum(q_wide[:, :, :dim] * k_new.astype(jnp.float32)[:, None, :], axis=-1, keepdims=True) * (half ** -0.5)
    new_row = row[:, :, :dim] < 2
    v_f = v_new.astype(jnp.float32)[:, None, :]
    mx[:batch] = jnp.where(new_row, s_new, NEG)
    sm[:batch] = jnp.where(new_row, 1.0, 0.0)
    acc[:batch, :, :dim] = jnp.where(new_row, v_f, 0.0)
    acc[:batch, :, dim:] = jnp.zeros((batch, 8, dim), jnp.float32)
    mx[batch] = jnp.zeros((8, dim), jnp.float32)
    sm[batch] = jnp.ones((8, dim), jnp.float32)
    acc[batch] = jnp.zeros((8, 2 * dim), jnp.float32)

    wing = CHUNK // 2
    spot = lax.broadcasted_iota(jnp.int32, (8, wing), 1) + lax.broadcasted_iota(jnp.int32, (8, wing), 0) // 2 * wing
    scale = half ** -0.5

    def chunk(buf, i):
        slot = lax.rem(row_tab[i], SLOTS)
        return jnp.concatenate([buf[slot, :, pl.ds(pl.multiple_of(off_tab[i] + w, wing), wing)] for w in (0, wing)], axis=0)

    def scores(i):
        b = row_tab[i]
        s = jnp.dot(q_all[b], chunk(k_buf, i), preferred_element_type=jnp.float32) * scale
        s = jnp.where(spot < lens_ref[jnp.minimum(b, batch - 1)] - off_tab[i], s, NEG)
        top = jnp.max(s, axis=-1, keepdims=True)
        e = jnp.exp(s - top)
        return e.astype(jnp.bfloat16), top, jnp.sum(e, axis=-1, keepdims=True)

    def merge(i, o, top, total):
        b = row_tab[i]
        old = mx[b]
        new = jnp.maximum(old, top)
        keep = jnp.exp(old - new)
        add = jnp.exp(top - new)
        mx[b] = new
        sm[b] = sm[b] * keep + total * add
        acc[b] = acc[b] * jnp.concatenate([keep, keep], axis=1) + o * jnp.concatenate([add, add], axis=1)

    def await_first(copy, i):
        @pl.when((off_tab[i] == 0) & (row_tab[i] < batch))
        def _():
            copy(row_tab[i]).wait()

    def refill_after(copy, i):
        @pl.when((off_tab[i + 1] == 0) & (row_tab[i] + SLOTS < batch))
        def _():
            copy(row_tab[i] + SLOTS).start(priority=0 if copy is fetch_k else 1)

    await_first(fetch_k, 0)
    p, top, total = scores(0)
    p_buf[0] = p
    refill_after(fetch_k, 0)

    def step(g, stats):
        await_first(fetch_k, g)
        await_first(fetch_v, g - 1)
        p_prev = p_buf[lax.rem(g - 1, 2)]
        p, top, total = scores(g)
        o = lax.dot_general(p_prev, chunk(v_buf, g - 1), (((1,), (1,)), ((), ())), preferred_element_type=jnp.float32)
        merge(g - 1, o, *stats)
        p_buf[lax.rem(g, 2)] = p
        refill_after(fetch_k, g)
        refill_after(fetch_v, g - 1)
        return top, total

    lax.fori_loop(1, items + 1, step, (top, total))

    lane2 = lax.broadcasted_iota(jnp.int32, (batch, dim), 1)

    def head(h):
        top_a, top_b = mx[:batch, h, :], mx[:batch, h + 2, :]
        top = jnp.maximum(top_a, top_b)
        share_a, share_b = jnp.exp(top_a - top), jnp.exp(top_b - top)
        numer = acc[:batch, h, :dim] * share_a + acc[:batch, h + 2, dim:] * share_b
        return numer / (sm[:batch, h, :] * share_a + sm[:batch, h + 2, :] * share_b)

    out = jnp.where(lane2 < half, head(0), head(1)).astype(jnp.bfloat16)
    weights[6].wait()
    part = project(out, wo_buf[...])
    cut = part_ref.shape[2]
    for i in range(2):
        part_ref[i] = part[:, i * cut:(i + 1) * cut]


def self_attention(x, k_cache, v_cache, seq_lens, gain, bias, w_q, w_k, w_v, w_o):
    batch, ctx, heads, head_dim = k_cache.shape
    dim = heads * head_dim
    model = x.shape[1]
    most = batch * (ctx // CHUNK) + 2
    k_t = k_cache.transpose(0, 2, 3, 1).reshape(batch, dim, ctx)
    v_t = v_cache.transpose(0, 2, 3, 1).reshape(batch, dim, ctx)
    vmem = pl.BlockSpec(memory_space=pltpu.VMEM)
    f32, bf16 = jnp.float32, jnp.bfloat16
    return pl.pallas_call(
        self_kernel,
        out_shape=(jax.ShapeDtypeStruct((2, batch, model // 2), bf16),
                   jax.ShapeDtypeStruct((batch, heads, head_dim), bf16),
                   jax.ShapeDtypeStruct((batch, heads, head_dim), bf16)),
        in_specs=[pl.BlockSpec(memory_space=pltpu.SMEM)] + [pl.BlockSpec(memory_space=pltpu.HBM)] * 9,
        out_specs=(vmem, vmem, vmem),
        scratch_shapes=[
            pltpu.VMEM((batch, model), bf16), pltpu.VMEM((1, model), f32), pltpu.VMEM((1, model), f32),
            pltpu.VMEM((model, dim), bf16), pltpu.VMEM((model, dim), bf16), pltpu.VMEM((model, dim), bf16),
            pltpu.VMEM((dim, model), bf16),
            pltpu.VMEM((SLOTS, dim, ctx), bf16), pltpu.VMEM((SLOTS, dim, ctx), bf16),
            pltpu.VMEM((batch + 1, 8, 2 * dim), bf16),
            pltpu.VMEM((2, 8, CHUNK // 2), bf16),
            pltpu.VMEM((batch + 1, 8, 2 * dim), f32), pltpu.VMEM((batch + 1, 8, dim), f32), pltpu.VMEM((batch + 1, 8, dim), f32),
            pltpu.SMEM((most,), jnp.int32), pltpu.SMEM((most,), jnp.int32),
            pltpu.SemaphoreType.DMA((7,)), pltpu.SemaphoreType.DMA((SLOTS,)), pltpu.SemaphoreType.DMA((SLOTS,)),
        ],
        cost_estimate=pl.CostEstimate(flops=2 * 2 * batch * ctx * dim * 8, bytes_accessed=batch * ctx * dim * 2, transcendentals=0),
        compiler_params=pltpu.CompilerParams(vmem_limit_bytes=32 << 20),
        name="self_attention",
    )(*[pltpu.with_memory_space_constraint(v, pltpu.HBM)
        for v in (seq_lens, x, gain.reshape(1, model), bias.reshape(1, model), w_q, w_k, w_v, w_o, k_t, v_t)])


def pack_kernel(a_hbm, b_hbm, out_ref, sem):
    width = a_hbm.shape[1]
    copies = [pltpu.make_async_copy(src, out_ref.at[:, pl.ds(i * width, width)], sem.at[i]) for i, src in enumerate((a_hbm, b_hbm))]
    for copy in copies:
        copy.start()
    for copy in copies:
        copy.wait()


def pack(*parts):
    model, width = parts[0].shape
    return pl.pallas_call(
        pack_kernel,
        out_shape=jax.ShapeDtypeStruct((model, 2 * width), parts[0].dtype),
        in_specs=[pl.BlockSpec(memory_space=pltpu.HBM)] * 2,
        out_specs=pl.BlockSpec(memory_space=pltpu.VMEM),
        scratch_shapes=[pltpu.SemaphoreType.DMA((2,))],
        compiler_params=pltpu.CompilerParams(vmem_limit_bytes=8 << 20),
        name="pack_weights",
    )(*[pltpu.with_memory_space_constraint(v, pltpu.HBM) for v in parts])


def post_kernel(part_ref, x_ref, gain2_ref, bias2_ref, gain3_ref, bias3_ref, enc, w0, w1, w2, w3, wqc, woc, wup, wdn, out_ref,
                mate_ref, k_all, v_all, q_buf, o_out, o_in, p_buf, a_buf, b_buf, c_buf,
                e_sem, a_send, a_recv, b_send, b_recv, c_send, c_recv, q_send, q_recv, o_send, o_recv):
    f32, bf16 = jnp.float32, jnp.bfloat16
    batch, model = x_ref.shape
    half = model // 2
    me = lax.axis_index('tp')
    chip, core = me // 2, me % 2
    chip_y, chip_x = chip // 2, chip % 2
    mate = 2 * chip + 1 - core

    def other(k):
        return 2 * (2 * (1 - chip_y if k // 2 else chip_y) + (1 - chip_x if k % 2 else chip_x)) + core

    barrier = pltpu.get_barrier_semaphore()
    for device in (other(3), other(2), other(1), mate):
        pl.semaphore_signal(barrier, inc=1, device_id={'tp': device}, device_id_type=MESH)
    with jax.named_scope('barrier'):
        pl.semaphore_wait(barrier, 4)

    sends = []

    def send(src, dst, send_sem, recv_sem, device):
        copy = pltpu.make_async_remote_copy(src_ref=src, dst_ref=dst, send_sem=send_sem, recv_sem=recv_sem,
                                            device_id={'tp': device}, device_id_type=MESH)
        copy.start()
        sends.append(copy)
        return copy

    def swap_halves(n, parts):
        return send(parts.at[1 - core], a_buf.at[n], a_send.at[n], a_recv.at[n], mate)

    def share(n, mine, copy):
        with jax.named_scope('mate_half'):
            copy.wait_recv()
        b_buf[n, chip] = (mine.astype(f32) + a_buf[n].astype(f32)).astype(bf16)
        return [send(b_buf.at[n, chip], b_buf.at[n, chip], b_send.at[n, k], b_recv.at[n, k], other(k)) for k in (3, 2, 1)]

    def finish(n, copies):
        with jax.named_scope('chip_sums'):
            for copy in copies:
                copy.wait_recv()
        total = b_buf[n, 0].astype(f32)
        for i in range(1, 4):
            total = total + b_buf[n, i].astype(f32)
        c_buf[n, core] = total.astype(bf16)
        return send(c_buf.at[n, core], c_buf.at[n, core], c_send.at[n], c_recv.at[n], mate)

    def whole(n, copy):
        with jax.named_scope('mate_sum'):
            copy.wait_recv()
        return jnp.concatenate([c_buf[n, 0], c_buf[n, 1]], axis=1).astype(f32)

    tokens = enc.shape[1]
    rows = PROJ_ROWS
    per = rows // tokens
    side = 2 * HEADS_DIM
    wide = 4 * side

    def weight(i):
        return jnp.concatenate([w[:, i * side:(i + 1) * side] for w in (w0, w1, w2, w3)], axis=1)

    def project_tokens(source, place, i, dest):
        def body(j, _):
            lines = source[pl.ds(j * per, per)].reshape(rows, model)
            got = project(lines, weight(i)).reshape(per, tokens, wide)
            dest[pl.ds(j * per, per), place * tokens:(place + 1) * tokens, :] = got
            return 0
        lax.fori_loop(0, batch // per, body, 0)

    a = swap_halves(0, part_ref)
    e = send(enc, mate_ref, e_sem.at[0], e_sem.at[1], mate)
    b = share(0, part_ref[core], a)
    project_tokens(enc, 0, 0, k_all)
    project_tokens(enc, 0, 1, v_all)
    c = finish(0, b)
    hidden = x_ref[...].astype(f32) + whole(0, c)
    normed = layer_norm(hidden, gain2_ref[...], bias2_ref[...])
    q_buf[0] = project(normed, wqc[...])
    qs = [send(q_buf.at[0], q_buf.at[k], q_send.at[k], q_recv.at[k], other(k)) for k in (3, 2, 1)]
    with jax.named_scope('mate_tokens'):
        e.wait_recv()
    project_tokens(mate_ref, 1, 0, k_all)
    project_tokens(mate_ref, 1, 1, v_all)
    with jax.named_scope('other_heads'):
        for copy in qs:
            copy.wait_recv()
    q_eight = jnp.concatenate([q_buf[k] for k in range(4)], axis=1).astype(f32)
    many = 8 * GROUP
    col = lax.broadcasted_iota(jnp.int32, (many, wide), 1)
    line = lax.broadcasted_iota(jnp.int32, (many, wide), 0)
    own = col // HEADS_DIM == line % 8
    span = GROUP * 2 * tokens
    match = lax.broadcasted_iota(jnp.int32, (many, span), 1) // (2 * tokens) == lax.broadcasted_iota(jnp.int32, (many, span), 0) // 8
    nt = (((1,), (1,)), ((), ()))
    scale = HEADS_DIM ** -0.5

    def squeeze(values):
        return jnp.sum(jnp.where(own, values, 0.0).reshape(GROUP, 8, wide), axis=1)

    for g in range(batch // GROUP):
        at = slice(g * GROUP, (g + 1) * GROUP)
        q_g = jnp.broadcast_to(q_eight[at][:, None, :], (GROUP, 8, wide)).reshape(many, wide)
        q_g = jnp.where(own, q_g, 0.0).astype(bf16)
        s = lax.dot_general(q_g, k_all[at].reshape(span, wide), nt, preferred_element_type=f32) * scale
        s = jnp.where(match, s, NEG)
        top = jnp.max(s, axis=-1, keepdims=True)
        p = jnp.exp(s - top)
        total = jnp.sum(p, axis=-1, keepdims=True)
        o = squeeze(jnp.dot(p.astype(bf16), v_all[at].reshape(span, wide), preferred_element_type=f32))
        stat = squeeze(jnp.where(col % HEADS_DIM < HEADS_DIM // 2, top, total))
        for k in range(4):
            o_out[k, g * GROUP:(g + 1) * GROUP, :] = o[:, k * side:(k + 1) * side]
            o_out[k, batch + g * GROUP:batch + (g + 1) * GROUP, :] = stat[:, k * side:(k + 1) * side]
    os = [send(o_out.at[k], o_in.at[k], o_send.at[k], o_recv.at[k], other(k)) for k in (3, 2, 1)]
    with jax.named_scope('partial_heads'):
        for copy in os:
            copy.wait_recv()
    low = lax.broadcasted_iota(jnp.int32, (batch, side), 1) < HEADS_DIM
    middle = HEADS_DIM // 2

    def spread(stat, at):
        return jnp.where(low, stat[:, at:at + 1], stat[:, HEADS_DIM + at:HEADS_DIM + at + 1])

    pieces = [o_out[0]] + [o_in[k] for k in range(1, 4)]
    top_of = [spread(p[batch:], 0) for p in pieces]
    sum_of = [spread(p[batch:], middle) for p in pieces]
    top = functools.reduce(jnp.maximum, top_of)
    shares = [jnp.exp(t - top) for t in top_of]
    denom = sum(s * w for s, w in zip(sum_of, shares))
    numer = sum(p[:batch] * w for p, w in zip(pieces, shares))
    cross = (numer / denom).astype(bf16)
    part2 = project(cross, woc[...])
    for i in range(2):
        p_buf[0, i] = part2[:, i * half:(i + 1) * half]
    a = swap_halves(1, p_buf.at[0])
    c = finish(1, share(1, p_buf[0, core], a))
    hidden = hidden + whole(1, c)
    normed = layer_norm(hidden, gain3_ref[...], bias3_ref[...])
    up = jnp.dot(normed, wup[...], preferred_element_type=f32)
    up = (0.5 * up * (1.0 + lax.erf(up * (2.0 ** -0.5)))).astype(bf16)
    part3 = project(up, wdn[...])
    for i in range(2):
        p_buf[1, i] = part3[:, i * half:(i + 1) * half]
    a = swap_halves(2, p_buf.at[1])
    c = finish(2, share(2, p_buf[1, core], a))
    out_ref[...] = (hidden + whole(2, c)).astype(bf16)
    with jax.named_scope('drain'):
        for copy in sends:
            copy.wait_send()


def post_attention(part, x, gain2, bias2, gain3, bias3, enc, weights, wq_c, wo_c, w_up, w_down):
    batch, model = x.shape
    f32, bf16 = jnp.float32, jnp.bfloat16
    vmem = pl.BlockSpec(memory_space=pltpu.VMEM)
    tokens = enc.shape[1]
    side = 2 * HEADS_DIM
    dma = pltpu.SemaphoreType.DMA
    return pl.pallas_call(
        post_kernel,
        out_shape=jax.ShapeDtypeStruct((batch, model), bf16),
        in_specs=[vmem] * 15,
        out_specs=vmem,
        scratch_shapes=[
            pltpu.VMEM((batch, tokens, model), bf16),
            pltpu.VMEM((batch, 2 * tokens, 4 * side), bf16), pltpu.VMEM((batch, 2 * tokens, 4 * side), bf16),
            pltpu.VMEM((4, batch, side), bf16), pltpu.VMEM((4, 2 * batch, side), f32), pltpu.VMEM((4, 2 * batch, side), f32),
            pltpu.VMEM((2, 2, batch, model // 2), bf16), pltpu.VMEM((3, batch, model // 2), bf16),
            pltpu.VMEM((3, 4, batch, model // 2), bf16), pltpu.VMEM((3, 2, batch, model // 2), bf16),
            dma((2,)), dma((3,)), dma((3,)), dma((3, 4)), dma((3, 4)), dma((3,)), dma((3,)), dma((4,)), dma((4,)), dma((4,)), dma((4,)),
        ],
        compiler_params=pltpu.CompilerParams(collective_id=0, has_side_effects=True, vmem_limit_bytes=24 << 20),
        cost_estimate=pl.CostEstimate(flops=2 * batch * 2 * tokens * model * 8 * side, bytes_accessed=9 << 20, transcendentals=0),
        name="post_attention",
    )(part, x, gain2.reshape(1, model), bias2.reshape(1, model), gain3.reshape(1, model), bias3.reshape(1, model),
      enc, *weights, wq_c, wo_c, w_up, w_down)


def local_step(x, k_cache, v_cache, seq_lens, nbr_enc, ln1_gain, ln1_bias, w_q, w_k, w_v, w_o, ln2_gain, ln2_bias, wq_c, wk_c, wv_c, wo_c, ln3_gain, ln3_bias, w_up, w_down):
    mine = pack(wk_c, wv_c)
    weights = [mine] + [lax.ppermute(mine, 'tp', [(t, t ^ (2 * k)) for t in range(8)]) for k in (1, 2, 3)]
    part, k_new, v_new = self_attention(x, k_cache, v_cache, seq_lens, ln1_gain, ln1_bias, w_q, w_k, w_v, w_o)
    out = post_attention(part, x, ln2_gain, ln2_bias, ln3_gain, ln3_bias, nbr_enc, weights, wq_c, wo_c, w_up, w_down)
    return out, k_new, v_new


def solution(mesh):
    row_spec = P('dp', None)
    cache_spec = P('dp', None, 'tp', None)
    head_spec = P('dp', 'tp', None)
    vec_spec = P(None)
    col_split = P(None, 'tp')
    row_split = P('tp', None)
    in_specs = (row_spec, cache_spec, cache_spec, P('dp'), P('dp', 'tp', None), vec_spec, vec_spec, col_split, col_split, col_split, row_split, vec_spec, vec_spec, col_split, col_split, col_split, row_split, vec_spec, vec_spec, col_split, row_split)
    out_specs = (row_spec, head_spec, head_spec)
    return jax.shard_map(local_step, mesh=mesh, in_specs=in_specs, out_specs=out_specs, check_vma=False)
```

```python
import functools

import jax
import jax.numpy as jnp
from jax import lax
from jax.experimental import pallas as pl
from jax.experimental.pallas import tpu as pltpu
from jax.sharding import PartitionSpec as P

LN_EPS = 1e-5
CHUNK = 2048
SLOTS = 5
NEG = -1e30
HEADS_DIM = 64
PROJ_ROWS = 512
GROUP = 4
MESH = pl.DeviceIdType.MESH


def layer_norm(values, ln_gain, ln_bias):
    row_mean = jnp.mean(values, axis=-1, keepdims=True)
    centred = values - row_mean
    row_var = jnp.mean(jnp.square(centred), axis=-1, keepdims=True)
    return (centred * lax.rsqrt(row_var + LN_EPS) * ln_gain + ln_bias).astype(jnp.bfloat16)


def project(operand, weight):
    return jnp.dot(operand, weight, preferred_element_type=jnp.float32).astype(jnp.bfloat16)


def self_kernel(lens_ref, x_hbm, gain_hbm, bias_hbm, wq_hbm, wk_hbm, wv_hbm, wo_hbm, k_hbm, v_hbm,
                part_ref, know_ref, vnow_ref,
                x_ref, gain_ref, bias_ref, wq_buf, wk_buf, wv_buf, wo_buf, k_buf, v_buf, q_all, p_buf, acc, mx, sm, row_tab, off_tab,
                w_sem, k_sem, v_sem):
    batch = x_ref.shape[0]
    dim = k_buf.shape[1]
    weights = [pltpu.make_async_copy(src, dst, w_sem.at[i]) for i, (src, dst) in enumerate(
        ((x_hbm, x_ref), (gain_hbm, gain_ref), (bias_hbm, bias_ref), (wq_hbm, wq_buf), (wk_hbm, wk_buf), (wv_hbm, wv_buf),
         (wo_hbm, wo_buf)))]
    for w in weights:
        w.start()

    def fetch(hbm, buf, sem, b):
        size = pl.multiple_of((lens_ref[b] + 127) // 128 * 128, 128)
        slot = lax.rem(b, SLOTS)
        return pltpu.make_async_copy(hbm.at[b, :, pl.ds(0, size)], buf.at[slot, :, pl.ds(0, size)], sem.at[slot])

    def fetch_k(b):
        return fetch(k_hbm, k_buf, k_sem, b)

    def fetch_v(b):
        return fetch(v_hbm, v_buf, v_sem, b)

    for b in range(SLOTS):
        fetch_k(b).start(priority=0)
        v_buf[b] = jnp.zeros(v_buf.shape[1:], v_buf.dtype)
        fetch_v(b).start(priority=1)

    def build_row(b, at):
        def build(j, at):
            row_tab[at] = b
            off_tab[at] = j * CHUNK
            return at + 1
        return lax.fori_loop(0, (lens_ref[b] + CHUNK - 1) // CHUNK, build, at)

    items = lax.fori_loop(0, batch, build_row, jnp.int32(0))
    row_tab[items] = batch
    off_tab[items] = 0

    for w in weights[:3]:
        w.wait()
    normed = layer_norm(x_ref[...].astype(jnp.float32), gain_ref[...], bias_ref[...])
    for w in weights[3:6]:
        w.wait()
    q_new = project(normed, wq_buf[...])
    k_new = project(normed, wk_buf[...])
    v_new = project(normed, wv_buf[...])
    half = dim // 2
    for h in range(2):
        know_ref[:, h, :] = k_new[:, h * half:(h + 1) * half]
        vnow_ref[:, h, :] = v_new[:, h * half:(h + 1) * half]
    lane = lax.broadcasted_iota(jnp.int32, (batch, 8, dim), 2)
    row = lax.broadcasted_iota(jnp.int32, (batch, 8, dim), 1)
    q_f = q_new.astype(jnp.float32)
    q_all[:batch] = jnp.where(lane // half == row, q_f[:, None, :], 0.0).astype(jnp.bfloat16)
    q_all[batch] = jnp.zeros((8, dim), jnp.bfloat16)
    mx[...] = jnp.full(mx.shape, NEG, jnp.float32)
    sm[...] = jnp.zeros_like(sm)
    acc[...] = jnp.zeros_like(acc)

    spot = lax.broadcasted_iota(jnp.int32, (8, CHUNK), 1)
    scale = half ** -0.5

    def scores(i):
        b = row_tab[i]
        off = pl.multiple_of(off_tab[i], CHUNK)
        keys = k_buf[lax.rem(b, SLOTS), :, pl.ds(off, CHUNK)]
        s = jnp.dot(q_all[b], keys, preferred_element_type=jnp.float32) * scale
        s = jnp.where(spot < lens_ref[jnp.minimum(b, batch - 1)] - off_tab[i], s, NEG)
        top = jnp.max(s, axis=-1, keepdims=True)
        e = jnp.exp(s - top)
        return e.astype(jnp.bfloat16).astype(jnp.float32), top, jnp.sum(e, axis=-1, keepdims=True)

    def weigh(i, par, h):
        slot = lax.rem(row_tab[i], SLOTS)
        out = None
        for t in range(0, CHUNK, 128):
            values = v_buf[slot, h * half:(h + 1) * half, pl.ds(pl.multiple_of(off_tab[i] + t, 128), 128)].astype(jnp.float32)
            term = values * p_buf[par, h:h + 1, t:t + 128]
            out = term if out is None else out + term
        return out

    def merge(i, par, top, total):
        b = row_tab[i]
        old = mx[b]
        new = jnp.maximum(old, top)
        keep = jnp.exp(old - new)
        add = jnp.exp(top - new)
        mx[b] = new
        sm[b] = sm[b] * keep + total * add
        for h in range(2):
            at = slice(h * half, (h + 1) * half)
            acc[b, at, :] = acc[b, at, :] * keep[h:h + 1, :] + weigh(i, par, h) * add[h:h + 1, :]

    def await_first(copy, i):
        @pl.when((off_tab[i] == 0) & (row_tab[i] < batch))
        def _():
            copy(row_tab[i]).wait()

    def refill_after(copy, i):
        @pl.when((off_tab[i + 1] == 0) & (row_tab[i] + SLOTS < batch))
        def _():
            copy(row_tab[i] + SLOTS).start(priority=0 if copy is fetch_k else 1)

    await_first(fetch_k, 0)
    p, top, total = scores(0)
    p_buf[0] = p
    refill_after(fetch_k, 0)

    def step(g, stats):
        await_first(fetch_k, g)
        await_first(fetch_v, g - 1)
        p, top, total = scores(g)
        merge(g - 1, lax.rem(g - 1, 2), *stats)
        p_buf[lax.rem(g, 2)] = p
        refill_after(fetch_k, g)
        refill_after(fetch_v, g - 1)
        return top, total

    lax.fori_loop(1, items + 1, step, (top, total))

    lane2 = lax.broadcasted_iota(jnp.int32, (batch, dim), 1)

    eye = lax.broadcasted_iota(jnp.int32, (dim, dim), 0) == lax.broadcasted_iota(jnp.int32, (dim, dim), 1)
    old_part = []
    for b in range(batch):
        column = jnp.sum(acc[b], axis=-1, keepdims=True)
        old_part.append(jnp.sum(jnp.where(eye, column, 0.0), axis=0, keepdims=True))
    old_part = jnp.concatenate(old_part, axis=0)
    first = lane2 < half
    prod = q_f * k_new.astype(jnp.float32) * scale
    s_new = jnp.where(first, jnp.sum(jnp.where(first, prod, 0.0), axis=-1, keepdims=True),
                      jnp.sum(jnp.where(first, 0.0, prod), axis=-1, keepdims=True))
    top_old = jnp.where(first, mx[:batch, 0, :], mx[:batch, 1, :])
    sum_old = jnp.where(first, sm[:batch, 0, :], sm[:batch, 1, :])
    top_all = jnp.maximum(top_old, s_new)
    share_old, share_new = jnp.exp(top_old - top_all), jnp.exp(s_new - top_all)
    out = (old_part * share_old + v_new.astype(jnp.float32) * share_new) / (sum_old * share_old + share_new)
    out = out.astype(jnp.bfloat16)
    weights[6].wait()
    part = project(out, wo_buf[...])
    cut = part_ref.shape[2]
    for i in range(2):
        part_ref[i] = part[:, i * cut:(i + 1) * cut]


def self_attention(x, k_cache, v_cache, seq_lens, gain, bias, w_q, w_k, w_v, w_o):
    batch, ctx, heads, head_dim = k_cache.shape
    dim = heads * head_dim
    model = x.shape[1]
    most = batch * (ctx // CHUNK) + 2
    k_t = k_cache.transpose(0, 2, 3, 1).reshape(batch, dim, ctx)
    v_t = v_cache.transpose(0, 2, 3, 1).reshape(batch, dim, ctx)
    vmem = pl.BlockSpec(memory_space=pltpu.VMEM)
    f32, bf16 = jnp.float32, jnp.bfloat16
    return pl.pallas_call(
        self_kernel,
        out_shape=(jax.ShapeDtypeStruct((2, batch, model // 2), bf16),
                   jax.ShapeDtypeStruct((batch, heads, head_dim), bf16),
                   jax.ShapeDtypeStruct((batch, heads, head_dim), bf16)),
        in_specs=[pl.BlockSpec(memory_space=pltpu.SMEM)] + [pl.BlockSpec(memory_space=pltpu.HBM)] * 9,
        out_specs=(vmem, vmem, vmem),
        scratch_shapes=[
            pltpu.VMEM((batch, model), bf16), pltpu.VMEM((1, model), f32), pltpu.VMEM((1, model), f32),
            pltpu.VMEM((model, dim), bf16), pltpu.VMEM((model, dim), bf16), pltpu.VMEM((model, dim), bf16),
            pltpu.VMEM((dim, model), bf16),
            pltpu.VMEM((SLOTS, dim, ctx), bf16), pltpu.VMEM((SLOTS, dim, ctx), bf16),
            pltpu.VMEM((batch + 1, 8, dim), bf16),
            pltpu.VMEM((2, 8, CHUNK), f32),
            pltpu.VMEM((batch + 1, dim, dim), f32), pltpu.VMEM((batch + 1, 8, dim), f32), pltpu.VMEM((batch + 1, 8, dim), f32),
            pltpu.SMEM((most,), jnp.int32), pltpu.SMEM((most,), jnp.int32),
            pltpu.SemaphoreType.DMA((7,)), pltpu.SemaphoreType.DMA((SLOTS,)), pltpu.SemaphoreType.DMA((SLOTS,)),
        ],
        cost_estimate=pl.CostEstimate(flops=2 * 2 * batch * ctx * dim * 8, bytes_accessed=batch * ctx * dim * 2, transcendentals=0),
        compiler_params=pltpu.CompilerParams(vmem_limit_bytes=32 << 20),
        name="self_attention",
    )(*[pltpu.with_memory_space_constraint(v, pltpu.HBM)
        for v in (seq_lens, x, gain.reshape(1, model), bias.reshape(1, model), w_q, w_k, w_v, w_o, k_t, v_t)])


def pack_kernel(a_hbm, b_hbm, out_ref, sem):
    width = a_hbm.shape[1]
    copies = [pltpu.make_async_copy(src, out_ref.at[:, pl.ds(i * width, width)], sem.at[i]) for i, src in enumerate((a_hbm, b_hbm))]
    for copy in copies:
        copy.start()
    for copy in copies:
        copy.wait()


def pack(*parts):
    model, width = parts[0].shape
    return pl.pallas_call(
        pack_kernel,
        out_shape=jax.ShapeDtypeStruct((model, 2 * width), parts[0].dtype),
        in_specs=[pl.BlockSpec(memory_space=pltpu.HBM)] * 2,
        out_specs=pl.BlockSpec(memory_space=pltpu.VMEM),
        scratch_shapes=[pltpu.SemaphoreType.DMA((2,))],
        compiler_params=pltpu.CompilerParams(vmem_limit_bytes=8 << 20),
        name="pack_weights",
    )(*[pltpu.with_memory_space_constraint(v, pltpu.HBM) for v in parts])


def post_kernel(part_ref, x_ref, gain2_ref, bias2_ref, gain3_ref, bias3_ref, enc, w0, w1, w2, w3, wqc, woc, wup, wdn, out_ref,
                mate_ref, k_all, v_all, q_buf, o_out, o_in, p_buf, a_buf, b_buf, c_buf,
                e_sem, a_send, a_recv, b_send, b_recv, c_send, c_recv, q_send, q_recv, o_send, o_recv):
    f32, bf16 = jnp.float32, jnp.bfloat16
    batch, model = x_ref.shape
    half = model // 2
    me = lax.axis_index('tp')
    chip, core = me // 2, me % 2
    chip_y, chip_x = chip // 2, chip % 2
    mate = 2 * chip + 1 - core

    def other(k):
        return 2 * (2 * (1 - chip_y if k // 2 else chip_y) + (1 - chip_x if k % 2 else chip_x)) + core

    barrier = pltpu.get_barrier_semaphore()
    for device in (other(3), other(2), other(1), mate):
        pl.semaphore_signal(barrier, inc=1, device_id={'tp': device}, device_id_type=MESH)
    with jax.named_scope('barrier'):
        pl.semaphore_wait(barrier, 4)

    sends = []

    def send(src, dst, send_sem, recv_sem, device):
        copy = pltpu.make_async_remote_copy(src_ref=src, dst_ref=dst, send_sem=send_sem, recv_sem=recv_sem,
                                            device_id={'tp': device}, device_id_type=MESH)
        copy.start()
        sends.append(copy)
        return copy

    def swap_halves(n, parts):
        return send(parts.at[1 - core], a_buf.at[n], a_send.at[n], a_recv.at[n], mate)

    def share(n, mine, copy):
        with jax.named_scope('mate_half'):
            copy.wait_recv()
        b_buf[n, chip] = (mine.astype(f32) + a_buf[n].astype(f32)).astype(bf16)
        return [send(b_buf.at[n, chip], b_buf.at[n, chip], b_send.at[n, k], b_recv.at[n, k], other(k)) for k in (3, 2, 1)]

    def finish(n, copies):
        with jax.named_scope('chip_sums'):
            for copy in copies:
                copy.wait_recv()
        total = b_buf[n, 0].astype(f32)
        for i in range(1, 4):
            total = total + b_buf[n, i].astype(f32)
        c_buf[n, core] = total.astype(bf16)
        return send(c_buf.at[n, core], c_buf.at[n, core], c_send.at[n], c_recv.at[n], mate)

    def whole(n, copy):
        with jax.named_scope('mate_sum'):
            copy.wait_recv()
        return jnp.concatenate([c_buf[n, 0], c_buf[n, 1]], axis=1).astype(f32)

    tokens = enc.shape[1]
    rows = PROJ_ROWS
    per = rows // tokens
    side = 2 * HEADS_DIM
    wide = 4 * side

    def weight(i):
        return jnp.concatenate([w[:, i * side:(i + 1) * side] for w in (w0, w1, w2, w3)], axis=1)

    def project_tokens(source, place, i, dest):
        def body(j, _):
            lines = source[pl.ds(j * per, per)].reshape(rows, model)
            got = project(lines, weight(i)).reshape(per, tokens, wide)
            dest[pl.ds(j * per, per), place * tokens:(place + 1) * tokens, :] = got
            return 0
        lax.fori_loop(0, batch // per, body, 0)

    a = swap_halves(0, part_ref)
    e = send(enc, mate_ref, e_sem.at[0], e_sem.at[1], mate)
    b = share(0, part_ref[core], a)
    project_tokens(enc, 0, 0, k_all)
    project_tokens(enc, 0, 1, v_all)
    c = finish(0, b)
    hidden = x_ref[...].astype(f32) + whole(0, c)
    normed = layer_norm(hidden, gain2_ref[...], bias2_ref[...])
    q_buf[0] = project(normed, wqc[...])
    qs = [send(q_buf.at[0], q_buf.at[k], q_send.at[k], q_recv.at[k], other(k)) for k in (3, 2, 1)]
    with jax.named_scope('mate_tokens'):
        e.wait_recv()
    project_tokens(mate_ref, 1, 0, k_all)
    project_tokens(mate_ref, 1, 1, v_all)
    with jax.named_scope('other_heads'):
        for copy in qs:
            copy.wait_recv()
    q_eight = jnp.concatenate([q_buf[k] for k in range(4)], axis=1).astype(f32)
    many = 8 * GROUP
    col = lax.broadcasted_iota(jnp.int32, (many, wide), 1)
    line = lax.broadcasted_iota(jnp.int32, (many, wide), 0)
    own = col // HEADS_DIM == line % 8
    span = GROUP * 2 * tokens
    match = lax.broadcasted_iota(jnp.int32, (many, span), 1) // (2 * tokens) == lax.broadcasted_iota(jnp.int32, (many, span), 0) // 8
    nt = (((1,), (1,)), ((), ()))
    scale = HEADS_DIM ** -0.5

    def squeeze(values):
        return jnp.sum(jnp.where(own, values, 0.0).reshape(GROUP, 8, wide), axis=1)

    for g in range(batch // GROUP):
        at = slice(g * GROUP, (g + 1) * GROUP)
        q_g = jnp.broadcast_to(q_eight[at][:, None, :], (GROUP, 8, wide)).reshape(many, wide)
        q_g = jnp.where(own, q_g, 0.0).astype(bf16)
        s = lax.dot_general(q_g, k_all[at].reshape(span, wide), nt, preferred_element_type=f32) * scale
        s = jnp.where(match, s, NEG)
        top = jnp.max(s, axis=-1, keepdims=True)
        p = jnp.exp(s - top)
        total = jnp.sum(p, axis=-1, keepdims=True)
        o = squeeze(jnp.dot(p.astype(bf16), v_all[at].reshape(span, wide), preferred_element_type=f32))
        stat = squeeze(jnp.where(col % HEADS_DIM < HEADS_DIM // 2, top, total))
        for k in range(4):
            o_out[k, g * GROUP:(g + 1) * GROUP, :] = o[:, k * side:(k + 1) * side]
            o_out[k, batch + g * GROUP:batch + (g + 1) * GROUP, :] = stat[:, k * side:(k + 1) * side]
    os = [send(o_out.at[k], o_in.at[k], o_send.at[k], o_recv.at[k], other(k)) for k in (3, 2, 1)]
    with jax.named_scope('partial_heads'):
        for copy in os:
            copy.wait_recv()
    low = lax.broadcasted_iota(jnp.int32, (batch, side), 1) < HEADS_DIM
    middle = HEADS_DIM // 2

    def spread(stat, at):
        return jnp.where(low, stat[:, at:at + 1], stat[:, HEADS_DIM + at:HEADS_DIM + at + 1])

    pieces = [o_out[0]] + [o_in[k] for k in range(1, 4)]
    top_of = [spread(p[batch:], 0) for p in pieces]
    sum_of = [spread(p[batch:], middle) for p in pieces]
    top = functools.reduce(jnp.maximum, top_of)
    shares = [jnp.exp(t - top) for t in top_of]
    denom = sum(s * w for s, w in zip(sum_of, shares))
    numer = sum(p[:batch] * w for p, w in zip(pieces, shares))
    cross = (numer / denom).astype(bf16)
    part2 = project(cross, woc[...])
    for i in range(2):
        p_buf[0, i] = part2[:, i * half:(i + 1) * half]
    a = swap_halves(1, p_buf.at[0])
    c = finish(1, share(1, p_buf[0, core], a))
    hidden = hidden + whole(1, c)
    normed = layer_norm(hidden, gain3_ref[...], bias3_ref[...])
    up = jnp.dot(normed, wup[...], preferred_element_type=f32)
    up = (0.5 * up * (1.0 + lax.erf(up * (2.0 ** -0.5)))).astype(bf16)
    part3 = project(up, wdn[...])
    for i in range(2):
        p_buf[1, i] = part3[:, i * half:(i + 1) * half]
    a = swap_halves(2, p_buf.at[1])
    c = finish(2, share(2, p_buf[1, core], a))
    out_ref[...] = (hidden + whole(2, c)).astype(bf16)
    with jax.named_scope('drain'):
        for copy in sends:
            copy.wait_send()


def post_attention(part, x, gain2, bias2, gain3, bias3, enc, weights, wq_c, wo_c, w_up, w_down):
    batch, model = x.shape
    f32, bf16 = jnp.float32, jnp.bfloat16
    vmem = pl.BlockSpec(memory_space=pltpu.VMEM)
    tokens = enc.shape[1]
    side = 2 * HEADS_DIM
    dma = pltpu.SemaphoreType.DMA
    return pl.pallas_call(
        post_kernel,
        out_shape=jax.ShapeDtypeStruct((batch, model), bf16),
        in_specs=[vmem] * 15,
        out_specs=vmem,
        scratch_shapes=[
            pltpu.VMEM((batch, tokens, model), bf16),
            pltpu.VMEM((batch, 2 * tokens, 4 * side), bf16), pltpu.VMEM((batch, 2 * tokens, 4 * side), bf16),
            pltpu.VMEM((4, batch, side), bf16), pltpu.VMEM((4, 2 * batch, side), f32), pltpu.VMEM((4, 2 * batch, side), f32),
            pltpu.VMEM((2, 2, batch, model // 2), bf16), pltpu.VMEM((3, batch, model // 2), bf16),
            pltpu.VMEM((3, 4, batch, model // 2), bf16), pltpu.VMEM((3, 2, batch, model // 2), bf16),
            dma((2,)), dma((3,)), dma((3,)), dma((3, 4)), dma((3, 4)), dma((3,)), dma((3,)), dma((4,)), dma((4,)), dma((4,)), dma((4,)),
        ],
        compiler_params=pltpu.CompilerParams(collective_id=0, has_side_effects=True, vmem_limit_bytes=24 << 20),
        cost_estimate=pl.CostEstimate(flops=2 * batch * 2 * tokens * model * 8 * side, bytes_accessed=9 << 20, transcendentals=0),
        name="post_attention",
    )(part, x, gain2.reshape(1, model), bias2.reshape(1, model), gain3.reshape(1, model), bias3.reshape(1, model),
      enc, *weights, wq_c, wo_c, w_up, w_down)


def local_step(x, k_cache, v_cache, seq_lens, nbr_enc, ln1_gain, ln1_bias, w_q, w_k, w_v, w_o, ln2_gain, ln2_bias, wq_c, wk_c, wv_c, wo_c, ln3_gain, ln3_bias, w_up, w_down):
    mine = pack(wk_c, wv_c)
    weights = [mine] + [lax.ppermute(mine, 'tp', [(t, t ^ (2 * k)) for t in range(8)]) for k in (1, 2, 3)]
    part, k_new, v_new = self_attention(x, k_cache, v_cache, seq_lens, ln1_gain, ln1_bias, w_q, w_k, w_v, w_o)
    out = post_attention(part, x, ln2_gain, ln2_bias, ln3_gain, ln3_bias, nbr_enc, weights, wq_c, wo_c, w_up, w_down)
    return out, k_new, v_new


def solution(mesh):
    row_spec = P('dp', None)
    cache_spec = P('dp', None, 'tp', None)
    head_spec = P('dp', 'tp', None)
    vec_spec = P(None)
    col_split = P(None, 'tp')
    row_split = P('tp', None)
    in_specs = (row_spec, cache_spec, cache_spec, P('dp'), P('dp', 'tp', None), vec_spec, vec_spec, col_split, col_split, col_split, row_split, vec_spec, vec_spec, col_split, col_split, col_split, row_split, vec_spec, vec_spec, col_split, row_split)
    out_specs = (row_spec, head_spec, head_spec)
    return jax.shard_map(local_step, mesh=mesh, in_specs=in_specs, out_specs=out_specs, check_vma=False)
```

```python
import functools

import jax
import jax.numpy as jnp
from jax import lax
from jax.experimental import pallas as pl
from jax.experimental.pallas import tpu as pltpu
from jax.sharding import PartitionSpec as P

LN_EPS = 1e-5
CHUNK = 2048
SLOTS = 5
UNROLL = 2
NEG = -1e30
HEADS_DIM = 64
PROJ_ROWS = 512
GROUP = 4
MESH = pl.DeviceIdType.MESH


def layer_norm(values, ln_gain, ln_bias):
    row_mean = jnp.mean(values, axis=-1, keepdims=True)
    centred = values - row_mean
    row_var = jnp.mean(jnp.square(centred), axis=-1, keepdims=True)
    return (centred * lax.rsqrt(row_var + LN_EPS) * ln_gain + ln_bias).astype(jnp.bfloat16)


def project(operand, weight):
    return jnp.dot(operand, weight, preferred_element_type=jnp.float32).astype(jnp.bfloat16)


def self_kernel(lens_ref, x_hbm, gain_hbm, bias_hbm, wq_hbm, wk_hbm, wv_hbm, wo_hbm, k_hbm, v_hbm,
                part_ref, know_ref, vnow_ref,
                x_ref, gain_ref, bias_ref, wq_buf, wk_buf, wv_buf, wo_buf, k_buf, v_buf, q_all, p_buf, acc, mx, sm, row_tab, off_tab,
                w_sem, k_sem, v_sem):
    batch = x_ref.shape[0]
    dim = k_buf.shape[1]
    weights = [pltpu.make_async_copy(src, dst, w_sem.at[i]) for i, (src, dst) in enumerate(
        ((x_hbm, x_ref), (gain_hbm, gain_ref), (bias_hbm, bias_ref), (wq_hbm, wq_buf), (wk_hbm, wk_buf), (wv_hbm, wv_buf),
         (wo_hbm, wo_buf)))]
    for w in weights:
        w.start()

    def fetch(hbm, buf, sem, b):
        size = pl.multiple_of((lens_ref[b] + 127) // 128 * 128, 128)
        slot = lax.rem(b, SLOTS)
        return pltpu.make_async_copy(hbm.at[b, :, pl.ds(0, size)], buf.at[slot, :, pl.ds(0, size)], sem.at[slot])

    def fetch_k(b):
        return fetch(k_hbm, k_buf, k_sem, b)

    def fetch_v(b):
        return fetch(v_hbm, v_buf, v_sem, b)

    for b in range(SLOTS):
        k_buf[b] = jnp.zeros(k_buf.shape[1:], k_buf.dtype)
        fetch_k(b).start(priority=0)
        v_buf[b] = jnp.zeros(v_buf.shape[1:], v_buf.dtype)
        fetch_v(b).start(priority=1)

    def build_row(b, at):
        def build(j, at):
            row_tab[at] = b
            off_tab[at] = j * CHUNK
            return at + 1
        return lax.fori_loop(0, (lens_ref[b] + CHUNK - 1) // CHUNK, build, at)

    items = lax.fori_loop(0, batch, build_row, jnp.int32(0))
    groups = (items + UNROLL - 1) // UNROLL
    for extra in range(2 * UNROLL + 1):
        row_tab[items + extra] = batch
        off_tab[items + extra] = 0

    for w in weights[:3]:
        w.wait()
    normed = layer_norm(x_ref[...].astype(jnp.float32), gain_ref[...], bias_ref[...])
    for w in weights[3:6]:
        w.wait()
    q_new = project(normed, wq_buf[...])
    k_new = project(normed, wk_buf[...])
    v_new = project(normed, wv_buf[...])
    half = dim // 2
    for h in range(2):
        know_ref[:, h, :] = k_new[:, h * half:(h + 1) * half]
        vnow_ref[:, h, :] = v_new[:, h * half:(h + 1) * half]
    lane = lax.broadcasted_iota(jnp.int32, (batch, 8, 2 * dim), 2)
    row = lax.broadcasted_iota(jnp.int32, (batch, 8, 2 * dim), 1)
    q_f = q_new.astype(jnp.float32)
    q_wide = jnp.where(lane // half == row, jnp.concatenate([q_f, q_f], axis=1)[:, None, :], 0.0)
    q_all[:batch] = jnp.where(lane // half == row, jnp.concatenate([q_f, q_f], axis=1)[:, None, :], 0.0).astype(jnp.bfloat16)
    q_all[batch] = jnp.zeros((8, 2 * dim), jnp.bfloat16)
    s_new = jnp.sum(q_wide[:, :, :dim] * k_new.astype(jnp.float32)[:, None, :], axis=-1, keepdims=True) * (half ** -0.5)
    new_row = row[:, :, :dim] < 2
    v_f = v_new.astype(jnp.float32)[:, None, :]
    mx[:batch] = jnp.where(new_row, s_new, NEG)
    sm[:batch] = jnp.where(new_row, 1.0, 0.0)
    acc[:batch, :, :dim] = jnp.where(new_row, v_f, 0.0)
    acc[:batch, :, dim:] = jnp.zeros((batch, 8, dim), jnp.float32)
    mx[batch] = jnp.zeros((8, dim), jnp.float32)
    sm[batch] = jnp.ones((8, dim), jnp.float32)
    acc[batch] = jnp.zeros((8, 2 * dim), jnp.float32)

    wing = CHUNK // 2
    spot = lax.broadcasted_iota(jnp.int32, (8, wing), 1) + lax.broadcasted_iota(jnp.int32, (8, wing), 0) // 2 * wing
    scale = half ** -0.5

    def chunk(buf, i):
        slot = lax.rem(row_tab[i], SLOTS)
        return jnp.concatenate([buf[slot, :, pl.ds(pl.multiple_of(off_tab[i] + w, wing), wing)] for w in (0, wing)], axis=0)

    def scores(i):
        b = row_tab[i]
        s = jnp.dot(q_all[b], chunk(k_buf, i), preferred_element_type=jnp.float32) * scale
        s = jnp.where(spot < lens_ref[jnp.minimum(b, batch - 1)] - off_tab[i], s, NEG)
        top = jnp.max(s, axis=-1, keepdims=True)
        e = jnp.exp(s - top)
        return e.astype(jnp.bfloat16), top, jnp.sum(e, axis=-1, keepdims=True)

    def merge(i, o, top, total):
        b = row_tab[i]
        old = mx[b]
        new = jnp.maximum(old, top)
        keep = jnp.exp(old - new)
        add = jnp.exp(top - new)
        mx[b] = new
        sm[b] = sm[b] * keep + total * add
        acc[b] = acc[b] * jnp.concatenate([keep, keep], axis=1) + o * jnp.concatenate([add, add], axis=1)

    def await_first(copy, i):
        @pl.when((off_tab[i] == 0) & (row_tab[i] < batch))
        def _():
            copy(row_tab[i]).wait()

    def refill_after(copy, i):
        @pl.when((off_tab[i + 1] == 0) & (row_tab[i] + SLOTS < batch))
        def _():
            copy(row_tab[i] + SLOTS).start(priority=0 if copy is fetch_k else 1)

    def score_group(g):
        out = [scores(g * UNROLL + u) for u in range(UNROLL)]
        return out, tuple(x for o in out for x in o[1:])

    def keep_weights(g, out):
        for u in range(UNROLL):
            p_buf[lax.rem(g, 2), u] = out[u][0]

    for u in range(UNROLL):
        await_first(fetch_k, u)
    first, stats = score_group(0)
    keep_weights(0, first)
    for u in range(UNROLL):
        refill_after(fetch_k, u)

    def step(g, stats):
        now, prev = g * UNROLL, (g - 1) * UNROLL
        for u in range(UNROLL):
            await_first(fetch_k, now + u)
        for u in range(UNROLL):
            await_first(fetch_v, prev + u)
        p_prev = [p_buf[lax.rem(g - 1, 2), u] for u in range(UNROLL)]
        out, new_stats = score_group(g)
        o = [lax.dot_general(p_prev[u], chunk(v_buf, prev + u), (((1,), (1,)), ((), ())), preferred_element_type=jnp.float32)
             for u in range(UNROLL)]
        for u in range(UNROLL):
            merge(prev + u, o[u], stats[2 * u], stats[2 * u + 1])
        keep_weights(g, out)
        for u in range(UNROLL):
            refill_after(fetch_k, now + u)
        for u in range(UNROLL):
            refill_after(fetch_v, prev + u)
        return new_stats

    lax.fori_loop(1, groups + 1, step, stats)

    lane2 = lax.broadcasted_iota(jnp.int32, (batch, dim), 1)

    def head(h):
        top_a, top_b = mx[:batch, h, :], mx[:batch, h + 2, :]
        top = jnp.maximum(top_a, top_b)
        share_a, share_b = jnp.exp(top_a - top), jnp.exp(top_b - top)
        numer = acc[:batch, h, :dim] * share_a + acc[:batch, h + 2, dim:] * share_b
        return numer / (sm[:batch, h, :] * share_a + sm[:batch, h + 2, :] * share_b)

    out = jnp.where(lane2 < half, head(0), head(1)).astype(jnp.bfloat16)
    weights[6].wait()
    part = project(out, wo_buf[...])
    cut = part_ref.shape[2]
    for i in range(2):
        part_ref[i] = part[:, i * cut:(i + 1) * cut]


def self_attention(x, k_cache, v_cache, seq_lens, gain, bias, w_q, w_k, w_v, w_o):
    batch, ctx, heads, head_dim = k_cache.shape
    dim = heads * head_dim
    model = x.shape[1]
    most = batch * (ctx // CHUNK) + 2 * UNROLL + 2
    k_t = k_cache.transpose(0, 2, 3, 1).reshape(batch, dim, ctx)
    v_t = v_cache.transpose(0, 2, 3, 1).reshape(batch, dim, ctx)
    vmem = pl.BlockSpec(memory_space=pltpu.VMEM)
    f32, bf16 = jnp.float32, jnp.bfloat16
    return pl.pallas_call(
        self_kernel,
        out_shape=(jax.ShapeDtypeStruct((2, batch, model // 2), bf16),
                   jax.ShapeDtypeStruct((batch, heads, head_dim), bf16),
                   jax.ShapeDtypeStruct((batch, heads, head_dim), bf16)),
        in_specs=[pl.BlockSpec(memory_space=pltpu.SMEM)] + [pl.BlockSpec(memory_space=pltpu.HBM)] * 9,
        out_specs=(vmem, vmem, vmem),
        scratch_shapes=[
            pltpu.VMEM((batch, model), bf16), pltpu.VMEM((1, model), f32), pltpu.VMEM((1, model), f32),
            pltpu.VMEM((model, dim), bf16), pltpu.VMEM((model, dim), bf16), pltpu.VMEM((model, dim), bf16),
            pltpu.VMEM((dim, model), bf16),
            pltpu.VMEM((SLOTS, dim, ctx), bf16), pltpu.VMEM((SLOTS, dim, ctx), bf16),
            pltpu.VMEM((batch + 1, 8, 2 * dim), bf16),
            pltpu.VMEM((2, UNROLL, 8, CHUNK // 2), bf16),
            pltpu.VMEM((batch + 1, 8, 2 * dim), f32), pltpu.VMEM((batch + 1, 8, dim), f32), pltpu.VMEM((batch + 1, 8, dim), f32),
            pltpu.SMEM((most,), jnp.int32), pltpu.SMEM((most,), jnp.int32),
            pltpu.SemaphoreType.DMA((7,)), pltpu.SemaphoreType.DMA((SLOTS,)), pltpu.SemaphoreType.DMA((SLOTS,)),
        ],
        cost_estimate=pl.CostEstimate(flops=2 * 2 * batch * ctx * dim * 8, bytes_accessed=batch * ctx * dim * 2, transcendentals=0),
        compiler_params=pltpu.CompilerParams(vmem_limit_bytes=32 << 20),
        name="self_attention",
    )(*[pltpu.with_memory_space_constraint(v, pltpu.HBM)
        for v in (seq_lens, x, gain.reshape(1, model), bias.reshape(1, model), w_q, w_k, w_v, w_o, k_t, v_t)])


def pack_kernel(a_hbm, b_hbm, out_ref, sem):
    width = a_hbm.shape[1]
    copies = [pltpu.make_async_copy(src, out_ref.at[:, pl.ds(i * width, width)], sem.at[i]) for i, src in enumerate((a_hbm, b_hbm))]
    for copy in copies:
        copy.start()
    for copy in copies:
        copy.wait()


def pack(*parts):
    model, width = parts[0].shape
    return pl.pallas_call(
        pack_kernel,
        out_shape=jax.ShapeDtypeStruct((model, 2 * width), parts[0].dtype),
        in_specs=[pl.BlockSpec(memory_space=pltpu.HBM)] * 2,
        out_specs=pl.BlockSpec(memory_space=pltpu.VMEM),
        scratch_shapes=[pltpu.SemaphoreType.DMA((2,))],
        compiler_params=pltpu.CompilerParams(vmem_limit_bytes=8 << 20),
        name="pack_weights",
    )(*[pltpu.with_memory_space_constraint(v, pltpu.HBM) for v in parts])


def post_kernel(part_ref, x_ref, gain2_ref, bias2_ref, gain3_ref, bias3_ref, enc, w0, w1, w2, w3, wqc, woc, wup, wdn, out_ref,
                mate_ref, k_all, v_all, q_buf, o_out, o_in, p_buf, a_buf, b_buf, c_buf,
                e_sem, a_send, a_recv, b_send, b_recv, c_send, c_recv, q_send, q_recv, o_send, o_recv):
    f32, bf16 = jnp.float32, jnp.bfloat16
    batch, model = x_ref.shape
    half = model // 2
    me = lax.axis_index('tp')
    chip, core = me // 2, me % 2
    chip_y, chip_x = chip // 2, chip % 2
    mate = 2 * chip + 1 - core

    def other(k):
        return 2 * (2 * (1 - chip_y if k // 2 else chip_y) + (1 - chip_x if k % 2 else chip_x)) + core

    barrier = pltpu.get_barrier_semaphore()
    for device in (other(3), other(2), other(1), mate):
        pl.semaphore_signal(barrier, inc=1, device_id={'tp': device}, device_id_type=MESH)
    with jax.named_scope('barrier'):
        pl.semaphore_wait(barrier, 4)

    sends = []

    def send(src, dst, send_sem, recv_sem, device):
        copy = pltpu.make_async_remote_copy(src_ref=src, dst_ref=dst, send_sem=send_sem, recv_sem=recv_sem,
                                            device_id={'tp': device}, device_id_type=MESH)
        copy.start()
        sends.append(copy)
        return copy

    def swap_halves(n, parts):
        return send(parts.at[1 - core], a_buf.at[n], a_send.at[n], a_recv.at[n], mate)

    def share(n, mine, copy):
        with jax.named_scope('mate_half'):
            copy.wait_recv()
        b_buf[n, chip] = (mine.astype(f32) + a_buf[n].astype(f32)).astype(bf16)
        return [send(b_buf.at[n, chip], b_buf.at[n, chip], b_send.at[n, k], b_recv.at[n, k], other(k)) for k in (3, 2, 1)]

    def finish(n, copies):
        with jax.named_scope('chip_sums'):
            for copy in copies:
                copy.wait_recv()
        total = b_buf[n, 0].astype(f32)
        for i in range(1, 4):
            total = total + b_buf[n, i].astype(f32)
        c_buf[n, core] = total.astype(bf16)
        return send(c_buf.at[n, core], c_buf.at[n, core], c_send.at[n], c_recv.at[n], mate)

    def whole(n, copy):
        with jax.named_scope('mate_sum'):
            copy.wait_recv()
        return jnp.concatenate([c_buf[n, 0], c_buf[n, 1]], axis=1).astype(f32)

    tokens = enc.shape[1]
    rows = PROJ_ROWS
    per = rows // tokens
    side = 2 * HEADS_DIM
    wide = 4 * side

    def weight(i):
        return jnp.concatenate([w[:, i * side:(i + 1) * side] for w in (w0, w1, w2, w3)], axis=1)

    def project_tokens(source, place, i, dest):
        def body(j, _):
            lines = source[pl.ds(j * per, per)].reshape(rows, model)
            got = project(lines, weight(i)).reshape(per, tokens, wide)
            dest[pl.ds(j * per, per), place * tokens:(place + 1) * tokens, :] = got
            return 0
        lax.fori_loop(0, batch // per, body, 0)

    a = swap_halves(0, part_ref)
    e = send(enc, mate_ref, e_sem.at[0], e_sem.at[1], mate)
    b = share(0, part_ref[core], a)
    project_tokens(enc, 0, 0, k_all)
    project_tokens(enc, 0, 1, v_all)
    c = finish(0, b)
    hidden = x_ref[...].astype(f32) + whole(0, c)
    normed = layer_norm(hidden, gain2_ref[...], bias2_ref[...])
    q_buf[0] = project(normed, wqc[...])
    qs = [send(q_buf.at[0], q_buf.at[k], q_send.at[k], q_recv.at[k], other(k)) for k in (3, 2, 1)]
    with jax.named_scope('mate_tokens'):
        e.wait_recv()
    project_tokens(mate_ref, 1, 0, k_all)
    project_tokens(mate_ref, 1, 1, v_all)
    with jax.named_scope('other_heads'):
        for copy in qs:
            copy.wait_recv()
    q_eight = jnp.concatenate([q_buf[k] for k in range(4)], axis=1).astype(f32)
    many = 8 * GROUP
    col = lax.broadcasted_iota(jnp.int32, (many, wide), 1)
    line = lax.broadcasted_iota(jnp.int32, (many, wide), 0)
    own = col // HEADS_DIM == line % 8
    span = GROUP * 2 * tokens
    match = lax.broadcasted_iota(jnp.int32, (many, span), 1) // (2 * tokens) == lax.broadcasted_iota(jnp.int32, (many, span), 0) // 8
    nt = (((1,), (1,)), ((), ()))
    scale = HEADS_DIM ** -0.5

    def squeeze(values):
        return jnp.sum(jnp.where(own, values, 0.0).reshape(GROUP, 8, wide), axis=1)

    for g in range(batch // GROUP):
        at = slice(g * GROUP, (g + 1) * GROUP)
        q_g = jnp.broadcast_to(q_eight[at][:, None, :], (GROUP, 8, wide)).reshape(many, wide)
        q_g = jnp.where(own, q_g, 0.0).astype(bf16)
        s = lax.dot_general(q_g, k_all[at].reshape(span, wide), nt, preferred_element_type=f32) * scale
        s = jnp.where(match, s, NEG)
        top = jnp.max(s, axis=-1, keepdims=True)
        p = jnp.exp(s - top)
        total = jnp.sum(p, axis=-1, keepdims=True)
        o = squeeze(jnp.dot(p.astype(bf16), v_all[at].reshape(span, wide), preferred_element_type=f32))
        stat = squeeze(jnp.where(col % HEADS_DIM < HEADS_DIM // 2, top, total))
        for k in range(4):
            o_out[k, g * GROUP:(g + 1) * GROUP, :] = o[:, k * side:(k + 1) * side]
            o_out[k, batch + g * GROUP:batch + (g + 1) * GROUP, :] = stat[:, k * side:(k + 1) * side]
    os = [send(o_out.at[k], o_in.at[k], o_send.at[k], o_recv.at[k], other(k)) for k in (3, 2, 1)]
    with jax.named_scope('partial_heads'):
        for copy in os:
            copy.wait_recv()
    low = lax.broadcasted_iota(jnp.int32, (batch, side), 1) < HEADS_DIM
    middle = HEADS_DIM // 2

    def spread(stat, at):
        return jnp.where(low, stat[:, at:at + 1], stat[:, HEADS_DIM + at:HEADS_DIM + at + 1])

    pieces = [o_out[0]] + [o_in[k] for k in range(1, 4)]
    top_of = [spread(p[batch:], 0) for p in pieces]
    sum_of = [spread(p[batch:], middle) for p in pieces]
    top = functools.reduce(jnp.maximum, top_of)
    shares = [jnp.exp(t - top) for t in top_of]
    denom = sum(s * w for s, w in zip(sum_of, shares))
    numer = sum(p[:batch] * w for p, w in zip(pieces, shares))
    cross = (numer / denom).astype(bf16)
    part2 = project(cross, woc[...])
    for i in range(2):
        p_buf[0, i] = part2[:, i * half:(i + 1) * half]
    a = swap_halves(1, p_buf.at[0])
    c = finish(1, share(1, p_buf[0, core], a))
    hidden = hidden + whole(1, c)
    normed = layer_norm(hidden, gain3_ref[...], bias3_ref[...])
    up = jnp.dot(normed, wup[...], preferred_element_type=f32)
    up = (0.5 * up * (1.0 + lax.erf(up * (2.0 ** -0.5)))).astype(bf16)
    part3 = project(up, wdn[...])
    for i in range(2):
        p_buf[1, i] = part3[:, i * half:(i + 1) * half]
    a = swap_halves(2, p_buf.at[1])
    c = finish(2, share(2, p_buf[1, core], a))
    out_ref[...] = (hidden + whole(2, c)).astype(bf16)
    with jax.named_scope('drain'):
        for copy in sends:
            copy.wait_send()


def post_attention(part, x, gain2, bias2, gain3, bias3, enc, weights, wq_c, wo_c, w_up, w_down):
    batch, model = x.shape
    f32, bf16 = jnp.float32, jnp.bfloat16
    vmem = pl.BlockSpec(memory_space=pltpu.VMEM)
    tokens = enc.shape[1]
    side = 2 * HEADS_DIM
    dma = pltpu.SemaphoreType.DMA
    return pl.pallas_call(
        post_kernel,
        out_shape=jax.ShapeDtypeStruct((batch, model), bf16),
        in_specs=[vmem] * 15,
        out_specs=vmem,
        scratch_shapes=[
            pltpu.VMEM((batch, tokens, model), bf16),
            pltpu.VMEM((batch, 2 * tokens, 4 * side), bf16), pltpu.VMEM((batch, 2 * tokens, 4 * side), bf16),
            pltpu.VMEM((4, batch, side), bf16), pltpu.VMEM((4, 2 * batch, side), f32), pltpu.VMEM((4, 2 * batch, side), f32),
            pltpu.VMEM((2, 2, batch, model // 2), bf16), pltpu.VMEM((3, batch, model // 2), bf16),
            pltpu.VMEM((3, 4, batch, model // 2), bf16), pltpu.VMEM((3, 2, batch, model // 2), bf16),
            dma((2,)), dma((3,)), dma((3,)), dma((3, 4)), dma((3, 4)), dma((3,)), dma((3,)), dma((4,)), dma((4,)), dma((4,)), dma((4,)),
        ],
        compiler_params=pltpu.CompilerParams(collective_id=0, has_side_effects=True, vmem_limit_bytes=24 << 20),
        cost_estimate=pl.CostEstimate(flops=2 * batch * 2 * tokens * model * 8 * side, bytes_accessed=9 << 20, transcendentals=0),
        name="post_attention",
    )(part, x, gain2.reshape(1, model), bias2.reshape(1, model), gain3.reshape(1, model), bias3.reshape(1, model),
      enc, *weights, wq_c, wo_c, w_up, w_down)


def local_step(x, k_cache, v_cache, seq_lens, nbr_enc, ln1_gain, ln1_bias, w_q, w_k, w_v, w_o, ln2_gain, ln2_bias, wq_c, wk_c, wv_c, wo_c, ln3_gain, ln3_bias, w_up, w_down):
    mine = pack(wk_c, wv_c)
    weights = [mine] + [lax.ppermute(mine, 'tp', [(t, t ^ (2 * k)) for t in range(8)]) for k in (1, 2, 3)]
    part, k_new, v_new = self_attention(x, k_cache, v_cache, seq_lens, ln1_gain, ln1_bias, w_q, w_k, w_v, w_o)
    out = post_attention(part, x, ln2_gain, ln2_bias, ln3_gain, ln3_bias, nbr_enc, weights, wq_c, wo_c, w_up, w_down)
    return out, k_new, v_new


def solution(mesh):
    row_spec = P('dp', None)
    cache_spec = P('dp', None, 'tp', None)
    head_spec = P('dp', 'tp', None)
    vec_spec = P(None)
    col_split = P(None, 'tp')
    row_split = P('tp', None)
    in_specs = (row_spec, cache_spec, cache_spec, P('dp'), P('dp', 'tp', None), vec_spec, vec_spec, col_split, col_split, col_split, row_split, vec_spec, vec_spec, col_split, col_split, col_split, row_split, vec_spec, vec_spec, col_split, row_split)
    out_specs = (row_spec, head_spec, head_spec)
    return jax.shard_map(local_step, mesh=mesh, in_specs=in_specs, out_specs=out_specs, check_vma=False)
```

```python
import functools

import jax
import jax.numpy as jnp
from jax import lax
from jax.experimental import pallas as pl
from jax.experimental.pallas import tpu as pltpu
from jax.sharding import PartitionSpec as P

LN_EPS = 1e-5
CHUNK = 1024
SLOTS = 24
UNROLL = 4
NEG = -1e30
HEADS_DIM = 64
PROJ_ROWS = 512
GROUP = 4
MESH = pl.DeviceIdType.MESH


def layer_norm(values, ln_gain, ln_bias):
    row_mean = jnp.mean(values, axis=-1, keepdims=True)
    centred = values - row_mean
    row_var = jnp.mean(jnp.square(centred), axis=-1, keepdims=True)
    return (centred * lax.rsqrt(row_var + LN_EPS) * ln_gain + ln_bias).astype(jnp.bfloat16)


def project(operand, weight):
    return jnp.dot(operand, weight, preferred_element_type=jnp.float32).astype(jnp.bfloat16)


def self_kernel(lens_ref, x_hbm, gain_hbm, bias_hbm, wq_hbm, wk_hbm, wv_hbm, wo_hbm, k_hbm, v_hbm,
                part_ref, know_ref, vnow_ref,
                x_ref, gain_ref, bias_ref, wq_buf, wk_buf, wv_buf, wo_buf, k_buf, v_buf, q_all, p_buf, acc, mx, sm, row_tab, off_tab, rem_tab,
                w_sem, k_sem, v_sem):
    batch = x_ref.shape[0]
    dim = k_buf.shape[1]
    weights = [pltpu.make_async_copy(src, dst, w_sem.at[i]) for i, (src, dst) in enumerate(
        ((x_hbm, x_ref), (gain_hbm, gain_ref), (bias_hbm, bias_ref), (wq_hbm, wq_buf), (wk_hbm, wk_buf), (wv_hbm, wv_buf),
         (wo_hbm, wo_buf)))]
    for w in weights:
        w.start()

    def build(i, carry):
        b, start, left = carry
        row_tab[i] = b
        off_tab[i] = start
        rem_tab[i] = left
        more = left > CHUNK
        nb = jnp.minimum(b + 1, batch)
        fresh = lens_ref[jnp.minimum(nb, batch - 1)]
        return jnp.where(more, b, nb), jnp.where(more, start + CHUNK, 0), jnp.where(more, left - CHUNK, fresh)

    def fetch(hbm, buf, sem, i, slot, thread):
        b = jnp.minimum(row_tab[i], batch - 1)
        start = pl.multiple_of(off_tab[i], CHUNK)
        pltpu.make_async_copy(hbm.at[b, :, pl.ds(start, CHUNK)], buf.at[slot], sem.at[slot // UNROLL]).start(priority=thread)

    def await_group(hbm, buf, sem, slot):
        pltpu.make_async_copy(hbm.at[pl.ds(0, UNROLL), :, pl.ds(0, CHUNK)], buf.at[pl.ds(slot, UNROLL)], sem.at[slot // UNROLL]).wait()

    carry = (jnp.int32(0), jnp.int32(0), lens_ref[0])
    for i in range(SLOTS):
        carry = build(i, carry)
        fetch(k_hbm, k_buf, k_sem, i, i, 0)
        fetch(v_hbm, v_buf, v_sem, i, i, 1)

    def count(b, total):
        return total + (lens_ref[b] + CHUNK - 1) // CHUNK

    groups = (lax.fori_loop(0, batch, count, jnp.int32(0)) + UNROLL - 1) // UNROLL
    lax.fori_loop(SLOTS, (groups + 1) * UNROLL, build, carry)

    for w in weights[:3]:
        w.wait()
    normed = layer_norm(x_ref[...].astype(jnp.float32), gain_ref[...], bias_ref[...])
    for w in weights[3:6]:
        w.wait()
    q_new = project(normed, wq_buf[...])
    k_new = project(normed, wk_buf[...])
    v_new = project(normed, wv_buf[...])
    half = dim // 2
    for h in range(2):
        know_ref[:, h, :] = k_new[:, h * half:(h + 1) * half]
        vnow_ref[:, h, :] = v_new[:, h * half:(h + 1) * half]
    lane = lax.broadcasted_iota(jnp.int32, (batch, 8, dim), 2)
    row = lax.broadcasted_iota(jnp.int32, (batch, 8, dim), 1)
    q_f = q_new.astype(jnp.float32)
    for side in range(2):
        q_all[side, :batch] = jnp.where(lane // half + 2 * side == row, q_f[:, None, :], 0.0).astype(jnp.bfloat16)
        q_all[side, batch] = jnp.zeros((8, dim), jnp.bfloat16)
    own = lane // half == row
    s_new = jnp.sum(jnp.where(own, (q_f * k_new.astype(jnp.float32))[:, None, :], 0.0), axis=-1, keepdims=True) * (half ** -0.5)
    new_row = row < 2
    mx[:batch] = jnp.where(new_row, s_new, NEG)
    sm[:batch] = jnp.where(new_row, 1.0, 0.0)
    acc[:batch] = jnp.where(new_row, v_new.astype(jnp.float32)[:, None, :], 0.0)
    mx[batch] = jnp.zeros((8, dim), jnp.float32)
    sm[batch] = jnp.ones((8, dim), jnp.float32)
    acc[batch] = jnp.zeros((8, dim), jnp.float32)

    spot = lax.broadcasted_iota(jnp.int32, (8, CHUNK), 1)
    line = lax.broadcasted_iota(jnp.int32, (8, CHUNK), 0)
    line1 = lax.broadcasted_iota(jnp.int32, (8, dim), 0)
    scale = half ** -0.5
    pairs = range(0, UNROLL, 2)

    def scores(i, slot):
        q_two = jnp.concatenate([q_all[0, row_tab[i]], q_all[1, row_tab[i + 1]]], axis=1)
        keys = jnp.concatenate([k_buf[slot], k_buf[slot + 1]], axis=0)
        s = jnp.dot(q_two, keys, preferred_element_type=jnp.float32) * scale
        s = jnp.where(spot < jnp.where(line < 2, rem_tab[i], rem_tab[i + 1]), s, NEG)
        top = jnp.max(s, axis=-1, keepdims=True)
        e = jnp.exp(s - top)
        return e.astype(jnp.bfloat16), top, jnp.sum(e, axis=-1, keepdims=True)

    def weigh(p, slot):
        values = jnp.concatenate([v_buf[slot], v_buf[slot + 1]], axis=0)
        return lax.dot_general(p, values, (((1,), (1,)), ((), ())), preferred_element_type=jnp.float32)

    def merge(i, o, top, total):
        for side in range(2):
            b = row_tab[i + side]
            mine = line1 // 2 == side
            top_s = jnp.where(mine, top, NEG)
            old = mx[b]
            new = jnp.maximum(old, top_s)
            keep = jnp.exp(old - new)
            add = jnp.exp(top_s - new)
            mx[b] = new
            sm[b] = sm[b] * keep + jnp.where(mine, total, 0.0) * add
            acc[b] = acc[b] * keep + jnp.where(mine, o[:, side * dim:(side + 1) * dim], 0.0) * add

    def score_group(g, slot):
        out = [scores(g * UNROLL + u, slot + u) for u in pairs]
        return out, tuple(x for o in out for x in o[1:])

    def keep_weights(g, out):
        for j, o in enumerate(out):
            p_buf[lax.rem(g, 2), j] = o[0]

    depth = SLOTS // UNROLL
    await_group(k_hbm, k_buf, k_sem, 0)
    first, stats = score_group(0, 0)
    keep_weights(0, first)
    for u in range(UNROLL):
        fetch(k_hbm, k_buf, k_sem, SLOTS + u, u, 0)

    def step(g, stats):
        now, prev = g * UNROLL, (g - 1) * UNROLL
        slot_a = lax.rem(g, depth) * UNROLL
        slot_b = lax.rem(g - 1, depth) * UNROLL

        @pl.when(g < groups)
        def _():
            await_group(k_hbm, k_buf, k_sem, slot_a)

        await_group(v_hbm, v_buf, v_sem, slot_b)
        p_prev = [p_buf[lax.rem(g - 1, 2), j] for j in range(len(pairs))]
        out, new_stats = score_group(g, slot_a)
        o = [weigh(p_prev[j], slot_b + u) for j, u in enumerate(pairs)]
        for j, u in enumerate(pairs):
            merge(prev + u, o[j], stats[2 * j], stats[2 * j + 1])
        keep_weights(g, out)

        @pl.when(g + depth < groups)
        def _():
            for u in range(UNROLL):
                fetch(k_hbm, k_buf, k_sem, now + SLOTS + u, slot_a + u, 0)

        @pl.when(g - 1 + depth < groups)
        def _():
            for u in range(UNROLL):
                fetch(v_hbm, v_buf, v_sem, prev + SLOTS + u, slot_b + u, 1)

        return new_stats

    lax.fori_loop(1, groups + 1, step, stats)

    lane2 = lax.broadcasted_iota(jnp.int32, (batch, dim), 1)

    def head(h):
        top_a, top_b = mx[:batch, h, :], mx[:batch, h + 2, :]
        top = jnp.maximum(top_a, top_b)
        share_a, share_b = jnp.exp(top_a - top), jnp.exp(top_b - top)
        numer = acc[:batch, h, :] * share_a + acc[:batch, h + 2, :] * share_b
        return numer / (sm[:batch, h, :] * share_a + sm[:batch, h + 2, :] * share_b)

    out = jnp.where(lane2 < half, head(0), head(1)).astype(jnp.bfloat16)
    weights[6].wait()
    part = project(out, wo_buf[...])
    cut = part_ref.shape[2]
    for i in range(2):
        part_ref[i] = part[:, i * cut:(i + 1) * cut]


def self_attention(x, k_cache, v_cache, seq_lens, gain, bias, w_q, w_k, w_v, w_o):
    batch, ctx, heads, head_dim = k_cache.shape
    dim = heads * head_dim
    model = x.shape[1]
    most = batch * (ctx // CHUNK) + 2 * UNROLL + 2
    k_t = k_cache.transpose(0, 2, 3, 1).reshape(batch, dim, ctx)
    v_t = v_cache.transpose(0, 2, 3, 1).reshape(batch, dim, ctx)
    vmem = pl.BlockSpec(memory_space=pltpu.VMEM)
    f32, bf16 = jnp.float32, jnp.bfloat16
    return pl.pallas_call(
        self_kernel,
        out_shape=(jax.ShapeDtypeStruct((2, batch, model // 2), bf16),
                   jax.ShapeDtypeStruct((batch, heads, head_dim), bf16),
                   jax.ShapeDtypeStruct((batch, heads, head_dim), bf16)),
        in_specs=[pl.BlockSpec(memory_space=pltpu.SMEM)] + [pl.BlockSpec(memory_space=pltpu.HBM)] * 9,
        out_specs=(vmem, vmem, vmem),
        scratch_shapes=[
            pltpu.VMEM((batch, model), bf16), pltpu.VMEM((1, model), f32), pltpu.VMEM((1, model), f32),
            pltpu.VMEM((model, dim), bf16), pltpu.VMEM((model, dim), bf16), pltpu.VMEM((model, dim), bf16),
            pltpu.VMEM((dim, model), bf16),
            pltpu.VMEM((SLOTS, dim, CHUNK), bf16), pltpu.VMEM((SLOTS, dim, CHUNK), bf16),
            pltpu.VMEM((2, batch + 1, 8, dim), bf16),
            pltpu.VMEM((2, UNROLL // 2, 8, CHUNK), bf16),
            pltpu.VMEM((batch + 1, 8, dim), f32), pltpu.VMEM((batch + 1, 8, dim), f32), pltpu.VMEM((batch + 1, 8, dim), f32),
            pltpu.SMEM((most,), jnp.int32), pltpu.SMEM((most,), jnp.int32), pltpu.SMEM((most,), jnp.int32),
            pltpu.SemaphoreType.DMA((7,)), pltpu.SemaphoreType.DMA((SLOTS // UNROLL,)), pltpu.SemaphoreType.DMA((SLOTS // UNROLL,)),
        ],
        cost_estimate=pl.CostEstimate(flops=2 * 2 * batch * ctx * dim * 8, bytes_accessed=batch * ctx * dim * 2, transcendentals=0),
        compiler_params=pltpu.CompilerParams(vmem_limit_bytes=32 << 20),
        name="self_attention",
    )(*[pltpu.with_memory_space_constraint(v, pltpu.HBM)
        for v in (seq_lens, x, gain.reshape(1, model), bias.reshape(1, model), w_q, w_k, w_v, w_o, k_t, v_t)])


def pack_kernel(a_hbm, b_hbm, out_ref, sem):
    width = a_hbm.shape[1]
    copies = [pltpu.make_async_copy(src, out_ref.at[:, pl.ds(i * width, width)], sem.at[i]) for i, src in enumerate((a_hbm, b_hbm))]
    for copy in copies:
        copy.start()
    for copy in copies:
        copy.wait()


def pack(*parts):
    model, width = parts[0].shape
    return pl.pallas_call(
        pack_kernel,
        out_shape=jax.ShapeDtypeStruct((model, 2 * width), parts[0].dtype),
        in_specs=[pl.BlockSpec(memory_space=pltpu.HBM)] * 2,
        out_specs=pl.BlockSpec(memory_space=pltpu.VMEM),
        scratch_shapes=[pltpu.SemaphoreType.DMA((2,))],
        compiler_params=pltpu.CompilerParams(vmem_limit_bytes=8 << 20),
        name="pack_weights",
    )(*[pltpu.with_memory_space_constraint(v, pltpu.HBM) for v in parts])


def post_kernel(part_ref, x_ref, gain2_ref, bias2_ref, gain3_ref, bias3_ref, enc, w0, w1, w2, w3, wqc, woc, wup, wdn, out_ref,
                mate_ref, k_all, v_all, q_buf, s_buf, w_buf, o_out, o_in, p_buf, a_buf, b_buf, c_buf,
                e_sem, a_send, a_recv, b_send, b_recv, c_send, c_recv, q_send, q_recv, o_send, o_recv):
    f32, bf16 = jnp.float32, jnp.bfloat16
    batch, model = x_ref.shape
    half = model // 2
    me = lax.axis_index('tp')
    chip, core = me // 2, me % 2
    chip_y, chip_x = chip // 2, chip % 2
    mate = 2 * chip + 1 - core

    def other(k):
        return 2 * (2 * (1 - chip_y if k // 2 else chip_y) + (1 - chip_x if k % 2 else chip_x)) + core

    barrier = pltpu.get_barrier_semaphore()
    for device in (other(3), other(2), other(1), mate):
        pl.semaphore_signal(barrier, inc=1, device_id={'tp': device}, device_id_type=MESH)
    with jax.named_scope('barrier'):
        pl.semaphore_wait(barrier, 4)

    sends = []

    def send(src, dst, send_sem, recv_sem, device):
        copy = pltpu.make_async_remote_copy(src_ref=src, dst_ref=dst, send_sem=send_sem, recv_sem=recv_sem,
                                            device_id={'tp': device}, device_id_type=MESH)
        copy.start()
        sends.append(copy)
        return copy

    def swap_halves(n, parts):
        return send(parts.at[1 - core], a_buf.at[n], a_send.at[n], a_recv.at[n], mate)

    def share(n, mine, copy):
        with jax.named_scope('mate_half'):
            copy.wait_recv()
        b_buf[n, chip] = (mine.astype(f32) + a_buf[n].astype(f32)).astype(bf16)
        return [send(b_buf.at[n, chip], b_buf.at[n, chip], b_send.at[n, k], b_recv.at[n, k], other(k)) for k in (3, 2, 1)]

    def finish(n, copies):
        with jax.named_scope('chip_sums'):
            for copy in copies:
                copy.wait_recv()
        total = b_buf[n, 0].astype(f32)
        for i in range(1, 4):
            total = total + b_buf[n, i].astype(f32)
        c_buf[n, core] = total.astype(bf16)
        return send(c_buf.at[n, core], c_buf.at[n, core], c_send.at[n], c_recv.at[n], mate)

    def whole(n, copy):
        with jax.named_scope('mate_sum'):
            copy.wait_recv()
        return jnp.concatenate([c_buf[n, 0], c_buf[n, 1]], axis=1).astype(f32)

    tokens = enc.shape[1]
    rows = PROJ_ROWS
    per = rows // tokens
    side = 2 * HEADS_DIM
    wide = 4 * side

    def weight(i):
        return jnp.concatenate([w[:, i * side:(i + 1) * side] for w in (w0, w1, w2, w3)], axis=1)

    def project_tokens(source, place, i, dest):
        def body(j, _):
            lines = source[pl.ds(j * per, per)].reshape(rows, model)
            got = project(lines, weight(i)).reshape(per, tokens, wide)
            dest[pl.ds(j * per, per), place * tokens:(place + 1) * tokens, :] = got
            return 0
        lax.fori_loop(0, batch // per, body, 0)

    a = swap_halves(0, part_ref)
    e = send(enc, mate_ref, e_sem.at[0], e_sem.at[1], mate)
    b = share(0, part_ref[core], a)
    project_tokens(enc, 0, 0, k_all)
    project_tokens(enc, 0, 1, v_all)
    c = finish(0, b)
    hidden = x_ref[...].astype(f32) + whole(0, c)
    normed = layer_norm(hidden, gain2_ref[...], bias2_ref[...])
    q_buf[0] = project(normed, wqc[...])
    qs = [send(q_buf.at[0], q_buf.at[k], q_send.at[k], q_recv.at[k], other(k)) for k in (3, 2, 1)]
    with jax.named_scope('mate_tokens'):
        e.wait_recv()
    project_tokens(mate_ref, 1, 0, k_all)
    project_tokens(mate_ref, 1, 1, v_all)
    with jax.named_scope('other_heads'):
        for copy in qs:
            copy.wait_recv()
    q_eight = jnp.concatenate([q_buf[k] for k in range(4)], axis=1).astype(f32)
    many = 8 * GROUP
    col = lax.broadcasted_iota(jnp.int32, (many, wide), 1)
    line = lax.broadcasted_iota(jnp.int32, (many, wide), 0)
    own = col // HEADS_DIM == line % 8
    span = GROUP * 2 * tokens
    match = lax.broadcasted_iota(jnp.int32, (many, span), 1) // (2 * tokens) == lax.broadcasted_iota(jnp.int32, (many, span), 0) // 8
    nt = (((1,), (1,)), ((), ()))
    scale = HEADS_DIM ** -0.5

    def squeeze(values):
        return jnp.sum(jnp.where(own, values, 0.0).reshape(GROUP, 8, wide), axis=1)

    groups = batch // GROUP
    for g in range(groups):
        at = slice(g * GROUP, (g + 1) * GROUP)
        q_g = jnp.broadcast_to(q_eight[at][:, None, :], (GROUP, 8, wide)).reshape(many, wide)
        q_g = jnp.where(own, q_g, 0.0).astype(bf16)
        s_buf[g] = lax.dot_general(q_g, k_all[at].reshape(span, wide), nt, preferred_element_type=f32)
    stats = []
    for g in range(groups):
        s = jnp.where(match, s_buf[g] * scale, NEG)
        top = jnp.max(s, axis=-1, keepdims=True)
        p = jnp.exp(s - top)
        w_buf[g] = p.astype(bf16)
        stats.append(squeeze(jnp.where(col % HEADS_DIM < HEADS_DIM // 2, top, jnp.sum(p, axis=-1, keepdims=True))))
    for g in range(groups):
        at = slice(g * GROUP, (g + 1) * GROUP)
        o = squeeze(jnp.dot(w_buf[g], v_all[at].reshape(span, wide), preferred_element_type=f32))
        for k in range(4):
            o_out[k, g * GROUP:(g + 1) * GROUP, :] = o[:, k * side:(k + 1) * side]
            o_out[k, batch + g * GROUP:batch + (g + 1) * GROUP, :] = stats[g][:, k * side:(k + 1) * side]
    os = [send(o_out.at[k], o_in.at[k], o_send.at[k], o_recv.at[k], other(k)) for k in (3, 2, 1)]
    with jax.named_scope('partial_heads'):
        for copy in os:
            copy.wait_recv()
    low = lax.broadcasted_iota(jnp.int32, (batch, side), 1) < HEADS_DIM
    middle = HEADS_DIM // 2

    def spread(stat, at):
        return jnp.where(low, stat[:, at:at + 1], stat[:, HEADS_DIM + at:HEADS_DIM + at + 1])

    pieces = [o_out[0]] + [o_in[k] for k in range(1, 4)]
    top_of = [spread(p[batch:], 0) for p in pieces]
    sum_of = [spread(p[batch:], middle) for p in pieces]
    top = functools.reduce(jnp.maximum, top_of)
    shares = [jnp.exp(t - top) for t in top_of]
    denom = sum(s * w for s, w in zip(sum_of, shares))
    numer = sum(p[:batch] * w for p, w in zip(pieces, shares))
    cross = (numer / denom).astype(bf16)
    part2 = project(cross, woc[...])
    for i in range(2):
        p_buf[0, i] = part2[:, i * half:(i + 1) * half]
    a = swap_halves(1, p_buf.at[0])
    c = finish(1, share(1, p_buf[0, core], a))
    hidden = hidden + whole(1, c)
    normed = layer_norm(hidden, gain3_ref[...], bias3_ref[...])
    up = jnp.dot(normed, wup[...], preferred_element_type=f32)
    up = (0.5 * up * (1.0 + lax.erf(up * (2.0 ** -0.5)))).astype(bf16)
    part3 = project(up, wdn[...])
    for i in range(2):
        p_buf[1, i] = part3[:, i * half:(i + 1) * half]
    a = swap_halves(2, p_buf.at[1])
    c = finish(2, share(2, p_buf[1, core], a))
    out_ref[...] = (hidden + whole(2, c)).astype(bf16)
    with jax.named_scope('drain'):
        for copy in sends:
            copy.wait_send()


def post_attention(part, x, gain2, bias2, gain3, bias3, enc, weights, wq_c, wo_c, w_up, w_down):
    batch, model = x.shape
    f32, bf16 = jnp.float32, jnp.bfloat16
    vmem = pl.BlockSpec(memory_space=pltpu.VMEM)
    tokens = enc.shape[1]
    side = 2 * HEADS_DIM
    dma = pltpu.SemaphoreType.DMA
    return pl.pallas_call(
        post_kernel,
        out_shape=jax.ShapeDtypeStruct((batch, model), bf16),
        in_specs=[vmem] * 15,
        out_specs=vmem,
        scratch_shapes=[
            pltpu.VMEM((batch, tokens, model), bf16),
            pltpu.VMEM((batch, 2 * tokens, 4 * side), bf16), pltpu.VMEM((batch, 2 * tokens, 4 * side), bf16),
            pltpu.VMEM((4, batch, side), bf16),
            pltpu.VMEM((batch // GROUP, 8 * GROUP, GROUP * 2 * tokens), f32), pltpu.VMEM((batch // GROUP, 8 * GROUP, GROUP * 2 * tokens), bf16),
            pltpu.VMEM((4, 2 * batch, side), f32), pltpu.VMEM((4, 2 * batch, side), f32),
            pltpu.VMEM((2, 2, batch, model // 2), bf16), pltpu.VMEM((3, batch, model // 2), bf16),
            pltpu.VMEM((3, 4, batch, model // 2), bf16), pltpu.VMEM((3, 2, batch, model // 2), bf16),
            dma((2,)), dma((3,)), dma((3,)), dma((3, 4)), dma((3, 4)), dma((3,)), dma((3,)), dma((4,)), dma((4,)), dma((4,)), dma((4,)),
        ],
        compiler_params=pltpu.CompilerParams(collective_id=0, has_side_effects=True, vmem_limit_bytes=24 << 20),
        cost_estimate=pl.CostEstimate(flops=2 * batch * 2 * tokens * model * 8 * side, bytes_accessed=9 << 20, transcendentals=0),
        name="post_attention",
    )(part, x, gain2.reshape(1, model), bias2.reshape(1, model), gain3.reshape(1, model), bias3.reshape(1, model),
      enc, *weights, wq_c, wo_c, w_up, w_down)


def local_step(x, k_cache, v_cache, seq_lens, nbr_enc, ln1_gain, ln1_bias, w_q, w_k, w_v, w_o, ln2_gain, ln2_bias, wq_c, wk_c, wv_c, wo_c, ln3_gain, ln3_bias, w_up, w_down):
    mine = pack(wk_c, wv_c)
    weights = [mine] + [lax.ppermute(mine, 'tp', [(t, t ^ (2 * k)) for t in range(8)]) for k in (1, 2, 3)]
    part, k_new, v_new = self_attention(x, k_cache, v_cache, seq_lens, ln1_gain, ln1_bias, w_q, w_k, w_v, w_o)
    out = post_attention(part, x, ln2_gain, ln2_bias, ln3_gain, ln3_bias, nbr_enc, weights, wq_c, wo_c, w_up, w_down)
    return out, k_new, v_new


def solution(mesh):
    row_spec = P('dp', None)
    cache_spec = P('dp', None, 'tp', None)
    head_spec = P('dp', 'tp', None)
    vec_spec = P(None)
    col_split = P(None, 'tp')
    row_split = P('tp', None)
    in_specs = (row_spec, cache_spec, cache_spec, P('dp'), P('dp', 'tp', None), vec_spec, vec_spec, col_split, col_split, col_split, row_split, vec_spec, vec_spec, col_split, col_split, col_split, row_split, vec_spec, vec_spec, col_split, row_split)
    out_specs = (row_spec, head_spec, head_spec)
    return jax.shard_map(local_step, mesh=mesh, in_specs=in_specs, out_specs=out_specs, check_vma=False)
```

```python
import functools

import jax
import jax.numpy as jnp
from jax import lax
from jax.experimental import pallas as pl
from jax.experimental.pallas import tpu as pltpu
from jax.sharding import PartitionSpec as P

LN_EPS = 1e-5
CHUNK = 1024
SLOTS = 24
UNROLL = 4
NEG = -1e30
HEADS_DIM = 64
PROJ_ROWS = 512
GROUP = 4
MESH = pl.DeviceIdType.MESH


def layer_norm(values, ln_gain, ln_bias):
    row_mean = jnp.mean(values, axis=-1, keepdims=True)
    centred = values - row_mean
    row_var = jnp.mean(jnp.square(centred), axis=-1, keepdims=True)
    return (centred * lax.rsqrt(row_var + LN_EPS) * ln_gain + ln_bias).astype(jnp.bfloat16)


def project(operand, weight):
    return jnp.dot(operand, weight, preferred_element_type=jnp.float32).astype(jnp.bfloat16)


def self_kernel(lens_ref, x_hbm, gain_hbm, bias_hbm, wq_hbm, wk_hbm, wv_hbm, wo_hbm, k_hbm, v_hbm,
                part_ref, know_ref, vnow_ref,
                x_ref, gain_ref, bias_ref, wq_buf, wk_buf, wv_buf, wo_buf, k_buf, v_buf, q_all, p_buf, acc, mx, sm, row_tab, src_tab, off_tab, rem_tab, size_tab,
                w_sem, k_sem, v_sem):
    batch = x_ref.shape[0]
    dim = k_buf.shape[1]
    weights = [pltpu.make_async_copy(src, dst, w_sem.at[i]) for i, (src, dst) in enumerate(
        ((x_hbm, x_ref), (gain_hbm, gain_ref), (bias_hbm, bias_ref), (wq_hbm, wq_buf), (wk_hbm, wk_buf), (wv_hbm, wv_buf),
         (wo_hbm, wo_buf)))]
    for w in weights:
        w.start()

    def build(i, carry):
        b, start, left = carry
        row_tab[i] = b
        src_tab[i] = jnp.minimum(b, batch - 1)
        off_tab[i] = start
        rem_tab[i] = left
        size_tab[i] = CHUNK if isinstance(i, int) else (jnp.minimum(left, CHUNK) + 127) & -128
        more = left > CHUNK
        nb = jnp.minimum(b + 1, batch)
        fresh = lens_ref[jnp.minimum(nb, batch - 1)]
        return jnp.where(more, b, nb), jnp.where(more, start + CHUNK, 0), jnp.where(more, left - CHUNK, fresh)

    def fetch(hbm, buf, sem, i, slot, u, thread):
        start = pl.multiple_of(off_tab[i], CHUNK)
        size = CHUNK if isinstance(i, int) else pl.multiple_of(size_tab[i], 128)
        pltpu.make_async_copy(
            hbm.at[src_tab[i], :, pl.ds(start, size)], buf.at[slot, :, pl.ds(u * CHUNK, size)], sem.at[slot]).start(priority=thread)

    def await_group(hbm, buf, sem, g, slot):
        size = pl.multiple_of(sum(size_tab[g * UNROLL + u] for u in range(UNROLL)), 128)
        pltpu.make_async_copy(hbm.at[0, :, pl.ds(0, size)], buf.at[slot, :, pl.ds(0, size)], sem.at[slot]).wait()

    carry = (jnp.int32(0), jnp.int32(0), lens_ref[0])
    for i in range(SLOTS):
        carry = build(i, carry)
        fetch(k_hbm, k_buf, k_sem, i, i // UNROLL, i % UNROLL, 0)
        fetch(v_hbm, v_buf, v_sem, i, i // UNROLL, i % UNROLL, 1)

    def count(b, total):
        return total + (lens_ref[b] + CHUNK - 1) // CHUNK

    groups = (lax.fori_loop(0, batch, count, jnp.int32(0)) + UNROLL - 1) // UNROLL
    lax.fori_loop(SLOTS, (groups + 1) * UNROLL, build, carry)

    for w in weights[:3]:
        w.wait()
    normed = layer_norm(x_ref[...].astype(jnp.float32), gain_ref[...], bias_ref[...])
    for w in weights[3:6]:
        w.wait()
    q_new = project(normed, wq_buf[...])
    k_new = project(normed, wk_buf[...])
    v_new = project(normed, wv_buf[...])
    half = dim // 2
    for h in range(2):
        know_ref[:, h, :] = k_new[:, h * half:(h + 1) * half]
        vnow_ref[:, h, :] = v_new[:, h * half:(h + 1) * half]
    lane = lax.broadcasted_iota(jnp.int32, (batch, 8, dim), 2)
    row = lax.broadcasted_iota(jnp.int32, (batch, 8, dim), 1)
    q_f = q_new.astype(jnp.float32)
    for side in range(2):
        q_all[side, :batch] = jnp.where(lane // half + 2 * side == row, q_f[:, None, :], 0.0).astype(jnp.bfloat16)
        q_all[side, batch] = jnp.zeros((8, dim), jnp.bfloat16)
    own = lane // half == row
    s_new = jnp.sum(jnp.where(own, (q_f * k_new.astype(jnp.float32))[:, None, :], 0.0), axis=-1, keepdims=True) * (half ** -0.5)
    new_row = row < 2
    mx[:batch] = jnp.where(new_row, s_new, NEG)
    sm[:batch] = jnp.where(new_row, 1.0, 0.0)
    acc[:batch] = jnp.where(new_row, v_new.astype(jnp.float32)[:, None, :], 0.0)
    mx[batch] = jnp.zeros((8, dim), jnp.float32)
    sm[batch] = jnp.ones((8, dim), jnp.float32)
    acc[batch] = jnp.zeros((8, dim), jnp.float32)

    spot = lax.broadcasted_iota(jnp.int32, (8, CHUNK), 1)
    line = lax.broadcasted_iota(jnp.int32, (8, CHUNK), 0)
    line1 = lax.broadcasted_iota(jnp.int32, (8, dim), 0)
    scale = half ** -0.5
    pairs = range(0, UNROLL, 2)

    def two(buf, slot, u):
        return jnp.concatenate([buf[slot, :, w * CHUNK:(w + 1) * CHUNK] for w in (u, u + 1)], axis=0)

    def scores(i, slot, u):
        q_two = jnp.concatenate([q_all[0, row_tab[i]], q_all[1, row_tab[i + 1]]], axis=1)
        s = jnp.dot(q_two, two(k_buf, slot, u), preferred_element_type=jnp.float32) * scale
        s = jnp.where(spot < jnp.where(line < 2, rem_tab[i], rem_tab[i + 1]), s, NEG)
        top = jnp.max(s, axis=-1, keepdims=True)
        e = jnp.exp(s - top)
        return e.astype(jnp.bfloat16), top, jnp.sum(e, axis=-1, keepdims=True)

    def weigh(p, slot, u):
        return lax.dot_general(p, two(v_buf, slot, u), (((1,), (1,)), ((), ())), preferred_element_type=jnp.float32)

    def merge(i, o, top, total):
        for side in range(2):
            b = row_tab[i + side]
            mine = line1 // 2 == side
            top_s = jnp.where(mine, top, NEG)
            old = mx[b]
            new = jnp.maximum(old, top_s)
            keep = jnp.exp(old - new)
            add = jnp.exp(top_s - new)
            mx[b] = new
            sm[b] = sm[b] * keep + jnp.where(mine, total, 0.0) * add
            acc[b] = acc[b] * keep + jnp.where(mine, o[:, side * dim:(side + 1) * dim], 0.0) * add

    def score_group(g, slot):
        out = [scores(g * UNROLL + u, slot, u) for u in pairs]
        return out, tuple(x for o in out for x in o[1:])

    def keep_weights(g, out):
        for j, o in enumerate(out):
            p_buf[lax.rem(g, 2), j] = o[0]

    depth = SLOTS // UNROLL
    await_group(k_hbm, k_buf, k_sem, 0, 0)
    first, stats = score_group(0, 0)
    keep_weights(0, first)
    for u in range(UNROLL):
        fetch(k_hbm, k_buf, k_sem, jnp.int32(SLOTS + u), 0, u, 0)

    def step(g, stats):
        now, prev = g * UNROLL, (g - 1) * UNROLL
        slot_a = lax.rem(g, depth)
        slot_b = lax.rem(g - 1, depth)

        @pl.when(g < groups)
        def _():
            await_group(k_hbm, k_buf, k_sem, g, slot_a)

        await_group(v_hbm, v_buf, v_sem, g - 1, slot_b)
        p_prev = [p_buf[lax.rem(g - 1, 2), j] for j in range(len(pairs))]
        out, new_stats = score_group(g, slot_a)
        o = [weigh(p_prev[j], slot_b, u) for j, u in enumerate(pairs)]
        for j, u in enumerate(pairs):
            merge(prev + u, o[j], stats[2 * j], stats[2 * j + 1])
        keep_weights(g, out)

        @pl.when(g + depth < groups)
        def _():
            for u in range(UNROLL):
                fetch(k_hbm, k_buf, k_sem, now + SLOTS + u, slot_a, u, 0)

        @pl.when(g - 1 + depth < groups)
        def _():
            for u in range(UNROLL):
                fetch(v_hbm, v_buf, v_sem, prev + SLOTS + u, slot_b, u, 1)

        return new_stats

    lax.fori_loop(1, groups + 1, step, stats)

    lane2 = lax.broadcasted_iota(jnp.int32, (batch, dim), 1)

    def head(h):
        top_a, top_b = mx[:batch, h, :], mx[:batch, h + 2, :]
        top = jnp.maximum(top_a, top_b)
        share_a, share_b = jnp.exp(top_a - top), jnp.exp(top_b - top)
        numer = acc[:batch, h, :] * share_a + acc[:batch, h + 2, :] * share_b
        return numer / (sm[:batch, h, :] * share_a + sm[:batch, h + 2, :] * share_b)

    out = jnp.where(lane2 < half, head(0), head(1)).astype(jnp.bfloat16)
    weights[6].wait()
    part = project(out, wo_buf[...])
    cut = part_ref.shape[2]
    for i in range(2):
        part_ref[i] = part[:, i * cut:(i + 1) * cut]


def self_attention(x, k_cache, v_cache, seq_lens, gain, bias, w_q, w_k, w_v, w_o):
    batch, ctx, heads, head_dim = k_cache.shape
    dim = heads * head_dim
    model = x.shape[1]
    most = batch * (ctx // CHUNK) + 2 * UNROLL + 2
    k_t = k_cache.transpose(0, 2, 3, 1).reshape(batch, dim, ctx)
    v_t = v_cache.transpose(0, 2, 3, 1).reshape(batch, dim, ctx)
    vmem = pl.BlockSpec(memory_space=pltpu.VMEM)
    f32, bf16 = jnp.float32, jnp.bfloat16
    return pl.pallas_call(
        self_kernel,
        out_shape=(jax.ShapeDtypeStruct((2, batch, model // 2), bf16),
                   jax.ShapeDtypeStruct((batch, heads, head_dim), bf16),
                   jax.ShapeDtypeStruct((batch, heads, head_dim), bf16)),
        in_specs=[pl.BlockSpec(memory_space=pltpu.SMEM)] + [pl.BlockSpec(memory_space=pltpu.HBM)] * 9,
        out_specs=(vmem, vmem, vmem),
        scratch_shapes=[
            pltpu.VMEM((batch, model), bf16), pltpu.VMEM((1, model), f32), pltpu.VMEM((1, model), f32),
            pltpu.VMEM((model, dim), bf16), pltpu.VMEM((model, dim), bf16), pltpu.VMEM((model, dim), bf16),
            pltpu.VMEM((dim, model), bf16),
            pltpu.VMEM((SLOTS // UNROLL, dim, UNROLL * CHUNK), bf16), pltpu.VMEM((SLOTS // UNROLL, dim, UNROLL * CHUNK), bf16),
            pltpu.VMEM((2, batch + 1, 8, dim), bf16),
            pltpu.VMEM((2, UNROLL // 2, 8, CHUNK), bf16),
            pltpu.VMEM((batch + 1, 8, dim), f32), pltpu.VMEM((batch + 1, 8, dim), f32), pltpu.VMEM((batch + 1, 8, dim), f32),
            *[pltpu.SMEM((most,), jnp.int32)] * 5,
            pltpu.SemaphoreType.DMA((7,)), pltpu.SemaphoreType.DMA((SLOTS // UNROLL,)), pltpu.SemaphoreType.DMA((SLOTS // UNROLL,)),
        ],
        cost_estimate=pl.CostEstimate(flops=2 * 2 * batch * ctx * dim * 8, bytes_accessed=batch * ctx * dim * 2, transcendentals=0),
        compiler_params=pltpu.CompilerParams(vmem_limit_bytes=32 << 20),
        name="self_attention",
    )(*[pltpu.with_memory_space_constraint(v, pltpu.HBM)
        for v in (seq_lens, x, gain.reshape(1, model), bias.reshape(1, model), w_q, w_k, w_v, w_o, k_t, v_t)])


def pack_kernel(a_hbm, b_hbm, out_ref, sem):
    width = a_hbm.shape[1]
    copies = [pltpu.make_async_copy(src, out_ref.at[:, pl.ds(i * width, width)], sem.at[i]) for i, src in enumerate((a_hbm, b_hbm))]
    for copy in copies:
        copy.start()
    for copy in copies:
        copy.wait()


def pack(*parts):
    model, width = parts[0].shape
    return pl.pallas_call(
        pack_kernel,
        out_shape=jax.ShapeDtypeStruct((model, 2 * width), parts[0].dtype),
        in_specs=[pl.BlockSpec(memory_space=pltpu.HBM)] * 2,
        out_specs=pl.BlockSpec(memory_space=pltpu.VMEM),
        scratch_shapes=[pltpu.SemaphoreType.DMA((2,))],
        compiler_params=pltpu.CompilerParams(vmem_limit_bytes=8 << 20),
        name="pack_weights",
    )(*[pltpu.with_memory_space_constraint(v, pltpu.HBM) for v in parts])


def post_kernel(part_ref, x_ref, gain2_ref, bias2_ref, gain3_ref, bias3_ref, enc, w0, w1, w2, w3, wqc, woc, wup, wdn, out_ref,
                mate_ref, k_all, v_all, q_buf, s_buf, w_buf, o_out, o_in, p_buf, a_buf, b_buf, c_buf,
                e_sem, a_send, a_recv, b_send, b_recv, c_send, c_recv, q_send, q_recv, o_send, o_recv):
    f32, bf16 = jnp.float32, jnp.bfloat16
    batch, model = x_ref.shape
    half = model // 2
    me = lax.axis_index('tp')
    chip, core = me // 2, me % 2
    chip_y, chip_x = chip // 2, chip % 2
    mate = 2 * chip + 1 - core

    def other(k):
        return 2 * (2 * (1 - chip_y if k // 2 else chip_y) + (1 - chip_x if k % 2 else chip_x)) + core

    barrier = pltpu.get_barrier_semaphore()
    for device in (other(3), other(2), other(1), mate):
        pl.semaphore_signal(barrier, inc=1, device_id={'tp': device}, device_id_type=MESH)
    with jax.named_scope('barrier'):
        pl.semaphore_wait(barrier, 4)

    sends = []

    def send(src, dst, send_sem, recv_sem, device):
        copy = pltpu.make_async_remote_copy(src_ref=src, dst_ref=dst, send_sem=send_sem, recv_sem=recv_sem,
                                            device_id={'tp': device}, device_id_type=MESH)
        copy.start()
        sends.append(copy)
        return copy

    def swap_halves(n, parts):
        return send(parts.at[1 - core], a_buf.at[n], a_send.at[n], a_recv.at[n], mate)

    def share(n, mine, copy):
        with jax.named_scope('mate_half'):
            copy.wait_recv()
        b_buf[n, chip] = (mine.astype(f32) + a_buf[n].astype(f32)).astype(bf16)
        return [send(b_buf.at[n, chip], b_buf.at[n, chip], b_send.at[n, k], b_recv.at[n, k], other(k)) for k in (3, 2, 1)]

    def finish(n, copies):
        with jax.named_scope('chip_sums'):
            for copy in copies:
                copy.wait_recv()
        total = b_buf[n, 0].astype(f32)
        for i in range(1, 4):
            total = total + b_buf[n, i].astype(f32)
        c_buf[n, core] = total.astype(bf16)
        return send(c_buf.at[n, core], c_buf.at[n, core], c_send.at[n], c_recv.at[n], mate)

    def whole(n, copy):
        with jax.named_scope('mate_sum'):
            copy.wait_recv()
        return jnp.concatenate([c_buf[n, 0], c_buf[n, 1]], axis=1).astype(f32)

    tokens = enc.shape[1]
    rows = PROJ_ROWS
    per = rows // tokens
    side = 2 * HEADS_DIM
    wide = 4 * side

    def weight(i):
        return jnp.concatenate([w[:, i * side:(i + 1) * side] for w in (w0, w1, w2, w3)], axis=1)

    def project_tokens(source, place, i, dest):
        def body(j, _):
            lines = source[pl.ds(j * per, per)].reshape(rows, model)
            got = project(lines, weight(i)).reshape(per, tokens, wide)
            dest[pl.ds(j * per, per), place * tokens:(place + 1) * tokens, :] = got
            return 0
        lax.fori_loop(0, batch // per, body, 0)

    a = swap_halves(0, part_ref)
    e = send(enc, mate_ref, e_sem.at[0], e_sem.at[1], mate)
    b = share(0, part_ref[core], a)
    project_tokens(enc, 0, 0, k_all)
    project_tokens(enc, 0, 1, v_all)
    c = finish(0, b)
    hidden = x_ref[...].astype(f32) + whole(0, c)
    normed = layer_norm(hidden, gain2_ref[...], bias2_ref[...])
    q_buf[0] = project(normed, wqc[...])
    qs = [send(q_buf.at[0], q_buf.at[k], q_send.at[k], q_recv.at[k], other(k)) for k in (3, 2, 1)]
    with jax.named_scope('mate_tokens'):
        e.wait_recv()
    project_tokens(mate_ref, 1, 0, k_all)
    project_tokens(mate_ref, 1, 1, v_all)
    with jax.named_scope('other_heads'):
        for copy in qs:
            copy.wait_recv()
    q_eight = jnp.concatenate([q_buf[k] for k in range(4)], axis=1).astype(f32)
    many = 8 * GROUP
    col = lax.broadcasted_iota(jnp.int32, (many, wide), 1)
    line = lax.broadcasted_iota(jnp.int32, (many, wide), 0)
    own = col // HEADS_DIM == line % 8
    span = GROUP * 2 * tokens
    match = lax.broadcasted_iota(jnp.int32, (many, span), 1) // (2 * tokens) == lax.broadcasted_iota(jnp.int32, (many, span), 0) // 8
    nt = (((1,), (1,)), ((), ()))
    scale = HEADS_DIM ** -0.5

    def squeeze(values):
        return jnp.sum(jnp.where(own, values, 0.0).reshape(GROUP, 8, wide), axis=1)

    groups = batch // GROUP
    for g in range(groups):
        at = slice(g * GROUP, (g + 1) * GROUP)
        q_g = jnp.broadcast_to(q_eight[at][:, None, :], (GROUP, 8, wide)).reshape(many, wide)
        q_g = jnp.where(own, q_g, 0.0).astype(bf16)
        s_buf[g] = lax.dot_general(q_g, k_all[at].reshape(span, wide), nt, preferred_element_type=f32)
    stats = []
    for g in range(groups):
        s = jnp.where(match, s_buf[g] * scale, NEG)
        top = jnp.max(s, axis=-1, keepdims=True)
        p = jnp.exp(s - top)
        w_buf[g] = p.astype(bf16)
        stats.append(squeeze(jnp.where(col % HEADS_DIM < HEADS_DIM // 2, top, jnp.sum(p, axis=-1, keepdims=True))))
    for g in range(groups):
        at = slice(g * GROUP, (g + 1) * GROUP)
        o = squeeze(jnp.dot(w_buf[g], v_all[at].reshape(span, wide), preferred_element_type=f32))
        for k in range(4):
            o_out[k, g * GROUP:(g + 1) * GROUP, :] = o[:, k * side:(k + 1) * side]
            o_out[k, batch + g * GROUP:batch + (g + 1) * GROUP, :] = stats[g][:, k * side:(k + 1) * side]
    os = [send(o_out.at[k], o_in.at[k], o_send.at[k], o_recv.at[k], other(k)) for k in (3, 2, 1)]
    with jax.named_scope('partial_heads'):
        for copy in os:
            copy.wait_recv()
    low = lax.broadcasted_iota(jnp.int32, (batch, side), 1) < HEADS_DIM
    middle = HEADS_DIM // 2

    def spread(stat, at):
        return jnp.where(low, stat[:, at:at + 1], stat[:, HEADS_DIM + at:HEADS_DIM + at + 1])

    pieces = [o_out[0]] + [o_in[k] for k in range(1, 4)]
    top_of = [spread(p[batch:], 0) for p in pieces]
    sum_of = [spread(p[batch:], middle) for p in pieces]
    top = functools.reduce(jnp.maximum, top_of)
    shares = [jnp.exp(t - top) for t in top_of]
    denom = sum(s * w for s, w in zip(sum_of, shares))
    numer = sum(p[:batch] * w for p, w in zip(pieces, shares))
    cross = (numer / denom).astype(bf16)
    part2 = project(cross, woc[...])
    for i in range(2):
        p_buf[0, i] = part2[:, i * half:(i + 1) * half]
    a = swap_halves(1, p_buf.at[0])
    c = finish(1, share(1, p_buf[0, core], a))
    hidden = hidden + whole(1, c)
    normed = layer_norm(hidden, gain3_ref[...], bias3_ref[...])
    up = jnp.dot(normed, wup[...], preferred_element_type=f32)
    up = (0.5 * up * (1.0 + lax.erf(up * (2.0 ** -0.5)))).astype(bf16)
    part3 = project(up, wdn[...])
    for i in range(2):
        p_buf[1, i] = part3[:, i * half:(i + 1) * half]
    a = swap_halves(2, p_buf.at[1])
    c = finish(2, share(2, p_buf[1, core], a))
    out_ref[...] = (hidden + whole(2, c)).astype(bf16)
    with jax.named_scope('drain'):
        for copy in sends:
            copy.wait_send()


def post_attention(part, x, gain2, bias2, gain3, bias3, enc, weights, wq_c, wo_c, w_up, w_down):
    batch, model = x.shape
    f32, bf16 = jnp.float32, jnp.bfloat16
    vmem = pl.BlockSpec(memory_space=pltpu.VMEM)
    tokens = enc.shape[1]
    side = 2 * HEADS_DIM
    dma = pltpu.SemaphoreType.DMA
    return pl.pallas_call(
        post_kernel,
        out_shape=jax.ShapeDtypeStruct((batch, model), bf16),
        in_specs=[vmem] * 15,
        out_specs=vmem,
        scratch_shapes=[
            pltpu.VMEM((batch, tokens, model), bf16),
            pltpu.VMEM((batch, 2 * tokens, 4 * side), bf16), pltpu.VMEM((batch, 2 * tokens, 4 * side), bf16),
            pltpu.VMEM((4, batch, side), bf16),
            pltpu.VMEM((batch // GROUP, 8 * GROUP, GROUP * 2 * tokens), f32), pltpu.VMEM((batch // GROUP, 8 * GROUP, GROUP * 2 * tokens), bf16),
            pltpu.VMEM((4, 2 * batch, side), f32), pltpu.VMEM((4, 2 * batch, side), f32),
            pltpu.VMEM((2, 2, batch, model // 2), bf16), pltpu.VMEM((3, batch, model // 2), bf16),
            pltpu.VMEM((3, 4, batch, model // 2), bf16), pltpu.VMEM((3, 2, batch, model // 2), bf16),
            dma((2,)), dma((3,)), dma((3,)), dma((3, 4)), dma((3, 4)), dma((3,)), dma((3,)), dma((4,)), dma((4,)), dma((4,)), dma((4,)),
        ],
        compiler_params=pltpu.CompilerParams(collective_id=0, has_side_effects=True, vmem_limit_bytes=24 << 20),
        cost_estimate=pl.CostEstimate(flops=2 * batch * 2 * tokens * model * 8 * side, bytes_accessed=9 << 20, transcendentals=0),
        name="post_attention",
    )(part, x, gain2.reshape(1, model), bias2.reshape(1, model), gain3.reshape(1, model), bias3.reshape(1, model),
      enc, *weights, wq_c, wo_c, w_up, w_down)


def local_step(x, k_cache, v_cache, seq_lens, nbr_enc, ln1_gain, ln1_bias, w_q, w_k, w_v, w_o, ln2_gain, ln2_bias, wq_c, wk_c, wv_c, wo_c, ln3_gain, ln3_bias, w_up, w_down):
    mine = pack(wk_c, wv_c)
    weights = [mine] + [lax.ppermute(mine, 'tp', [(t, t ^ (2 * k)) for t in range(8)]) for k in (1, 2, 3)]
    part, k_new, v_new = self_attention(x, k_cache, v_cache, seq_lens, ln1_gain, ln1_bias, w_q, w_k, w_v, w_o)
    out = post_attention(part, x, ln2_gain, ln2_bias, ln3_gain, ln3_bias, nbr_enc, weights, wq_c, wo_c, w_up, w_down)
    return out, k_new, v_new


def solution(mesh):
    row_spec = P('dp', None)
    cache_spec = P('dp', None, 'tp', None)
    head_spec = P('dp', 'tp', None)
    vec_spec = P(None)
    col_split = P(None, 'tp')
    row_split = P('tp', None)
    in_specs = (row_spec, cache_spec, cache_spec, P('dp'), P('dp', 'tp', None), vec_spec, vec_spec, col_split, col_split, col_split, row_split, vec_spec, vec_spec, col_split, col_split, col_split, row_split, vec_spec, vec_spec, col_split, row_split)
    out_specs = (row_spec, head_spec, head_spec)
    return jax.shard_map(local_step, mesh=mesh, in_specs=in_specs, out_specs=out_specs, check_vma=False)
```

```python
import functools

import jax
import jax.numpy as jnp
from jax import lax
from jax.experimental import pallas as pl
from jax.experimental.pallas import tpu as pltpu
from jax.sharding import PartitionSpec as P

LN_EPS = 1e-5
CHUNK = 1024
SLOTS = 24
UNROLL = 4
NEG = -1e30
HEADS_DIM = 64
PROJ_ROWS = 512
GROUP = 4
MESH = pl.DeviceIdType.MESH


def layer_norm(values, ln_gain, ln_bias):
    row_mean = jnp.mean(values, axis=-1, keepdims=True)
    centred = values - row_mean
    row_var = jnp.mean(jnp.square(centred), axis=-1, keepdims=True)
    return (centred * lax.rsqrt(row_var + LN_EPS) * ln_gain + ln_bias).astype(jnp.bfloat16)


def project(operand, weight):
    return jnp.dot(operand, weight, preferred_element_type=jnp.float32).astype(jnp.bfloat16)


def self_kernel(lens_hbm, x_hbm, gain_hbm, bias_hbm, wq_hbm, wk_hbm, wv_hbm, wo_hbm, k_hbm, v_hbm,
                part_ref, know_ref, vnow_ref,
                lens_ref, x_ref, gain_ref, bias_ref, wq_buf, wk_buf, wv_buf, wo_buf, k_buf, v_buf, q_all, p_buf, acc, mx, sm, row_tab, src_tab, off_tab, rem_tab, size_tab,
                w_sem, k_sem, v_sem):
    batch = x_ref.shape[0]
    dim = k_buf.shape[1]
    weights = [pltpu.make_async_copy(src, dst, w_sem.at[i]) for i, (src, dst) in enumerate(
        ((lens_hbm, lens_ref), (x_hbm, x_ref), (gain_hbm, gain_ref), (bias_hbm, bias_ref), (wq_hbm, wq_buf), (wk_hbm, wk_buf), (wv_hbm, wv_buf),
         (wo_hbm, wo_buf)))]
    for w in weights:
        w.start()

    def fetch(hbm, buf, sem, i, slot, u, thread):
        start = pl.multiple_of(off_tab[i], CHUNK)
        size = pl.multiple_of(size_tab[i], 128)
        pltpu.make_async_copy(
            hbm.at[src_tab[i], :, pl.ds(start, size)], buf.at[slot, :, pl.ds(u * CHUNK, size)], sem.at[slot]).start(priority=thread)

    def await_group(hbm, buf, sem, g, slot):
        size = pl.multiple_of(sum(size_tab[g * UNROLL + u] for u in range(UNROLL)), 128)
        pltpu.make_async_copy(hbm.at[0, :, pl.ds(0, size)], buf.at[slot, :, pl.ds(0, size)], sem.at[slot]).wait()

    for i in range(SLOTS):
        for hbm, buf, sem, thread in ((k_hbm, k_buf, k_sem, 0), (v_hbm, v_buf, v_sem, 1)):
            pltpu.make_async_copy(hbm.at[i, :, pl.ds(0, CHUNK)], buf.at[i // UNROLL, :, pl.ds(i % UNROLL * CHUNK, CHUNK)],
                                  sem.at[i // UNROLL]).start(priority=thread)
    weights[0].wait()

    def build(i, b, start):
        left = lens_ref[b] - start
        row_tab[i] = b
        src_tab[i] = b
        off_tab[i] = start
        rem_tab[i] = left
        return (jnp.minimum(left, CHUNK) + 127) & -128

    def build_first(b, _):
        size_tab[b] = jnp.where(b < SLOTS, CHUNK, build(b, b, 0))
        return 0

    def build_rest(b, at):
        def more(j, at):
            size_tab[at] = build(at, b, j * CHUNK)
            return at + 1
        return lax.fori_loop(1, (lens_ref[b] + CHUNK - 1) // CHUNK, more, at)

    lax.fori_loop(0, batch, build_first, 0)
    items = lax.fori_loop(0, batch, build_rest, jnp.int32(batch))
    groups = (items + UNROLL - 1) // UNROLL
    for extra in range(2 * UNROLL):
        row_tab[items + extra] = batch
        src_tab[items + extra] = batch - 1
        off_tab[items + extra] = 0
        rem_tab[items + extra] = 64
        size_tab[items + extra] = 128

    for w in weights[1:4]:
        w.wait()
    normed = layer_norm(x_ref[...].astype(jnp.float32), gain_ref[...], bias_ref[...])
    for w in weights[4:7]:
        w.wait()
    q_new = project(normed, wq_buf[...])
    k_new = project(normed, wk_buf[...])
    v_new = project(normed, wv_buf[...])
    half = dim // 2
    for h in range(2):
        know_ref[:, h, :] = k_new[:, h * half:(h + 1) * half]
        vnow_ref[:, h, :] = v_new[:, h * half:(h + 1) * half]
    lane = lax.broadcasted_iota(jnp.int32, (batch, 8, dim), 2)
    row = lax.broadcasted_iota(jnp.int32, (batch, 8, dim), 1)
    q_f = q_new.astype(jnp.float32)
    for side in range(2):
        q_all[side, :batch] = jnp.where(lane // half + 2 * side == row, q_f[:, None, :], 0.0).astype(jnp.bfloat16)
        q_all[side, batch] = jnp.zeros((8, dim), jnp.bfloat16)
    own = lane // half == row
    s_new = jnp.sum(jnp.where(own, (q_f * k_new.astype(jnp.float32))[:, None, :], 0.0), axis=-1, keepdims=True) * (half ** -0.5)
    new_row = row < 2
    mx[:batch] = jnp.where(new_row, s_new, NEG)
    sm[:batch] = jnp.where(new_row, 1.0, 0.0)
    acc[:batch] = jnp.where(new_row, v_new.astype(jnp.float32)[:, None, :], 0.0)
    mx[batch] = jnp.zeros((8, dim), jnp.float32)
    sm[batch] = jnp.ones((8, dim), jnp.float32)
    acc[batch] = jnp.zeros((8, dim), jnp.float32)

    spot = lax.broadcasted_iota(jnp.int32, (8, CHUNK), 1)
    line = lax.broadcasted_iota(jnp.int32, (8, CHUNK), 0)
    line1 = lax.broadcasted_iota(jnp.int32, (8, dim), 0)
    scale = half ** -0.5
    pairs = range(0, UNROLL, 2)

    def two(buf, slot, u):
        return jnp.concatenate([buf[slot, :, w * CHUNK:(w + 1) * CHUNK] for w in (u, u + 1)], axis=0)

    def scores(i, slot, u):
        q_two = jnp.concatenate([q_all[0, row_tab[i]], q_all[1, row_tab[i + 1]]], axis=1)
        s = jnp.dot(q_two, two(k_buf, slot, u), preferred_element_type=jnp.float32) * scale
        s = jnp.where(spot < jnp.where(line < 2, rem_tab[i], rem_tab[i + 1]), s, NEG)
        top = jnp.max(s, axis=-1, keepdims=True)
        e = jnp.exp(s - top)
        return e.astype(jnp.bfloat16), top, jnp.sum(e, axis=-1, keepdims=True)

    def weigh(p, slot, u):
        return lax.dot_general(p, two(v_buf, slot, u), (((1,), (1,)), ((), ())), preferred_element_type=jnp.float32)

    def merge(i, o, top, total):
        for side in range(2):
            b = row_tab[i + side]
            mine = line1 // 2 == side
            top_s = jnp.where(mine, top, NEG)
            old = mx[b]
            new = jnp.maximum(old, top_s)
            keep = jnp.exp(old - new)
            add = jnp.exp(top_s - new)
            mx[b] = new
            sm[b] = sm[b] * keep + jnp.where(mine, total, 0.0) * add
            acc[b] = acc[b] * keep + jnp.where(mine, o[:, side * dim:(side + 1) * dim], 0.0) * add

    def score_group(g, slot):
        out = [scores(g * UNROLL + u, slot, u) for u in pairs]
        return out, tuple(x for o in out for x in o[1:])

    def keep_weights(g, out):
        for j, o in enumerate(out):
            p_buf[lax.rem(g, 2), j] = o[0]

    depth = SLOTS // UNROLL
    await_group(k_hbm, k_buf, k_sem, 0, 0)
    first, stats = score_group(0, 0)
    keep_weights(0, first)
    for u in range(UNROLL):
        fetch(k_hbm, k_buf, k_sem, SLOTS + u, 0, u, 0)

    def step(g, stats):
        now, prev = g * UNROLL, (g - 1) * UNROLL
        slot_a = lax.rem(g, depth)
        slot_b = lax.rem(g - 1, depth)

        @pl.when(g < groups)
        def _():
            await_group(k_hbm, k_buf, k_sem, g, slot_a)

        await_group(v_hbm, v_buf, v_sem, g - 1, slot_b)
        p_prev = [p_buf[lax.rem(g - 1, 2), j] for j in range(len(pairs))]
        out, new_stats = score_group(g, slot_a)
        o = [weigh(p_prev[j], slot_b, u) for j, u in enumerate(pairs)]
        for j, u in enumerate(pairs):
            merge(prev + u, o[j], stats[2 * j], stats[2 * j + 1])
        keep_weights(g, out)

        @pl.when(g + depth < groups)
        def _():
            for u in range(UNROLL):
                fetch(k_hbm, k_buf, k_sem, now + SLOTS + u, slot_a, u, 0)

        @pl.when(g - 1 + depth < groups)
        def _():
            for u in range(UNROLL):
                fetch(v_hbm, v_buf, v_sem, prev + SLOTS + u, slot_b, u, 1)

        return new_stats

    lax.fori_loop(1, groups + 1, step, stats)

    lane2 = lax.broadcasted_iota(jnp.int32, (batch, dim), 1)

    def head(h):
        top_a, top_b = mx[:batch, h, :], mx[:batch, h + 2, :]
        top = jnp.maximum(top_a, top_b)
        share_a, share_b = jnp.exp(top_a - top), jnp.exp(top_b - top)
        numer = acc[:batch, h, :] * share_a + acc[:batch, h + 2, :] * share_b
        return numer / (sm[:batch, h, :] * share_a + sm[:batch, h + 2, :] * share_b)

    out = jnp.where(lane2 < half, head(0), head(1)).astype(jnp.bfloat16)
    weights[7].wait()
    part = project(out, wo_buf[...])
    cut = part_ref.shape[2]
    for i in range(2):
        part_ref[i] = part[:, i * cut:(i + 1) * cut]


def self_attention(x, k_cache, v_cache, seq_lens, gain, bias, w_q, w_k, w_v, w_o):
    batch, ctx, heads, head_dim = k_cache.shape
    dim = heads * head_dim
    model = x.shape[1]
    most = batch * (ctx // CHUNK) + 2 * UNROLL + 2
    k_t = k_cache.transpose(0, 2, 3, 1).reshape(batch, dim, ctx)
    v_t = v_cache.transpose(0, 2, 3, 1).reshape(batch, dim, ctx)
    vmem = pl.BlockSpec(memory_space=pltpu.VMEM)
    f32, bf16 = jnp.float32, jnp.bfloat16
    return pl.pallas_call(
        self_kernel,
        out_shape=(jax.ShapeDtypeStruct((2, batch, model // 2), bf16),
                   jax.ShapeDtypeStruct((batch, heads, head_dim), bf16),
                   jax.ShapeDtypeStruct((batch, heads, head_dim), bf16)),
        in_specs=[pl.BlockSpec(memory_space=pltpu.HBM)] * 10,
        out_specs=(vmem, vmem, vmem),
        scratch_shapes=[
            pltpu.SMEM((batch,), jnp.int32),
            pltpu.VMEM((batch, model), bf16), pltpu.VMEM((1, model), f32), pltpu.VMEM((1, model), f32),
            pltpu.VMEM((model, dim), bf16), pltpu.VMEM((model, dim), bf16), pltpu.VMEM((model, dim), bf16),
            pltpu.VMEM((dim, model), bf16),
            pltpu.VMEM((SLOTS // UNROLL, dim, UNROLL * CHUNK), bf16), pltpu.VMEM((SLOTS // UNROLL, dim, UNROLL * CHUNK), bf16),
            pltpu.VMEM((2, batch + 1, 8, dim), bf16),
            pltpu.VMEM((2, UNROLL // 2, 8, CHUNK), bf16),
            pltpu.VMEM((batch + 1, 8, dim), f32), pltpu.VMEM((batch + 1, 8, dim), f32), pltpu.VMEM((batch + 1, 8, dim), f32),
            *[pltpu.SMEM((most,), jnp.int32)] * 5,
            pltpu.SemaphoreType.DMA((8,)), pltpu.SemaphoreType.DMA((SLOTS // UNROLL,)), pltpu.SemaphoreType.DMA((SLOTS // UNROLL,)),
        ],
        cost_estimate=pl.CostEstimate(flops=2 * 2 * batch * ctx * dim * 8, bytes_accessed=batch * ctx * dim * 2, transcendentals=0),
        compiler_params=pltpu.CompilerParams(vmem_limit_bytes=32 << 20),
        name="self_attention",
    )(*[pltpu.with_memory_space_constraint(v, pltpu.HBM)
        for v in (seq_lens, x, gain.reshape(1, model), bias.reshape(1, model), w_q, w_k, w_v, w_o, k_t, v_t)])


def pack_kernel(a_hbm, b_hbm, out_ref, sem):
    width = a_hbm.shape[1]
    copies = [pltpu.make_async_copy(src, out_ref.at[:, pl.ds(i * width, width)], sem.at[i]) for i, src in enumerate((a_hbm, b_hbm))]
    for copy in copies:
        copy.start()
    for copy in copies:
        copy.wait()


def pack(*parts):
    model, width = parts[0].shape
    return pl.pallas_call(
        pack_kernel,
        out_shape=jax.ShapeDtypeStruct((model, 2 * width), parts[0].dtype),
        in_specs=[pl.BlockSpec(memory_space=pltpu.HBM)] * 2,
        out_specs=pl.BlockSpec(memory_space=pltpu.VMEM),
        scratch_shapes=[pltpu.SemaphoreType.DMA((2,))],
        compiler_params=pltpu.CompilerParams(vmem_limit_bytes=8 << 20),
        name="pack_weights",
    )(*[pltpu.with_memory_space_constraint(v, pltpu.HBM) for v in parts])


def post_kernel(part_ref, x_ref, gain2_ref, bias2_ref, gain3_ref, bias3_ref, enc, w0, w1, w2, w3, wqc, woc, wup, wdn, out_ref,
                mate_ref, k_all, v_all, q_buf, s_buf, w_buf, o_out, o_in, p_buf, a_buf, b_buf, c_buf,
                e_sem, a_send, a_recv, b_send, b_recv, c_send, c_recv, q_send, q_recv, o_send, o_recv):
    f32, bf16 = jnp.float32, jnp.bfloat16
    batch, model = x_ref.shape
    half = model // 2
    me = lax.axis_index('tp')
    chip, core = me // 2, me % 2
    chip_y, chip_x = chip // 2, chip % 2
    mate = 2 * chip + 1 - core

    def other(k):
        return 2 * (2 * (1 - chip_y if k // 2 else chip_y) + (1 - chip_x if k % 2 else chip_x)) + core

    barrier = pltpu.get_barrier_semaphore()
    for device in (other(3), other(2), other(1), mate):
        pl.semaphore_signal(barrier, inc=1, device_id={'tp': device}, device_id_type=MESH)
    with jax.named_scope('barrier'):
        pl.semaphore_wait(barrier, 4)

    sends = []

    def send(src, dst, send_sem, recv_sem, device):
        copy = pltpu.make_async_remote_copy(src_ref=src, dst_ref=dst, send_sem=send_sem, recv_sem=recv_sem,
                                            device_id={'tp': device}, device_id_type=MESH)
        copy.start()
        sends.append(copy)
        return copy

    def swap_halves(n, parts):
        return send(parts.at[1 - core], a_buf.at[n], a_send.at[n], a_recv.at[n], mate)

    def share(n, mine, copy):
        with jax.named_scope('mate_half'):
            copy.wait_recv()
        b_buf[n, chip] = (mine.astype(f32) + a_buf[n].astype(f32)).astype(bf16)
        return [send(b_buf.at[n, chip], b_buf.at[n, chip], b_send.at[n, k], b_recv.at[n, k], other(k)) for k in (3, 2, 1)]

    def finish(n, copies):
        with jax.named_scope('chip_sums'):
            for copy in copies:
                copy.wait_recv()
        total = b_buf[n, 0].astype(f32)
        for i in range(1, 4):
            total = total + b_buf[n, i].astype(f32)
        c_buf[n, core] = total.astype(bf16)
        return send(c_buf.at[n, core], c_buf.at[n, core], c_send.at[n], c_recv.at[n], mate)

    def whole(n, copy):
        with jax.named_scope('mate_sum'):
            copy.wait_recv()
        return jnp.concatenate([c_buf[n, 0], c_buf[n, 1]], axis=1).astype(f32)

    tokens = enc.shape[1]
    rows = PROJ_ROWS
    per = rows // tokens
    side = 2 * HEADS_DIM
    wide = 4 * side

    def weight(i):
        return jnp.concatenate([w[:, i * side:(i + 1) * side] for w in (w0, w1, w2, w3)], axis=1)

    def project_tokens(source, place, i, dest):
        def body(j, _):
            lines = source[pl.ds(j * per, per)].reshape(rows, model)
            got = project(lines, weight(i)).reshape(per, tokens, wide)
            dest[pl.ds(j * per, per), place * tokens:(place + 1) * tokens, :] = got
            return 0
        lax.fori_loop(0, batch // per, body, 0)

    a = swap_halves(0, part_ref)
    e = send(enc, mate_ref, e_sem.at[0], e_sem.at[1], mate)
    b = share(0, part_ref[core], a)
    project_tokens(enc, 0, 0, k_all)
    project_tokens(enc, 0, 1, v_all)
    c = finish(0, b)
    hidden = x_ref[...].astype(f32) + whole(0, c)
    normed = layer_norm(hidden, gain2_ref[...], bias2_ref[...])
    q_buf[0] = project(normed, wqc[...])
    qs = [send(q_buf.at[0], q_buf.at[k], q_send.at[k], q_recv.at[k], other(k)) for k in (3, 2, 1)]
    with jax.named_scope('mate_tokens'):
        e.wait_recv()
    project_tokens(mate_ref, 1, 0, k_all)
    project_tokens(mate_ref, 1, 1, v_all)
    with jax.named_scope('other_heads'):
        for copy in qs:
            copy.wait_recv()
    q_eight = jnp.concatenate([q_buf[k] for k in range(4)], axis=1).astype(f32)
    many = 8 * GROUP
    col = lax.broadcasted_iota(jnp.int32, (many, wide), 1)
    line = lax.broadcasted_iota(jnp.int32, (many, wide), 0)
    own = col // HEADS_DIM == line % 8
    span = GROUP * 2 * tokens
    match = lax.broadcasted_iota(jnp.int32, (many, span), 1) // (2 * tokens) == lax.broadcasted_iota(jnp.int32, (many, span), 0) // 8
    nt = (((1,), (1,)), ((), ()))
    scale = HEADS_DIM ** -0.5

    def squeeze(values):
        return jnp.sum(jnp.where(own, values, 0.0).reshape(GROUP, 8, wide), axis=1)

    groups = batch // GROUP
    for g in range(groups):
        at = slice(g * GROUP, (g + 1) * GROUP)
        q_g = jnp.broadcast_to(q_eight[at][:, None, :], (GROUP, 8, wide)).reshape(many, wide)
        q_g = jnp.where(own, q_g, 0.0).astype(bf16)
        s_buf[g] = lax.dot_general(q_g, k_all[at].reshape(span, wide), nt, preferred_element_type=f32)
    stats = []
    for g in range(groups):
        s = jnp.where(match, s_buf[g] * scale, NEG)
        top = jnp.max(s, axis=-1, keepdims=True)
        p = jnp.exp(s - top)
        w_buf[g] = p.astype(bf16)
        stats.append(squeeze(jnp.where(col % HEADS_DIM < HEADS_DIM // 2, top, jnp.sum(p, axis=-1, keepdims=True))))
    for g in range(groups):
        at = slice(g * GROUP, (g + 1) * GROUP)
        o = squeeze(jnp.dot(w_buf[g], v_all[at].reshape(span, wide), preferred_element_type=f32))
        for k in range(4):
            o_out[k, g * GROUP:(g + 1) * GROUP, :] = o[:, k * side:(k + 1) * side]
            o_out[k, batch + g * GROUP:batch + (g + 1) * GROUP, :] = stats[g][:, k * side:(k + 1) * side]
    os = [send(o_out.at[k], o_in.at[k], o_send.at[k], o_recv.at[k], other(k)) for k in (3, 2, 1)]
    with jax.named_scope('partial_heads'):
        for copy in os:
            copy.wait_recv()
    low = lax.broadcasted_iota(jnp.int32, (batch, side), 1) < HEADS_DIM
    middle = HEADS_DIM // 2

    def spread(stat, at):
        return jnp.where(low, stat[:, at:at + 1], stat[:, HEADS_DIM + at:HEADS_DIM + at + 1])

    pieces = [o_out[0]] + [o_in[k] for k in range(1, 4)]
    top_of = [spread(p[batch:], 0) for p in pieces]
    sum_of = [spread(p[batch:], middle) for p in pieces]
    top = functools.reduce(jnp.maximum, top_of)
    shares = [jnp.exp(t - top) for t in top_of]
    denom = sum(s * w for s, w in zip(sum_of, shares))
    numer = sum(p[:batch] * w for p, w in zip(pieces, shares))
    cross = (numer / denom).astype(bf16)
    part2 = project(cross, woc[...])
    for i in range(2):
        p_buf[0, i] = part2[:, i * half:(i + 1) * half]
    a = swap_halves(1, p_buf.at[0])
    c = finish(1, share(1, p_buf[0, core], a))
    hidden = hidden + whole(1, c)
    normed = layer_norm(hidden, gain3_ref[...], bias3_ref[...])
    up = jnp.dot(normed, wup[...], preferred_element_type=f32)
    up = (0.5 * up * (1.0 + lax.erf(up * (2.0 ** -0.5)))).astype(bf16)
    part3 = project(up, wdn[...])
    for i in range(2):
        p_buf[1, i] = part3[:, i * half:(i + 1) * half]
    a = swap_halves(2, p_buf.at[1])
    c = finish(2, share(2, p_buf[1, core], a))
    out_ref[...] = (hidden + whole(2, c)).astype(bf16)
    with jax.named_scope('drain'):
        for copy in sends:
            copy.wait_send()


def post_attention(part, x, gain2, bias2, gain3, bias3, enc, weights, wq_c, wo_c, w_up, w_down):
    batch, model = x.shape
    f32, bf16 = jnp.float32, jnp.bfloat16
    vmem = pl.BlockSpec(memory_space=pltpu.VMEM)
    tokens = enc.shape[1]
    side = 2 * HEADS_DIM
    dma = pltpu.SemaphoreType.DMA
    return pl.pallas_call(
        post_kernel,
        out_shape=jax.ShapeDtypeStruct((batch, model), bf16),
        in_specs=[vmem] * 15,
        out_specs=vmem,
        scratch_shapes=[
            pltpu.VMEM((batch, tokens, model), bf16),
            pltpu.VMEM((batch, 2 * tokens, 4 * side), bf16), pltpu.VMEM((batch, 2 * tokens, 4 * side), bf16),
            pltpu.VMEM((4, batch, side), bf16),
            pltpu.VMEM((batch // GROUP, 8 * GROUP, GROUP * 2 * tokens), f32), pltpu.VMEM((batch // GROUP, 8 * GROUP, GROUP * 2 * tokens), bf16),
            pltpu.VMEM((4, 2 * batch, side), f32), pltpu.VMEM((4, 2 * batch, side), f32),
            pltpu.VMEM((2, 2, batch, model // 2), bf16), pltpu.VMEM((3, batch, model // 2), bf16),
            pltpu.VMEM((3, 4, batch, model // 2), bf16), pltpu.VMEM((3, 2, batch, model // 2), bf16),
            dma((2,)), dma((3,)), dma((3,)), dma((3, 4)), dma((3, 4)), dma((3,)), dma((3,)), dma((4,)), dma((4,)), dma((4,)), dma((4,)),
        ],
        compiler_params=pltpu.CompilerParams(collective_id=0, has_side_effects=True, vmem_limit_bytes=24 << 20),
        cost_estimate=pl.CostEstimate(flops=2 * batch * 2 * tokens * model * 8 * side, bytes_accessed=9 << 20, transcendentals=0),
        name="post_attention",
    )(part, x, gain2.reshape(1, model), bias2.reshape(1, model), gain3.reshape(1, model), bias3.reshape(1, model),
      enc, *weights, wq_c, wo_c, w_up, w_down)


def local_step(x, k_cache, v_cache, seq_lens, nbr_enc, ln1_gain, ln1_bias, w_q, w_k, w_v, w_o, ln2_gain, ln2_bias, wq_c, wk_c, wv_c, wo_c, ln3_gain, ln3_bias, w_up, w_down):
    mine = pack(wk_c, wv_c)
    weights = [mine] + [lax.ppermute(mine, 'tp', [(t, t ^ (2 * k)) for t in range(8)]) for k in (1, 2, 3)]
    part, k_new, v_new = self_attention(x, k_cache, v_cache, seq_lens, ln1_gain, ln1_bias, w_q, w_k, w_v, w_o)
    out = post_attention(part, x, ln2_gain, ln2_bias, ln3_gain, ln3_bias, nbr_enc, weights, wq_c, wo_c, w_up, w_down)
    return out, k_new, v_new


def solution(mesh):
    row_spec = P('dp', None)
    cache_spec = P('dp', None, 'tp', None)
    head_spec = P('dp', 'tp', None)
    vec_spec = P(None)
    col_split = P(None, 'tp')
    row_split = P('tp', None)
    in_specs = (row_spec, cache_spec, cache_spec, P('dp'), P('dp', 'tp', None), vec_spec, vec_spec, col_split, col_split, col_split, row_split, vec_spec, vec_spec, col_split, col_split, col_split, row_split, vec_spec, vec_spec, col_split, row_split)
    out_specs = (row_spec, head_spec, head_spec)
    return jax.shard_map(local_step, mesh=mesh, in_specs=in_specs, out_specs=out_specs, check_vma=False)
```

```python
import functools

import jax
import jax.numpy as jnp
from jax import lax
from jax.experimental import pallas as pl
from jax.experimental.pallas import tpu as pltpu
from jax.sharding import PartitionSpec as P

LN_EPS = 1e-5
CHUNK = 1024
SLOTS = 24
UNROLL = 6
NEG = -1e30
HEADS_DIM = 64
PROJ_ROWS = 512
GROUP = 4
MESH = pl.DeviceIdType.MESH


def layer_norm(values, ln_gain, ln_bias):
    row_mean = jnp.mean(values, axis=-1, keepdims=True)
    centred = values - row_mean
    row_var = jnp.mean(jnp.square(centred), axis=-1, keepdims=True)
    return (centred * lax.rsqrt(row_var + LN_EPS) * ln_gain + ln_bias).astype(jnp.bfloat16)


def project(operand, weight):
    return jnp.dot(operand, weight, preferred_element_type=jnp.float32).astype(jnp.bfloat16)


def self_kernel(lens_hbm, x_hbm, gain_hbm, bias_hbm, wq_hbm, wk_hbm, wv_hbm, wo_hbm, k_hbm, v_hbm,
                part_ref, know_ref, vnow_ref,
                lens_ref, x_ref, gain_ref, bias_ref, wq_buf, wk_buf, wv_buf, wo_buf, k_buf, v_buf, q_all, p_buf, acc, mx, sm, row_tab, src_tab, off_tab, rem_tab, size_tab,
                w_sem, k_sem, v_sem):
    batch = x_ref.shape[0]
    dim = k_buf.shape[1]
    weights = [pltpu.make_async_copy(src, dst, w_sem.at[i]) for i, (src, dst) in enumerate(
        ((lens_hbm, lens_ref), (x_hbm, x_ref), (gain_hbm, gain_ref), (bias_hbm, bias_ref), (wq_hbm, wq_buf), (wk_hbm, wk_buf), (wv_hbm, wv_buf),
         (wo_hbm, wo_buf)))]
    for w in weights:
        w.start()

    def fetch(hbm, buf, sem, i, slot, u, thread):
        start = pl.multiple_of(off_tab[i], CHUNK)
        size = pl.multiple_of(size_tab[i], 128)
        pltpu.make_async_copy(
            hbm.at[src_tab[i], :, pl.ds(start, size)], buf.at[slot, :, pl.ds(u * CHUNK, size)], sem.at[slot]).start(priority=thread)

    def await_group(hbm, buf, sem, g, slot):
        size = pl.multiple_of(sum(size_tab[g * UNROLL + u] for u in range(UNROLL)), 128)
        pltpu.make_async_copy(hbm.at[0, :, pl.ds(0, size)], buf.at[slot, :, pl.ds(0, size)], sem.at[slot]).wait()

    for i in range(SLOTS):
        for hbm, buf, sem, thread in ((k_hbm, k_buf, k_sem, 0), (v_hbm, v_buf, v_sem, 1)):
            pltpu.make_async_copy(hbm.at[i, :, pl.ds(0, CHUNK)], buf.at[i // UNROLL, :, pl.ds(i % UNROLL * CHUNK, CHUNK)],
                                  sem.at[i // UNROLL]).start(priority=thread)
    weights[0].wait()

    def build(i, b, start):
        left = lens_ref[b] - start
        row_tab[i] = b
        src_tab[i] = b
        off_tab[i] = start
        rem_tab[i] = left
        return (jnp.minimum(left, CHUNK) + 127) & -128

    def build_first(b, _):
        size_tab[b] = jnp.where(b < SLOTS, CHUNK, build(b, b, 0))
        return 0

    def build_rest(b, at):
        def more(j, at):
            size_tab[at] = build(at, b, j * CHUNK)
            return at + 1
        return lax.fori_loop(1, (lens_ref[b] + CHUNK - 1) // CHUNK, more, at)

    lax.fori_loop(0, batch, build_first, 0)
    items = lax.fori_loop(0, batch, build_rest, jnp.int32(batch))
    groups = (items + UNROLL - 1) // UNROLL
    for extra in range(2 * UNROLL):
        row_tab[items + extra] = batch
        src_tab[items + extra] = batch - 1
        off_tab[items + extra] = 0
        rem_tab[items + extra] = 64
        size_tab[items + extra] = 128

    for w in weights[1:4]:
        w.wait()
    normed = layer_norm(x_ref[...].astype(jnp.float32), gain_ref[...], bias_ref[...])
    for w in weights[4:7]:
        w.wait()
    q_new = project(normed, wq_buf[...])
    k_new = project(normed, wk_buf[...])
    v_new = project(normed, wv_buf[...])
    half = dim // 2
    for h in range(2):
        know_ref[:, h, :] = k_new[:, h * half:(h + 1) * half]
        vnow_ref[:, h, :] = v_new[:, h * half:(h + 1) * half]
    lane = lax.broadcasted_iota(jnp.int32, (batch, 8, dim), 2)
    row = lax.broadcasted_iota(jnp.int32, (batch, 8, dim), 1)
    q_f = q_new.astype(jnp.float32)
    for side in range(2):
        q_all[side, :batch] = jnp.where(lane // half + 2 * side == row, q_f[:, None, :], 0.0).astype(jnp.bfloat16)
        q_all[side, batch] = jnp.zeros((8, dim), jnp.bfloat16)
    own = lane // half == row
    s_new = jnp.sum(jnp.where(own, (q_f * k_new.astype(jnp.float32))[:, None, :], 0.0), axis=-1, keepdims=True) * (half ** -0.5)
    new_row = row < 2
    mx[:batch] = jnp.where(new_row, s_new, NEG)
    sm[:batch] = jnp.where(new_row, 1.0, 0.0)
    acc[:batch] = jnp.where(new_row, v_new.astype(jnp.float32)[:, None, :], 0.0)
    mx[batch] = jnp.zeros((8, dim), jnp.float32)
    sm[batch] = jnp.ones((8, dim), jnp.float32)
    acc[batch] = jnp.zeros((8, dim), jnp.float32)

    spot = lax.broadcasted_iota(jnp.int32, (8, CHUNK), 1)
    line = lax.broadcasted_iota(jnp.int32, (8, CHUNK), 0)
    line1 = lax.broadcasted_iota(jnp.int32, (8, dim), 0)
    scale = half ** -0.5
    pairs = range(0, UNROLL, 2)

    def two(buf, slot, u):
        return jnp.concatenate([buf[slot, :, w * CHUNK:(w + 1) * CHUNK] for w in (u, u + 1)], axis=0)

    def scores(i, slot, u):
        q_two = jnp.concatenate([q_all[0, row_tab[i]], q_all[1, row_tab[i + 1]]], axis=1)
        s = jnp.dot(q_two, two(k_buf, slot, u), preferred_element_type=jnp.float32) * scale
        s = jnp.where(spot < jnp.where(line < 2, rem_tab[i], rem_tab[i + 1]), s, NEG)
        top = jnp.max(s, axis=-1, keepdims=True)
        e = jnp.exp(s - top)
        return e.astype(jnp.bfloat16), top, jnp.sum(e, axis=-1, keepdims=True)

    def weigh(p, slot, u):
        return lax.dot_general(p, two(v_buf, slot, u), (((1,), (1,)), ((), ())), preferred_element_type=jnp.float32)

    def merge(i, o, top, total):
        for side in range(2):
            b = row_tab[i + side]
            mine = line1 // 2 == side
            top_s = jnp.where(mine, top, NEG)
            old = mx[b]
            new = jnp.maximum(old, top_s)
            keep = jnp.exp(old - new)
            add = jnp.exp(top_s - new)
            mx[b] = new
            sm[b] = sm[b] * keep + jnp.where(mine, total, 0.0) * add
            acc[b] = acc[b] * keep + jnp.where(mine, o[:, side * dim:(side + 1) * dim], 0.0) * add

    def score_group(g, slot):
        out = [scores(g * UNROLL + u, slot, u) for u in pairs]
        return out, tuple(x for o in out for x in o[1:])

    def keep_weights(g, out):
        for j, o in enumerate(out):
            p_buf[lax.rem(g, 2), j] = o[0]

    depth = SLOTS // UNROLL
    await_group(k_hbm, k_buf, k_sem, 0, 0)
    first, stats = score_group(0, 0)
    keep_weights(0, first)
    for u in range(UNROLL):
        fetch(k_hbm, k_buf, k_sem, SLOTS + u, 0, u, 0)

    def step(g, stats):
        now, prev = g * UNROLL, (g - 1) * UNROLL
        slot_a = lax.rem(g, depth)
        slot_b = lax.rem(g - 1, depth)

        @pl.when(g < groups)
        def _():
            await_group(k_hbm, k_buf, k_sem, g, slot_a)

        await_group(v_hbm, v_buf, v_sem, g - 1, slot_b)
        p_prev = [p_buf[lax.rem(g - 1, 2), j] for j in range(len(pairs))]
        out, new_stats = score_group(g, slot_a)
        o = [weigh(p_prev[j], slot_b, u) for j, u in enumerate(pairs)]
        for j, u in enumerate(pairs):
            merge(prev + u, o[j], stats[2 * j], stats[2 * j + 1])
        keep_weights(g, out)

        @pl.when(g + depth < groups)
        def _():
            for u in range(UNROLL):
                fetch(k_hbm, k_buf, k_sem, now + SLOTS + u, slot_a, u, 0)

        @pl.when(g - 1 + depth < groups)
        def _():
            for u in range(UNROLL):
                fetch(v_hbm, v_buf, v_sem, prev + SLOTS + u, slot_b, u, 1)

        return new_stats

    lax.fori_loop(1, groups + 1, step, stats)

    lane2 = lax.broadcasted_iota(jnp.int32, (batch, dim), 1)

    def head(h):
        top_a, top_b = mx[:batch, h, :], mx[:batch, h + 2, :]
        top = jnp.maximum(top_a, top_b)
        share_a, share_b = jnp.exp(top_a - top), jnp.exp(top_b - top)
        numer = acc[:batch, h, :] * share_a + acc[:batch, h + 2, :] * share_b
        return numer / (sm[:batch, h, :] * share_a + sm[:batch, h + 2, :] * share_b)

    out = jnp.where(lane2 < half, head(0), head(1)).astype(jnp.bfloat16)
    weights[7].wait()
    part = project(out, wo_buf[...])
    cut = part_ref.shape[2]
    for i in range(2):
        part_ref[i] = part[:, i * cut:(i + 1) * cut]


def self_attention(x, k_cache, v_cache, seq_lens, gain, bias, w_q, w_k, w_v, w_o):
    batch, ctx, heads, head_dim = k_cache.shape
    dim = heads * head_dim
    model = x.shape[1]
    most = batch * (ctx // CHUNK) + 2 * UNROLL + 2
    k_t = k_cache.transpose(0, 2, 3, 1).reshape(batch, dim, ctx)
    v_t = v_cache.transpose(0, 2, 3, 1).reshape(batch, dim, ctx)
    vmem = pl.BlockSpec(memory_space=pltpu.VMEM)
    f32, bf16 = jnp.float32, jnp.bfloat16
    return pl.pallas_call(
        self_kernel,
        out_shape=(jax.ShapeDtypeStruct((2, batch, model // 2), bf16),
                   jax.ShapeDtypeStruct((batch, heads, head_dim), bf16),
                   jax.ShapeDtypeStruct((batch, heads, head_dim), bf16)),
        in_specs=[pl.BlockSpec(memory_space=pltpu.HBM)] * 10,
        out_specs=(vmem, vmem, vmem),
        scratch_shapes=[
            pltpu.SMEM((batch,), jnp.int32),
            pltpu.VMEM((batch, model), bf16), pltpu.VMEM((1, model), f32), pltpu.VMEM((1, model), f32),
            pltpu.VMEM((model, dim), bf16), pltpu.VMEM((model, dim), bf16), pltpu.VMEM((model, dim), bf16),
            pltpu.VMEM((dim, model), bf16),
            pltpu.VMEM((SLOTS // UNROLL, dim, UNROLL * CHUNK), bf16), pltpu.VMEM((SLOTS // UNROLL, dim, UNROLL * CHUNK), bf16),
            pltpu.VMEM((2, batch + 1, 8, dim), bf16),
            pltpu.VMEM((2, UNROLL // 2, 8, CHUNK), bf16),
            pltpu.VMEM((batch + 1, 8, dim), f32), pltpu.VMEM((batch + 1, 8, dim), f32), pltpu.VMEM((batch + 1, 8, dim), f32),
            *[pltpu.SMEM((most,), jnp.int32)] * 5,
            pltpu.SemaphoreType.DMA((8,)), pltpu.SemaphoreType.DMA((SLOTS // UNROLL,)), pltpu.SemaphoreType.DMA((SLOTS // UNROLL,)),
        ],
        cost_estimate=pl.CostEstimate(flops=2 * 2 * batch * ctx * dim * 8, bytes_accessed=batch * ctx * dim * 2, transcendentals=0),
        compiler_params=pltpu.CompilerParams(vmem_limit_bytes=32 << 20),
        name="self_attention",
    )(*[pltpu.with_memory_space_constraint(v, pltpu.HBM)
        for v in (seq_lens, x, gain.reshape(1, model), bias.reshape(1, model), w_q, w_k, w_v, w_o, k_t, v_t)])


def pack_kernel(a_hbm, b_hbm, out_ref, sem):
    width = a_hbm.shape[1]
    copies = [pltpu.make_async_copy(src, out_ref.at[:, pl.ds(i * width, width)], sem.at[i]) for i, src in enumerate((a_hbm, b_hbm))]
    for copy in copies:
        copy.start()
    for copy in copies:
        copy.wait()


def pack(*parts):
    model, width = parts[0].shape
    return pl.pallas_call(
        pack_kernel,
        out_shape=jax.ShapeDtypeStruct((model, 2 * width), parts[0].dtype),
        in_specs=[pl.BlockSpec(memory_space=pltpu.HBM)] * 2,
        out_specs=pl.BlockSpec(memory_space=pltpu.VMEM),
        scratch_shapes=[pltpu.SemaphoreType.DMA((2,))],
        compiler_params=pltpu.CompilerParams(vmem_limit_bytes=8 << 20),
        name="pack_weights",
    )(*[pltpu.with_memory_space_constraint(v, pltpu.HBM) for v in parts])


def post_kernel(part_ref, x_ref, gain2_ref, bias2_ref, gain3_ref, bias3_ref, enc, w0, w1, w2, w3, wqc, woc, wup, wdn, out_ref,
                mate_ref, k_all, v_all, q_buf, s_buf, w_buf, o_out, o_in, p_buf, a_buf, b_buf, c_buf,
                e_sem, a_send, a_recv, b_send, b_recv, c_send, c_recv, q_send, q_recv, o_send, o_recv):
    f32, bf16 = jnp.float32, jnp.bfloat16
    batch, model = x_ref.shape
    half = model // 2
    me = lax.axis_index('tp')
    chip, core = me // 2, me % 2
    chip_y, chip_x = chip // 2, chip % 2
    mate = 2 * chip + 1 - core

    def other(k):
        return 2 * (2 * (1 - chip_y if k // 2 else chip_y) + (1 - chip_x if k % 2 else chip_x)) + core

    barrier = pltpu.get_barrier_semaphore()
    for device in (other(3), other(2), other(1), mate):
        pl.semaphore_signal(barrier, inc=1, device_id={'tp': device}, device_id_type=MESH)
    with jax.named_scope('barrier'):
        pl.semaphore_wait(barrier, 4)

    sends = []

    def send(src, dst, send_sem, recv_sem, device):
        copy = pltpu.make_async_remote_copy(src_ref=src, dst_ref=dst, send_sem=send_sem, recv_sem=recv_sem,
                                            device_id={'tp': device}, device_id_type=MESH)
        copy.start()
        sends.append(copy)
        return copy

    def swap_halves(n, parts):
        return send(parts.at[1 - core], a_buf.at[n], a_send.at[n], a_recv.at[n], mate)

    def share(n, mine, copy):
        with jax.named_scope('mate_half'):
            copy.wait_recv()
        b_buf[n, chip] = (mine.astype(f32) + a_buf[n].astype(f32)).astype(bf16)
        return [send(b_buf.at[n, chip], b_buf.at[n, chip], b_send.at[n, k], b_recv.at[n, k], other(k)) for k in (3, 2, 1)]

    def finish(n, copies):
        with jax.named_scope('chip_sums'):
            for copy in copies:
                copy.wait_recv()
        total = b_buf[n, 0].astype(f32)
        for i in range(1, 4):
            total = total + b_buf[n, i].astype(f32)
        c_buf[n, core] = total.astype(bf16)
        return send(c_buf.at[n, core], c_buf.at[n, core], c_send.at[n], c_recv.at[n], mate)

    def whole(n, copy):
        with jax.named_scope('mate_sum'):
            copy.wait_recv()
        return jnp.concatenate([c_buf[n, 0], c_buf[n, 1]], axis=1).astype(f32)

    tokens = enc.shape[1]
    rows = PROJ_ROWS
    per = rows // tokens
    side = 2 * HEADS_DIM
    wide = 4 * side

    def weight(i):
        return jnp.concatenate([w[:, i * side:(i + 1) * side] for w in (w0, w1, w2, w3)], axis=1)

    def project_tokens(source, place, i, dest):
        def body(j, _):
            lines = source[pl.ds(j * per, per)].reshape(rows, model)
            got = project(lines, weight(i)).reshape(per, tokens, wide)
            dest[pl.ds(j * per, per), place * tokens:(place + 1) * tokens, :] = got
            return 0
        lax.fori_loop(0, batch // per, body, 0)

    a = swap_halves(0, part_ref)
    e = send(enc, mate_ref, e_sem.at[0], e_sem.at[1], mate)
    b = share(0, part_ref[core], a)
    project_tokens(enc, 0, 0, k_all)
    project_tokens(enc, 0, 1, v_all)
    c = finish(0, b)
    hidden = x_ref[...].astype(f32) + whole(0, c)
    normed = layer_norm(hidden, gain2_ref[...], bias2_ref[...])
    q_buf[0] = project(normed, wqc[...])
    qs = [send(q_buf.at[0], q_buf.at[k], q_send.at[k], q_recv.at[k], other(k)) for k in (3, 2, 1)]
    with jax.named_scope('mate_tokens'):
        e.wait_recv()
    project_tokens(mate_ref, 1, 0, k_all)
    project_tokens(mate_ref, 1, 1, v_all)
    with jax.named_scope('other_heads'):
        for copy in qs:
            copy.wait_recv()
    q_eight = jnp.concatenate([q_buf[k] for k in range(4)], axis=1).astype(f32)
    many = 8 * GROUP
    col = lax.broadcasted_iota(jnp.int32, (many, wide), 1)
    line = lax.broadcasted_iota(jnp.int32, (many, wide), 0)
    own = col // HEADS_DIM == line % 8
    span = GROUP * 2 * tokens
    match = lax.broadcasted_iota(jnp.int32, (many, span), 1) // (2 * tokens) == lax.broadcasted_iota(jnp.int32, (many, span), 0) // 8
    nt = (((1,), (1,)), ((), ()))
    scale = HEADS_DIM ** -0.5

    def squeeze(values):
        return jnp.sum(jnp.where(own, values, 0.0).reshape(GROUP, 8, wide), axis=1)

    groups = batch // GROUP
    for g in range(groups):
        at = slice(g * GROUP, (g + 1) * GROUP)
        q_g = jnp.broadcast_to(q_eight[at][:, None, :], (GROUP, 8, wide)).reshape(many, wide)
        q_g = jnp.where(own, q_g, 0.0).astype(bf16)
        s_buf[g] = lax.dot_general(q_g, k_all[at].reshape(span, wide), nt, preferred_element_type=f32)
    stats = []
    for g in range(groups):
        s = jnp.where(match, s_buf[g] * scale, NEG)
        top = jnp.max(s, axis=-1, keepdims=True)
        p = jnp.exp(s - top)
        w_buf[g] = p.astype(bf16)
        stats.append(squeeze(jnp.where(col % HEADS_DIM < HEADS_DIM // 2, top, jnp.sum(p, axis=-1, keepdims=True))))
    for g in range(groups):
        at = slice(g * GROUP, (g + 1) * GROUP)
        o = squeeze(jnp.dot(w_buf[g], v_all[at].reshape(span, wide), preferred_element_type=f32))
        for k in range(4):
            o_out[k, g * GROUP:(g + 1) * GROUP, :] = o[:, k * side:(k + 1) * side]
            o_out[k, batch + g * GROUP:batch + (g + 1) * GROUP, :] = stats[g][:, k * side:(k + 1) * side]
    os = [send(o_out.at[k], o_in.at[k], o_send.at[k], o_recv.at[k], other(k)) for k in (3, 2, 1)]
    with jax.named_scope('partial_heads'):
        for copy in os:
            copy.wait_recv()
    low = lax.broadcasted_iota(jnp.int32, (batch, side), 1) < HEADS_DIM
    middle = HEADS_DIM // 2

    def spread(stat, at):
        return jnp.where(low, stat[:, at:at + 1], stat[:, HEADS_DIM + at:HEADS_DIM + at + 1])

    pieces = [o_out[0]] + [o_in[k] for k in range(1, 4)]
    top_of = [spread(p[batch:], 0) for p in pieces]
    sum_of = [spread(p[batch:], middle) for p in pieces]
    top = functools.reduce(jnp.maximum, top_of)
    shares = [jnp.exp(t - top) for t in top_of]
    denom = sum(s * w for s, w in zip(sum_of, shares))
    numer = sum(p[:batch] * w for p, w in zip(pieces, shares))
    cross = (numer / denom).astype(bf16)
    part2 = project(cross, woc[...])
    for i in range(2):
        p_buf[0, i] = part2[:, i * half:(i + 1) * half]
    a = swap_halves(1, p_buf.at[0])
    c = finish(1, share(1, p_buf[0, core], a))
    hidden = hidden + whole(1, c)
    normed = layer_norm(hidden, gain3_ref[...], bias3_ref[...])
    up = jnp.dot(normed, wup[...], preferred_element_type=f32)
    up = (0.5 * up * (1.0 + lax.erf(up * (2.0 ** -0.5)))).astype(bf16)
    part3 = project(up, wdn[...])
    for i in range(2):
        p_buf[1, i] = part3[:, i * half:(i + 1) * half]
    a = swap_halves(2, p_buf.at[1])
    c = finish(2, share(2, p_buf[1, core], a))
    out_ref[...] = (hidden + whole(2, c)).astype(bf16)
    with jax.named_scope('drain'):
        for copy in sends:
            copy.wait_send()


def post_attention(part, x, gain2, bias2, gain3, bias3, enc, weights, wq_c, wo_c, w_up, w_down):
    batch, model = x.shape
    f32, bf16 = jnp.float32, jnp.bfloat16
    vmem = pl.BlockSpec(memory_space=pltpu.VMEM)
    tokens = enc.shape[1]
    side = 2 * HEADS_DIM
    dma = pltpu.SemaphoreType.DMA
    return pl.pallas_call(
        post_kernel,
        out_shape=jax.ShapeDtypeStruct((batch, model), bf16),
        in_specs=[vmem] * 15,
        out_specs=vmem,
        scratch_shapes=[
            pltpu.VMEM((batch, tokens, model), bf16),
            pltpu.VMEM((batch, 2 * tokens, 4 * side), bf16), pltpu.VMEM((batch, 2 * tokens, 4 * side), bf16),
            pltpu.VMEM((4, batch, side), bf16),
            pltpu.VMEM((batch // GROUP, 8 * GROUP, GROUP * 2 * tokens), f32), pltpu.VMEM((batch // GROUP, 8 * GROUP, GROUP * 2 * tokens), bf16),
            pltpu.VMEM((4, 2 * batch, side), f32), pltpu.VMEM((4, 2 * batch, side), f32),
            pltpu.VMEM((2, 2, batch, model // 2), bf16), pltpu.VMEM((3, batch, model // 2), bf16),
            pltpu.VMEM((3, 4, batch, model // 2), bf16), pltpu.VMEM((3, 2, batch, model // 2), bf16),
            dma((2,)), dma((3,)), dma((3,)), dma((3, 4)), dma((3, 4)), dma((3,)), dma((3,)), dma((4,)), dma((4,)), dma((4,)), dma((4,)),
        ],
        compiler_params=pltpu.CompilerParams(collective_id=0, has_side_effects=True, vmem_limit_bytes=24 << 20),
        cost_estimate=pl.CostEstimate(flops=2 * batch * 2 * tokens * model * 8 * side, bytes_accessed=9 << 20, transcendentals=0),
        name="post_attention",
    )(part, x, gain2.reshape(1, model), bias2.reshape(1, model), gain3.reshape(1, model), bias3.reshape(1, model),
      enc, *weights, wq_c, wo_c, w_up, w_down)


def local_step(x, k_cache, v_cache, seq_lens, nbr_enc, ln1_gain, ln1_bias, w_q, w_k, w_v, w_o, ln2_gain, ln2_bias, wq_c, wk_c, wv_c, wo_c, ln3_gain, ln3_bias, w_up, w_down):
    mine = pack(wk_c, wv_c)
    weights = [mine] + [lax.ppermute(mine, 'tp', [(t, t ^ (2 * k)) for t in range(8)]) for k in (1, 2, 3)]
    part, k_new, v_new = self_attention(x, k_cache, v_cache, seq_lens, ln1_gain, ln1_bias, w_q, w_k, w_v, w_o)
    out = post_attention(part, x, ln2_gain, ln2_bias, ln3_gain, ln3_bias, nbr_enc, weights, wq_c, wo_c, w_up, w_down)
    return out, k_new, v_new


def solution(mesh):
    row_spec = P('dp', None)
    cache_spec = P('dp', None, 'tp', None)
    head_spec = P('dp', 'tp', None)
    vec_spec = P(None)
    col_split = P(None, 'tp')
    row_split = P('tp', None)
    in_specs = (row_spec, cache_spec, cache_spec, P('dp'), P('dp', 'tp', None), vec_spec, vec_spec, col_split, col_split, col_split, row_split, vec_spec, vec_spec, col_split, col_split, col_split, row_split, vec_spec, vec_spec, col_split, row_split)
    out_specs = (row_spec, head_spec, head_spec)
    return jax.shard_map(local_step, mesh=mesh, in_specs=in_specs, out_specs=out_specs, check_vma=False)
```
